32 devices in a mesh: dp: 2 (over y), seq: 4 (over z), chan: 4 (over x, core).
Axes of the slice: x: 2, y: 2, z: 4, core: 2. Of those that a mesh axis runs over, the one named last changes fastest.
Arguments:
- layer_input: bfloat16 [2, 512, 2560], P('dp', ('seq', 'chan')), may hold values from -6 to 6
- inner_weight: bfloat16 [2560, 2560], P(None, 'chan'), may hold values from -0.125 to 0.125
- mixer_weight: bfloat16 [2560, 256], replicated, may hold values from -0.01171875 to 0.01171875
- step_weight: bfloat16 [2560, 40], P(None, 'chan'), may hold values from -0.125 to 0.125
- conv_inner: float32 [4, 2560], P(None, 'chan'), may hold values from -3 to 3
- conv_mixer: float32 [4, 256], replicated, may hold values from -3 to 3
- step_bias: float32 [40], P('chan'), may hold values from -2 to 1
- decay_log: float32 [40], P('chan'), as said below
- skip_gain: float32 [40], P('chan'), may hold values from 0.5 to 1.5
- output_grad: bfloat16 [2, 512, 2560], P('dp', 'seq', 'chan'), may hold values from -6 to 6
Outputs:
- input_grad: bfloat16 [2, 512, 2560], P('dp', ('seq', 'chan'))
- inner_weight_grad: float32 [2560, 2560], P(('dp', 'seq'), 'chan')
- mixer_weight_grad: float32 [2560, 256], P(('dp', 'seq', 'chan'))
- step_weight_grad: float32 [2560, 40], P(('dp', 'seq'), 'chan')
The draws below stay inside these ranges and needn't reach their ends.
Inputs may be any that keep to these rules, and one draw needn't show every extreme that they name: exp(decay_log) is at least 0.2 / 512.
All inputs are finite; a program needn't handle non-finite values.
Results may differ from the reference program's by a relative error of at most 0.014.
Values may be sent and summed in bfloat16 or wider, within the bound.
No kernel may reach another device: no remote copies, remote signals or barrier semaphores. Data moves between devices by JAX's collectives and lax.ppermute only.
A program may use at most 128 MiB of HBM per device.

```python
import math
import jax
import jax.numpy as jnp
from jax import lax

D = 2560
HEADS = 40
HDIM = 64
STATE = 128
KW = 4
BATCH = 2
LENGTH = 512
TOKENS = 1024
INNER = 2560


def draw_decay_log(key, part):
    base = jax.random.fold_in(key, 71)
    order_key, slow_key, fast_key = jax.random.split(base, 3)
    ranks = jax.random.permutation(order_key, HEADS)
    slow_count = HEADS // 2
    is_slow = ranks < slow_count
    slow_rate = jnp.exp(jax.random.uniform(slow_key, (HEADS,), jnp.float32, jnp.log(0.2), jnp.log(2.0))) / LENGTH
    fast_rate = jnp.exp(jax.random.uniform(fast_key, (HEADS,), jnp.float32, jnp.log(0.02), jnp.log(0.06)))
    return jnp.log(jnp.where(is_slow, slow_rate, fast_rate)).astype(jnp.float32)


def spiked(entries, own_key, source, target, parts, factor):
    def block_of(dim):
        return (jnp.arange(entries.shape[dim]) // (entries.shape[dim] // parts)).reshape((-1,) + (1,) * (entries.ndim - 1 - dim))

    first = jax.random.permutation(own_key, parts)[block_of(target)]
    other_side = (block_of(target) + parts // 2) % parts
    return jnp.where((block_of(source) == first) | (block_of(source) == other_side), factor * entries, entries)


def shard_levels(key, dims, cuts, least, top_value):
    gain = 1.0
    for position, shards_of in cuts:
        steps = jax.random.uniform(jax.random.fold_in(jax.random.fold_in(key, 6), position), (shards_of,), jnp.float32, least / len(cuts), top_value / len(cuts))
        gain = gain * jnp.repeat(jnp.exp(steps), dims[position] // shards_of).reshape((-1,) + (1,) * (len(dims) - 1 - position))
    return gain


def gaussian(stream_key, shape, width, most, cuts=(), held_as=jnp.bfloat16):
    values = jax.random.normal(stream_key, shape, jnp.float32) * width
    if len(cuts) > 0:
        values = shard_levels(stream_key, shape, cuts, -0.22, 0.18) * values
    return jnp.clip(values, min=-most, max=most).astype(held_as)


def noise_with(own_key, dims, width, most, cuts, heavy, kind=jnp.bfloat16):
    drawn = width * jax.random.normal(own_key, dims, jnp.float32)
    if cuts:
        drawn = drawn * shard_levels(own_key, dims, cuts, -0.22, 0.18)
    return jnp.clip(spiked(drawn, jax.random.fold_in(own_key, 3), *heavy), -most, most).astype(kind)


def setup_inputs(seed: int = 0) -> dict:
    splits = jax.random.split(jax.random.key(seed), 11)
    return {
        "layer_input": noise_with(splits[0], (BATCH, LENGTH, D), 1.0, 6.0, ((0, 2), (1, 16)), (1, 2, 16, 2.0)),
        "inner_weight": gaussian(splits[1], (D, INNER), D ** -0.5, 0.125, ((1, 4),)),
        "mixer_weight": gaussian(splits[2], (D, 2 * STATE), (0.1 / D ** 0.5), 0.01171875),
        "step_weight": gaussian(splits[3], (D, HEADS), D ** -0.5, 0.125, ((1, 4),)),
        "conv_inner": gaussian(splits[4], (KW, INNER), KW ** -0.5, 3.0, ((1, 4),), jnp.float32),
        "conv_mixer": gaussian(splits[5], (KW, 2 * STATE), KW ** -0.5, 3.0, (), jnp.float32),
        "step_bias": jnp.clip(-2.0 + 3.0 * jax.random.uniform(splits[6], (HEADS,), jnp.float32) ** shard_levels(splits[6], (HEADS,), ((0, 4),), -0.2, 0.2), -2.0, 1.0),
        "decay_log": draw_decay_log(jax.random.fold_in(splits[10], 71), 0),
        "skip_gain": jnp.clip(0.5 + 1.0 * jax.random.uniform(splits[8], (HEADS,), jnp.float32) ** shard_levels(splits[8], (HEADS,), ((0, 4),), -0.2, 0.2), 0.5, 1.5),
        "output_grad": gaussian(splits[9], (BATCH, LENGTH, INNER), 1.0, 6.0, ((0, 2), (1, 4), (2, 4))),
    }


block_tokens = 256

def conv_silu(inputs, history, kernel):
    length = inputs.shape[0]
    padded = jnp.concatenate([history, inputs], axis=0)
    summed = kernel[0][None, :] * padded[0:length]
    for offset in range(1, kernel.shape[0]):
        summed = summed + kernel[offset][None, :] * padded[offset:offset + length]
    return jax.nn.silu(summed)

def activations(inner_proj, mixer_proj, step_raw, inner_hist, mixer_hist, conv_inner, conv_mixer, step_bias, decay_log):
    length = inner_proj.shape[0]
    head_count = step_bias.shape[0]
    state_width = mixer_proj.shape[1] // 2
    inner_act = conv_silu(inner_proj, inner_hist, conv_inner).reshape(length, head_count, -1)
    mixer_act = conv_silu(mixer_proj, mixer_hist, conv_mixer)
    step_size = jax.nn.softplus(step_raw + step_bias[None, :])
    log_decay = -step_size * jnp.exp(decay_log)[None, :]
    return (inner_act, mixer_act[:, :state_width], mixer_act[:, state_width:], step_size, log_decay)

def spanned_scan(inner_act, input_mix, output_mix, step_size, log_decay, skip_gain, initial):
    length, head_count, head_dim = inner_act.shape
    block_len = min(block_tokens, length)
    blocks = length // block_len
    highest = lax.Precision.HIGHEST

    def to_blocks(values):
        return values.reshape((blocks, block_len) + values.shape[1:])

    def advance(carry_state, pieces):
        part_inner, part_input, part_output, part_step, part_decay = pieces
        cumulative = jnp.cumsum(part_decay, axis=0)
        scores = jnp.dot(part_output, part_input.T, precision=highest)
        causal = (jnp.arange(block_len)[:, None] >= jnp.arange(block_len)[None, :])[:, :, None]
        spread = cumulative[:, None, :] - cumulative[None, :, :]
        weights = jnp.where(causal, jnp.exp(jnp.where(causal, spread, 0.0)), 0.0)
        weights = weights * scores[:, :, None] * part_step[None, :, :]
        within = jnp.einsum('ijh,jhp->ihp', weights, part_inner, precision=highest)
        carried = jnp.exp(cumulative)[:, :, None] * jnp.einsum('in,hpn->ihp', part_output, carry_state, precision=highest)
        result = within + carried + skip_gain[None, :, None] * part_inner
        tail_weight = jnp.exp(cumulative[-1][None, :] - cumulative) * part_step
        update_term = jnp.einsum('jh,jhp,jn->hpn', tail_weight, part_inner, part_input, precision=highest)
        carry_state = jnp.exp(cumulative[-1])[:, None, None] * carry_state + update_term
        return (carry_state, result)
    final, results = lax.scan(jax.checkpoint(advance), initial, (to_blocks(inner_act), to_blocks(input_mix), to_blocks(output_mix), to_blocks(step_size), to_blocks(log_decay)))
    return (results.reshape(length, head_count, head_dim), final)

def contract_rows(left_rows, right_rows):
    return lax.dot_general(left_rows, right_rows, (((0,), (0,)), ((), ())), preferred_element_type=jnp.float32)

def project_back(gradient, weight):
    return lax.dot_general(gradient, weight, (((1,), (1,)), ((), ())), preferred_element_type=jnp.float32)

def reference(layer_input, inner_weight, mixer_weight, step_weight, conv_inner, conv_mixer, step_bias, decay_log, skip_gain, output_grad):
    history_len = KW - 1
    highest = lax.Precision.HIGHEST
    inner_acc = jnp.zeros((D, INNER), jnp.float32)
    mixer_acc = jnp.zeros((D, 2 * STATE), jnp.float32)
    step_acc = jnp.zeros((D, HEADS), jnp.float32)
    input_grads = []
    zero_inner = jnp.zeros((history_len, INNER), jnp.float32)
    zero_mixer = jnp.zeros((history_len, 2 * STATE), jnp.float32)
    initial = jnp.zeros((HEADS, HDIM, STATE), jnp.float32)
    for batch_row in range(BATCH):
        tokens = layer_input[batch_row]
        inner_proj = jnp.dot(tokens, inner_weight, preferred_element_type=jnp.float32).astype(jnp.bfloat16)
        mixer_proj = jnp.dot(tokens, mixer_weight, preferred_element_type=jnp.float32).astype(jnp.bfloat16)
        step_raw = jnp.dot(tokens, step_weight, preferred_element_type=jnp.float32)
        inner_wide = lax.optimization_barrier(inner_proj).astype(jnp.float32)
        mixer_wide = lax.optimization_barrier(mixer_proj).astype(jnp.float32)

        def layer(inner_in, mixer_in, step_in):
            acts = activations(inner_in, mixer_in, step_in, zero_inner, zero_mixer, conv_inner, conv_mixer, step_bias, decay_log)
            result, final = spanned_scan(acts[0], acts[1], acts[2], acts[3], acts[4], skip_gain, initial)
            return result.reshape(LENGTH, INNER)
        unused, pull = jax.vjp(layer, inner_wide, mixer_wide, step_raw)
        grad_inner, grad_mixer, grad_step = pull(output_grad[batch_row].astype(jnp.float32))
        grad_inner = grad_inner.astype(jnp.bfloat16)
        grad_step = grad_step.astype(jnp.bfloat16)
        summed = project_back(grad_inner, inner_weight) + project_back(grad_step, step_weight)
        summed = summed + lax.dot_general(grad_mixer, mixer_weight.astype(jnp.float32), (((1,), (1,)), ((), ())), precision=highest)
        input_grads.append(summed.astype(jnp.bfloat16))
        inner_acc = inner_acc + contract_rows(tokens, grad_inner)
        step_acc = step_acc + contract_rows(tokens, grad_step)
        mixer_acc = mixer_acc + lax.dot_general(tokens.astype(jnp.float32), grad_mixer, (((0,), (0,)), ((), ())), precision=highest)
    norm_factor = 1.0 / math.sqrt(TOKENS)
    return (jnp.stack(input_grads, axis=0), inner_acc * norm_factor, mixer_acc * norm_factor, step_acc * norm_factor)
```

```python
import functools
import math

import jax
import jax.numpy as jnp
from jax import lax
from jax.experimental import pallas as pl
from jax.experimental.pallas import tpu as pltpu
from jax.sharding import PartitionSpec as P


F32 = jnp.float32
BF16 = jnp.bfloat16
LANES = 128
PAD = 8
HIGHEST = lax.Precision.HIGHEST
DIRECT = 8


def dot(left, right, left_dim=1, right_dim=0, precision=None):
    return lax.dot_general(
        left,
        right,
        (((left_dim,), (right_dim,)), ((), ())),
        precision=precision,
        preferred_element_type=F32,
    )


def pieces(values):
    high = values.astype(BF16)
    rest = values - high.astype(F32)
    middle = rest.astype(BF16)
    low = (rest - middle.astype(F32)).astype(BF16)
    return high, middle, low


def head_map(width, head_dim):
    row = lax.broadcasted_iota(jnp.int32, (LANES, width), 0)
    column = lax.broadcasted_iota(jnp.int32, (LANES, width), 1)
    start = row * head_dim
    return jnp.where((column >= start) & (column < start + head_dim), 1.0, 0.0).astype(BF16)


def spread(values, heads):
    high, middle, low = pieces(values)
    return dot(high, heads) + dot(middle, heads) + dot(low, heads)


def collect(values, heads):
    high, middle, low = pieces(values)
    return dot(high, heads, 1, 1) + dot(middle, heads, 1, 1) + dot(low, heads, 1, 1)


def sigmoid(values):
    return 1.0 / (1.0 + jnp.exp(-values))


def softplus(values):
    small = jnp.exp(-jnp.abs(values))
    series = small * (1.0 - small * (0.5 - small * (1.0 / 3.0)))
    return jnp.maximum(values, 0.0) + jnp.where(small < 1e-3, series, jnp.log(1.0 + small))


def triangle(length):
    row = lax.broadcasted_iota(jnp.int32, (length, length), 0)
    column = lax.broadcasted_iota(jnp.int32, (length, length), 1)
    return row, column


def convolve(values, history, kernel, scratch):
    length = values.shape[0]
    taps = kernel.shape[0]
    scratch[:PAD] = history.astype(F32)
    scratch[PAD:] = values.astype(F32)
    total = kernel[taps - 1 : taps] * scratch[PAD : PAD + length]
    for tap in range(taps - 1):
        start = PAD - (taps - 1) + tap
        total = total + kernel[tap : tap + 1] * scratch[start : start + length]
    return total


def convolve_back(gradient, kernel, scratch):
    length = gradient.shape[0]
    taps = kernel.shape[0]
    zeros = jnp.zeros((PAD, gradient.shape[1]), F32)
    scratch[:PAD] = zeros
    scratch[PAD : PAD + length] = gradient
    scratch[PAD + length :] = zeros
    extent = length + PAD
    total = None
    for tap in range(taps):
        start = taps - 1 - tap
        term = kernel[tap : tap + 1] * scratch[start : start + extent]
        total = term if total is None else total + term
    return total


def blocks(
    rows,
    padded,
    dp_count,
    place_ref,
    own_ref,
    step_ref,
    bias_ref,
    log_ref,
    skip_ref,
    out_ref,
    head_ref,
    near_ref,
    far_ref,
    scratch,
):
    dp_place = place_ref[1]
    seq_count = out_ref.shape[0]
    head_count = bias_ref.shape[1]
    scratch[...] = jnp.zeros_like(scratch)
    scratch[:head_count] = step_ref[...].astype(F32)
    turned = scratch[...].T.astype(BF16)
    near_ref[...] = turned
    far_ref[...] = turned
    head_ref[...] = jnp.zeros_like(head_ref)
    head_ref[0:1, :head_count] = bias_ref[...]
    head_ref[1:2, :head_count] = log_ref[...]
    head_ref[2:3, :head_count] = skip_ref[...]
    fill = jnp.zeros((own_ref.shape[0], padded - rows), F32)
    for target in range(seq_count):
        for hop in range(dp_count):
            wanted = lax.rem(dp_place + hop, dp_count)
            chosen = None
            for other in range(dp_count):
                start = (other * seq_count + target) * rows
                part = own_ref[:, start : start + rows].astype(F32)
                chosen = part if chosen is None else jnp.where(wanted == other, part, chosen)
            span = slice(hop * padded, (hop + 1) * padded)
            if padded > rows:
                chosen = jnp.concatenate([chosen, fill], axis=1)
            out_ref[target, :, span] = chosen.astype(BF16)


def add_up(*refs):
    total = refs[0][...].astype(F32)
    for part in refs[1:-1]:
        total = total + part[...].astype(F32)
    refs[-1][...] = total.astype(refs[-1].dtype)


def project(count, place_ref, *refs):
    tokens = refs[:count]
    inner_ref, mixer_ref, step_ref, inner_out, mixer_out, raw_out, tail_out, scratch = refs[count:]
    place = place_ref[2]
    rows = tokens[0].shape[0]
    for hop in range(count):
        source = lax.rem(place - hop + count, count)
        scratch[pl.ds(pl.multiple_of(source * rows, rows), rows)] = tokens[hop][...]
    gathered = scratch[...]
    length = gathered.shape[0]
    width = inner_ref.shape[1]
    whole = width // (2 * LANES) * (2 * LANES)
    mixer = dot(gathered, mixer_ref[...]).astype(BF16)
    first = dot(gathered, inner_ref[:, :whole]).astype(BF16)
    joined = jnp.concatenate([inner_ref[:, whole:], step_ref[...]], axis=1)
    second = dot(gathered, joined)
    raw_out[...] = second[:, width - whole :]
    inner = jnp.concatenate([first, second[:, : width - whole].astype(BF16)], axis=1)
    inner_out[...] = inner
    mixer_out[...] = mixer
    tail_out[:, :width] = inner[length - 2 * PAD :]
    tail_out[:, width:] = mixer[length - 2 * PAD :]


def prepare(head_dim, relative, place_ref, *refs):
    (
        inner_ref,
        mixer_ref,
        history_ref,
        raw_ref,
        head_ref,
        upstream_ref,
        conv_inner_ref,
        conv_mixer_ref,
        inner_pre_ref,
        mixer_pre_ref,
        step_ref,
        decay_ref,
    ) = refs[:12]
    message_refs = refs[12:-2]
    inner_scratch, mixer_scratch = refs[-2:]
    length, width = inner_ref.shape
    state = mixer_ref.shape[1] // 2
    place = place_ref[0]
    history = history_ref[...].astype(F32)[PAD:]
    inner_pre = convolve(inner_ref[...], history[:, :width], conv_inner_ref[...], inner_scratch)
    mixer_pre = convolve(mixer_ref[...], history[:, width:], conv_mixer_ref[...], mixer_scratch)
    inner_pre_ref[...] = inner_pre
    mixer_pre_ref[...] = mixer_pre
    inner_act = inner_pre * sigmoid(inner_pre)
    mixer_act = mixer_pre * sigmoid(mixer_pre)
    step = softplus(raw_ref[...] + head_ref[0:1])
    log_decay = -step * jnp.exp(head_ref[1:2])
    row, column = triangle(length)
    lower = jnp.where(row >= column, 1.0, 0.0)
    decay = dot(lower, log_decay, precision=HIGHEST)
    step_ref[...] = step
    decay_ref[...] = decay
    heads = head_map(width, head_dim)
    last = decay[length - 1 : length]
    tail = spread(jnp.exp(last - decay) * step, heads)
    lead = spread(jnp.exp(decay), heads)
    upstream = upstream_ref[...].astype(F32)
    forward = dot(mixer_act[:, :state], tail * inner_act, 0, 0, HIGHEST).astype(BF16)
    backward = dot(mixer_act[:, state:], lead * upstream, 0, 0, HIGHEST).astype(BF16)
    high, middle, low = pieces(last)
    kinds = (high.astype(F32), middle.astype(F32), low.astype(F32))
    index = lax.broadcasted_iota(jnp.int32, (PAD, LANES), 0)
    stacked = jnp.zeros((PAD, LANES), F32)
    for number, kind in enumerate(kinds):
        stacked = jnp.where(index == number, kind, stacked)
    extra = dot(stacked.astype(BF16), heads).astype(BF16)
    if relative:
        count = len(message_refs) + 1
        for hop, message_ref in enumerate(message_refs, 1):
            message_ref[:state] = jnp.where(place + hop < count, forward, backward)
            message_ref[state:] = extra
    else:
        message_ref = message_refs[0]
        for target in range(message_ref.shape[0]):
            message_ref[target, :state] = jnp.where(target > place, forward, backward)
            message_ref[target, state:] = extra


def within(
    head_dim,
    inner_pre_ref,
    mixer_pre_ref,
    step_ref,
    decay_ref,
    head_ref,
    upstream_ref,
    inner_grad_ref,
    mixer_grad_ref,
    row_ref,
    column_ref,
):
    length, width = inner_pre_ref.shape
    state = mixer_pre_ref.shape[1] // 2
    mixer_pre = mixer_pre_ref[...]
    mixer_act = mixer_pre * sigmoid(mixer_pre)
    input_mix = mixer_act[:, :state]
    output_mix = mixer_act[:, state:]
    decay = decay_ref[...]
    step = step_ref[...]
    turned = decay.T
    row, column = triangle(length)
    causal = column >= row
    scores = dot(input_mix, output_mix, 1, 1, HIGHEST)
    heads = head_map(width, head_dim)
    skip = spread(head_ref[...], heads)[2:3]
    step_wide = spread(step, heads)
    group_heads = LANES // head_dim
    lane = lax.broadcasted_iota(jnp.int32, (length, LANES), 1)
    mixed = jnp.zeros((length, length), F32)
    rows = jnp.zeros((length, LANES), F32)
    columns = []
    for group in range(width // LANES):
        span = slice(group * LANES, (group + 1) * LANES)
        inner_pre = inner_pre_ref[:, span]
        inner_act = inner_pre * sigmoid(inner_pre)
        high = inner_act.astype(BF16)
        low = (inner_act - high.astype(F32)).astype(BF16)
        upstream = upstream_ref[:, span]
        total = None
        for member in range(group_heads):
            head = group * group_heads + member
            mine = (lane >= member * head_dim) & (lane < (member + 1) * head_dim)
            mine_upstream = jnp.where(mine, upstream.astype(F32), 0.0).astype(BF16)
            spread_of = turned[head : head + 1] - decay[:, head : head + 1]
            fall = jnp.exp(jnp.where(causal, spread_of, -1e30))
            match = dot(high, mine_upstream, 1, 1) + dot(low, mine_upstream, 1, 1)
            weight = fall * scores
            cross = weight * match
            step_column = step[:, head : head + 1]
            mixed = mixed + step_column * (fall * match)
            rows = jnp.where(lane == head, jnp.sum(cross, axis=1, keepdims=True), rows)
            columns.append(jnp.sum(step_column * cross, axis=0, keepdims=True))
            weight_high = weight.astype(BF16)
            weight_low = (weight - weight_high.astype(F32)).astype(BF16)
            term = dot(weight_high, mine_upstream) + dot(weight_low, mine_upstream)
            total = term if total is None else total + term
        inner_grad_ref[:, span] = step_wide[:, span] * total + skip[:, span] * upstream.astype(F32)
    mixer_grad_ref[:, :state] = dot(mixed, output_mix, precision=HIGHEST)
    mixer_grad_ref[:, state:] = dot(mixed, input_mix, 0, 0, HIGHEST)
    row_ref[...] = rows
    index = lax.broadcasted_iota(jnp.int32, (LANES, length), 0)
    stacked = jnp.zeros((LANES, length), F32)
    for number, kind in enumerate(columns):
        stacked = jnp.where(index == number, kind, stacked)
    column_ref[...] = stacked


def finish(
    head_dim,
    relative,
    count,
    chan_count,
    place_ref,
    *refs,
):
    messages = refs[: count - 1] if relative else refs[:1]
    inner_scratch, mixer_scratch = refs[-2:]
    mixer_sent_refs = refs[-2 - chan_count : -2]
    refs = refs[len(messages) : -2 - chan_count]
    (
        inner_pre_ref,
        mixer_pre_ref,
        step_ref,
        decay_ref,
        raw_ref,
        head_ref,
        upstream_ref,
        conv_inner_ref,
        conv_mixer_ref,
        inner_grad_ref,
        mixer_grad_ref,
        row_ref,
        column_ref,
        pair_ref,
        mixer_out_ref,
        step_out_ref,
    ) = refs
    length, width = inner_pre_ref.shape
    state = mixer_pre_ref.shape[1] // 2
    place = place_ref[0]

    def message(hop):
        if relative:
            return messages[hop - 1][...].astype(F32)
        return messages[0][lax.rem(place - hop + count, count)].astype(F32)

    def shard_decay(parts):
        return parts[state : state + 1] + parts[state + 1 : state + 2] + parts[state + 2 : state + 3]

    start = jnp.zeros((state, width), F32)
    running = jnp.zeros((1, width), F32)
    end = jnp.zeros((state, width), F32)
    if relative:
        received = [None] + [message(hop) for hop in range(1, count)]
        back_running = jnp.zeros((1, width), F32)
        for hop in range(1, count):
            factor = jnp.where(hop <= place, jnp.exp(running), 0.0)
            start = start + factor * received[hop][:state]
            running = running + shard_decay(received[hop])
            other = count - hop
            factor = jnp.where(other > place, jnp.exp(back_running), 0.0)
            end = end + factor * received[other][:state]
            back_running = back_running + shard_decay(received[other])
    else:

        def before(hop, carried):
            start, running = carried
            parts = message(hop)
            return start + jnp.exp(running) * parts[:state], running + shard_decay(parts)

        def after(step, carried):
            end, running = carried
            parts = message(count - step)
            return end + jnp.exp(running) * parts[:state], running + shard_decay(parts)

        start, unused = lax.fori_loop(1, place + 1, before, (start, running))
        end, unused = lax.fori_loop(1, count - place, after, (end, running))

    inner_pre = inner_pre_ref[...]
    mixer_pre = mixer_pre_ref[...]
    inner_sig = sigmoid(inner_pre)
    mixer_sig = sigmoid(mixer_pre)
    inner_act = inner_pre * inner_sig
    mixer_act = mixer_pre * mixer_sig
    input_mix = mixer_act[:, :state]
    output_mix = mixer_act[:, state:]
    decay = decay_ref[...]
    step = step_ref[...]
    upstream = upstream_ref[...].astype(F32)
    heads = head_map(width, head_dim)
    last = decay[length - 1 : length]
    lead = jnp.exp(decay)
    rest = jnp.exp(last - decay)
    lead_wide = spread(lead, heads)
    tail_wide = spread(rest * step, heads)
    from_end = dot(input_mix, end, precision=HIGHEST)
    from_start = dot(output_mix, start, precision=HIGHEST)
    inner_grad = inner_grad_ref[...] + tail_wide * from_end
    input_grad = mixer_grad_ref[:, :state] + dot(tail_wide * inner_act, end, 1, 1, HIGHEST)
    output_grad = mixer_grad_ref[:, state:] + dot(lead_wide * upstream, start, 1, 1, HIGHEST)
    end_part = rest * collect(inner_act * from_end, heads)
    start_part = lead * collect(upstream * from_start, heads)
    product = jnp.sum(end * start, axis=0, keepdims=True)
    product = collect(jnp.broadcast_to(product, (PAD, width)), heads)[0:1]
    step_grad = row_ref[...] + end_part
    sums = start_part - step * step_grad
    total = jnp.sum(step * end_part, axis=0, keepdims=True) + jnp.exp(last) * product
    row, column = triangle(length)
    upper = jnp.where(column >= row, 1.0, 0.0)
    decay_grad = (
        dot(upper, sums, precision=HIGHEST) + dot(upper, column_ref[...], 1, 1, HIGHEST) + total
    )
    step_grad = step_grad - jnp.exp(head_ref[1:2]) * decay_grad
    raw_grad = step_grad * sigmoid(raw_ref[...] + head_ref[0:1])
    step_out_ref[...] = raw_grad.astype(BF16)
    turned = raw_grad.T
    groups = width // length
    packed = jnp.zeros((PAD, width), F32)
    index = lax.broadcasted_iota(jnp.int32, (PAD, width), 0)
    head_count = width // head_dim
    for number in range(-(-head_count // groups)):
        line = [turned[number * groups + group : number * groups + group + 1] for group in range(groups)]
        packed = jnp.where(index == number, jnp.concatenate(line, axis=1), packed)
    inner_slope = inner_sig * (1.0 + inner_pre * (1.0 - inner_sig))
    mixer_slope = mixer_sig * (1.0 + mixer_pre * (1.0 - mixer_sig))
    inner_total = convolve_back(inner_grad * inner_slope, conv_inner_ref[...], inner_scratch)
    mixer_total = jnp.concatenate([input_grad, output_grad], axis=1) * mixer_slope
    mixer_total = convolve_back(mixer_total, conv_mixer_ref[...], mixer_scratch)
    taps = conv_inner_ref.shape[0] - 1
    early = PAD - taps
    inner_scratch[:PAD] = jnp.where(index >= early, inner_total[:PAD], packed)
    mixed = 2 * state
    inner_scratch[early - taps : early, :mixed] = mixer_total[early:PAD]
    pair_ref[:length] = inner_total[PAD:].astype(BF16)
    pair_ref[length:] = inner_scratch[:PAD].astype(BF16)
    mixer_out_ref[...] = mixer_total[PAD:].astype(BF16)
    rows = length // chan_count
    back = mixer_total[:PAD].astype(BF16)
    mixer_scratch[:length] = mixer_total[PAD:]
    for hop, sent_ref in enumerate(mixer_sent_refs):
        target = lax.rem(place_ref[2] + hop, chan_count)
        start = pl.multiple_of(target * rows, rows)
        sent_ref[:rows] = mixer_scratch[pl.ds(start, rows)].astype(BF16)
        sent_ref[rows:] = back


def add_late(ending, extra, taps, valid):
    index = lax.broadcasted_iota(jnp.int32, ending.shape, 0)
    late = jnp.where((index >= PAD - taps) & valid, extra, 0.0)
    return ending + late


def project_back(
    taps,
    seq_count,
    place_ref,
    pair_ref,
    next_ref,
    mixer_ref,
    step_ref,
    inner_weight_ref,
    mixer_weight_ref,
    step_weight_ref,
    out_ref,
    inner_scratch,
    mixer_scratch,
):
    count, rows, _ = out_ref.shape
    length, mixed = mixer_ref.shape
    width = pair_ref.shape[1]
    valid = place_ref[0] < seq_count - 1
    extra = next_ref[length:].astype(F32)
    head = length - PAD
    inner_scratch[:head] = pair_ref[:head]
    ending = add_late(pair_ref[head:length].astype(F32), extra, taps, valid)
    inner_scratch[head:] = ending.astype(BF16)
    shifted = jnp.concatenate([extra[PAD - taps :, :mixed], extra[: PAD - taps, :mixed]], axis=0)
    mixer_scratch[:head] = mixer_ref[:head]
    ending = add_late(mixer_ref[head:].astype(F32), shifted, taps, valid)
    mixer_scratch[head:] = ending.astype(BF16)
    whole = width // (2 * LANES) * (2 * LANES)
    share = dot(inner_scratch[:, :whole], inner_weight_ref[:, :whole], 1, 1)
    left = jnp.concatenate([inner_scratch[:, whole:], step_ref[...]], axis=1)
    right = jnp.concatenate([inner_weight_ref[:, whole:], step_weight_ref[...]], axis=1)
    share = share + dot(left, right, 1, 1)
    share = share + dot(mixer_scratch[...], mixer_weight_ref[...], 1, 1)
    share = share.astype(BF16)
    for target in range(count):
        span = slice(target * rows, (target + 1) * rows)
        out_ref[target] = share[span]


def turn(relative, place_ref, *refs):
    column_refs, out_ref, columns = refs[:-2], refs[-2], refs[-1]
    seq_place = place_ref[0]
    chan_place = place_ref[2]
    chan_count = len(column_refs)
    seq_count, rows, _ = column_refs[0].shape
    length = chan_count * rows
    for hop in range(seq_count):
        source = lax.rem(seq_place - hop + seq_count, seq_count) if relative else hop
        for chan_hop in range(chan_count):
            chan_source = lax.rem(chan_place - chan_hop + chan_count, chan_count)
            start = pl.multiple_of(hop * length + chan_source * rows, rows)
            columns[pl.ds(start, rows)] = column_refs[chan_hop][source]
    out_ref[...] = columns[...].T


def arrange(relative, taps, place_ref, pair_refs, grads, steps):
    seq_place = place_ref[0]
    seq_count = len(pair_refs) if relative else pair_refs[0].shape[0]
    length = grads.shape[0] // seq_count

    def message(hop):
        return pair_refs[hop][...] if relative else pair_refs[0][hop]

    for hop in range(seq_count):
        if relative:
            shard = lax.rem(seq_place - hop + seq_count, seq_count)
            after = (hop - 1) % seq_count
        else:
            shard = hop
            after = (hop + 1) % seq_count
        pair = message(hop)
        start = hop * length
        head = length - PAD
        grads[start : start + head] = pair[:head]
        extra = message(after)[length:].astype(F32)
        ending = add_late(pair[head:length].astype(F32), extra, taps, shard < seq_count - 1)
        grads[start + head : start + length] = ending.astype(BF16)
        packed = pair[length:].astype(F32)
        groups = packed.shape[1] // length
        lines = [packed[:, group * length : (group + 1) * length] for group in range(groups)]
        steps[:, start : start + length] = jnp.concatenate(lines, axis=0).astype(BF16)


def leave(relative, taps, rows, scale, place_ref, *refs):
    turned_ref = refs[0]
    out_ref, grads, steps = refs[-3:]
    arrange(relative, taps, place_ref, refs[1:-3], grads, steps)
    padded = turned_ref.shape[0] // 2
    chosen = turned_ref[padded : padded + rows]
    out_ref[:rows] = (dot(chosen, grads[...]) * scale).astype(BF16)
    lines = steps.shape[0]
    term = dot(steps[...], turned_ref[padded:], 1, 1) * scale
    out_ref[rows:, :padded] = term.astype(BF16)
    out_ref[rows:, padded:] = jnp.zeros((lines, out_ref.shape[1] - padded), BF16)


def keep(rows, scale, turned_ref, grads_ref, steps_ref, out_ref, step_ref):
    padded = turned_ref.shape[0] // 2
    out_ref[...] = dot(turned_ref[:rows], grads_ref[...]) * scale
    step_ref[...] = dot(steps_ref[...], turned_ref[:padded], 1, 1) * scale


def mix(relative, taps, rows, scale, place_ref, *refs):
    column_ref, out_ref, columns, grads = refs[0], refs[-3], refs[-2], refs[-1]
    grad_refs = refs[1:-3]
    seq_place = place_ref[0]
    dp_place = place_ref[1]
    chan_place = place_ref[2]
    seq_count, tokens, wide = column_ref.shape
    chan_count = out_ref.shape[0] // 2

    def message(hop):
        return grad_refs[hop][...] if relative else grad_refs[0][hop]

    for hop in range(seq_count):
        if relative:
            source = lax.rem(seq_place - hop + seq_count, seq_count)
            after = (hop - 1) % seq_count
        else:
            source = hop
            after = (hop + 1) % seq_count
        start = hop * tokens
        head = tokens - PAD
        columns[start : start + tokens] = column_ref[source]
        block = message(hop)
        grads[start : start + head] = block[:head]
        valid = (source < seq_count - 1) & (chan_place == chan_count - 1)
        extra = message(after)[tokens:].astype(F32)
        ending = add_late(block[head:tokens].astype(F32), extra, taps, valid)
        grads[start + head : start + tokens] = ending.astype(BF16)
    padded = wide // 2
    term = (dot(columns[...], grads[...], 0, 0) * scale).astype(BF16)
    for hop in range(2):
        target = lax.rem(dp_place + hop, 2)
        for chan in range(chan_count):
            start = hop * padded + chan * rows
            out_ref[target * chan_count + chan] = term[start : start + rows]


def shape(*dims, dtype=F32):
    return pltpu.VMEM(dims, dtype)


def ring(axis, hop):
    count = lax.axis_size(axis)
    return [(source, (source + hop) % count) for source in range(count)]


def call(body, place, arrays, out_shape, scratch=(), cost=3, plain=()):
    vmem = pltpu.MemorySpace.VMEM
    hbm = pltpu.MemorySpace.HBM
    arrays = [
        pltpu.with_memory_space_constraint(array, hbm if number in plain else vmem)
        for number, array in enumerate(arrays)
    ]
    in_specs = [pl.BlockSpec(memory_space=pltpu.VMEM)] * len(arrays)
    if place is not None:
        in_specs = [pl.BlockSpec(memory_space=pltpu.SMEM)] + in_specs
        arrays = [place] + arrays
    return pl.pallas_call(
        body,
        out_shape=out_shape,
        in_specs=in_specs,
        out_specs=[pl.BlockSpec(memory_space=pltpu.VMEM)] * len(out_shape),
        scratch_shapes=list(scratch),
        cost_estimate=pl.CostEstimate(flops=cost * 10**8, bytes_accessed=0, transcendentals=0),
        compiler_params=pltpu.CompilerParams(vmem_limit_bytes=24 * 2**20),
    )(*arrays)


def around(block, axis):
    count = lax.axis_size(axis)
    return [block] + [
        lax.ppermute(block, axis, ring(axis, hop)) for hop in reversed(range(1, count))
    ][::-1]


def body(
    layer_input,
    inner_weight,
    mixer_weight,
    step_weight,
    conv_inner,
    conv_mixer,
    step_bias,
    decay_log,
    skip_gain,
    output_grad,
):
    own = layer_input[0]
    dp_count = lax.axis_size("dp")
    seq_count = lax.axis_size("seq")
    chan_count = lax.axis_size("chan")
    place = lax.axis_index("seq")
    relative = seq_count <= DIRECT
    rows, model = own.shape
    length = rows * chan_count
    width = inner_weight.shape[1]
    head_count = step_bias.shape[0]
    head_dim = width // head_count
    mixed = mixer_weight.shape[1]
    state = mixed // 2
    upstream = output_grad[0]
    grad_rows = model // (dp_count * seq_count)
    padded = -(-grad_rows // LANES) * LANES
    taps = conv_inner.shape[0] - 1
    places = [place, lax.axis_index("dp"), lax.axis_index("chan")]
    places = jnp.stack(places).astype(jnp.int32)
    norm_factor = 1.0 / math.sqrt(length * seq_count * dp_count)

    gathered = around(own, "chan")
    sorted_columns, head_rows, step_near, step_far = call(
        functools.partial(blocks, grad_rows, padded, dp_count),
        places,
        [own, step_weight.T, step_bias[None], decay_log[None], skip_gain[None]],
        [
            shape(seq_count, rows, dp_count * padded, dtype=BF16),
            shape(PAD, LANES),
            shape(model, LANES, dtype=BF16),
            jax.ShapeDtypeStruct((model, LANES), BF16),
        ],
        [pltpu.VMEM((LANES, model), F32)],
        cost=2,
    )
    columns = lax.all_to_all(sorted_columns, "seq", split_axis=0, concat_axis=0)
    inner_proj, mixer_proj, step_raw, tail = call(
        functools.partial(project, chan_count),
        places,
        gathered + [inner_weight, mixer_weight, step_near],
        [
            shape(length, width, dtype=BF16),
            shape(length, mixed, dtype=BF16),
            shape(length, LANES),
            shape(2 * PAD, width + mixed, dtype=BF16),
        ],
        [pltpu.VMEM((length, model), BF16)],
        cost=4,
    )
    forward_pairs = [(source, source + 1) for source in range(seq_count - 1)]
    history = lax.ppermute(tail, "seq", forward_pairs)

    if relative:
        message_shapes = [shape(state + PAD, width, dtype=BF16)] * (seq_count - 1)
    else:
        message_shapes = [shape(seq_count, state + PAD, width, dtype=BF16)]
    inner_pre, mixer_pre, step, decay, *messages = call(
        functools.partial(prepare, head_dim, relative),
        places,
        [inner_proj, mixer_proj, history, step_raw, head_rows, upstream, conv_inner, conv_mixer],
        [
            shape(length, width),
            shape(length, mixed),
            shape(length, LANES),
            shape(length, LANES),
        ]
        + message_shapes,
        [pltpu.VMEM((PAD + length, width), F32), pltpu.VMEM((PAD + length, mixed), F32)],
    )
    if relative:
        received = [
            lax.ppermute(message, "seq", ring("seq", hop))
            for hop, message in enumerate(messages, 1)
        ]
    else:
        received = [lax.all_to_all(messages[0], "seq", split_axis=0, concat_axis=0)]
    inner_part, mixer_part, row_part, column_part = call(
        functools.partial(within, head_dim),
        None,
        [inner_pre, mixer_pre, step, decay, head_rows, upstream],
        [shape(length, width), shape(length, mixed), shape(length, LANES), shape(LANES, length)],
    )
    all_columns = around(columns, "chan")
    (turned,) = call(
        functools.partial(turn, relative),
        places,
        all_columns,
        [shape(dp_count * padded, seq_count * length, dtype=BF16)],
        [pltpu.VMEM((seq_count * length, dp_count * padded), BF16)],
    )

    pair, mixer_local, step_grad, *mixer_sent = call(
        functools.partial(finish, head_dim, relative, seq_count, chan_count),
        places,
        received
        + [
            inner_pre,
            mixer_pre,
            step,
            decay,
            step_raw,
            head_rows,
            upstream,
            conv_inner,
            conv_mixer,
            inner_part,
            mixer_part,
            row_part,
            column_part,
        ],
        [
            shape(length + PAD, width, dtype=BF16),
            shape(length, mixed, dtype=BF16),
            shape(length, LANES, dtype=BF16),
        ]
        + [shape(rows + PAD, mixed, dtype=BF16)] * chan_count,
        [pltpu.VMEM((length + 2 * PAD, width), F32), pltpu.VMEM((length + 2 * PAD, mixed), F32)],
        cost=5,
    )

    def over_seq(block):
        if relative:
            return around(block, "seq")
        return [lax.all_gather(block, "seq")]

    pairs = over_seq(pair)
    if relative:
        following = pairs[-1]
    else:
        following = lax.rem(place + 1, seq_count)
        following = lax.dynamic_index_in_dim(pairs[0], following, 0, False)

    mixer_rows = mixer_sent[:1] + [
        lax.ppermute(block, "chan", ring("chan", hop))
        for hop, block in enumerate(mixer_sent[1:], 1)
    ]
    (mixer_rows,) = call(add_up, None, mixer_rows, [shape(rows + PAD, mixed, dtype=BF16)], cost=1)
    mixers = over_seq(mixer_rows)

    (sent,) = call(
        functools.partial(project_back, taps, seq_count),
        places,
        [pair, following, mixer_local, step_grad, inner_weight, mixer_weight, step_far],
        [shape(chan_count, rows, model, dtype=BF16)],
        [pltpu.VMEM((length, width), BF16), pltpu.VMEM((length, mixed), BF16)],
        cost=4,
        plain=(4, 5, 6),
    )
    taken = lax.all_to_all(sent, "chan", split_axis=0, concat_axis=0)

    groups = width // length
    step_lines = PAD * groups
    leaving, grads, steps = call(
        functools.partial(leave, relative, taps, grad_rows, norm_factor),
        places,
        [turned] + pairs,
        [
            shape(grad_rows + step_lines, width, dtype=BF16),
            shape(seq_count * length, width, dtype=BF16),
            shape(step_lines, seq_count * length, dtype=BF16),
        ],
    )
    arrived = lax.ppermute(leaving, "dp", ring("dp", 1))
    kept, kept_step = call(
        functools.partial(keep, grad_rows, norm_factor),
        None,
        [turned, grads, steps],
        [shape(grad_rows, width), shape(step_lines, padded)],
    )
    (mixer_blocks,) = call(
        functools.partial(mix, relative, taps, grad_rows // chan_count, norm_factor),
        places,
        [columns] + mixers,
        [shape(dp_count * chan_count, grad_rows // chan_count, mixed, dtype=BF16)],
        [
            pltpu.VMEM((seq_count * rows, dp_count * padded), BF16),
            pltpu.VMEM((seq_count * rows, mixed), BF16),
        ],
        cost=2,
    )
    taken, mixer_blocks = lax.optimization_barrier((taken, mixer_blocks))
    mixer_blocks = lax.all_to_all(
        mixer_blocks, ("dp", "chan"), split_axis=0, concat_axis=0
    )
    mixer_weight_grad = jnp.sum(mixer_blocks.astype(F32), axis=0)
    input_grad = jnp.sum(taken.astype(F32), axis=0).astype(BF16)
    inner_weight_grad = kept + arrived[:grad_rows].astype(F32)
    kept_step = kept_step[:, :grad_rows] + arrived[grad_rows:, :grad_rows].astype(F32)
    lines = [kept_step[(head % groups) * PAD + head // groups] for head in range(head_count)]
    step_weight_grad = jnp.stack(lines, axis=1)
    return (input_grad[None], inner_weight_grad, mixer_weight_grad, step_weight_grad)


def solution(mesh):
    in_specs = (
        P("dp", ("seq", "chan"), None),
        P(None, "chan"),
        P(),
        P(None, "chan"),
        P(None, "chan"),
        P(),
        P("chan"),
        P("chan"),
        P("chan"),
        P("dp", "seq", "chan"),
    )
    out_specs = (
        P("dp", ("seq", "chan"), None),
        P(("dp", "seq"), "chan"),
        P(("dp", "seq", "chan"), None),
        P(("dp", "seq"), "chan"),
    )
    return jax.shard_map(body, mesh=mesh, in_specs=in_specs, out_specs=out_specs, check_vma=False)
```

```python
import functools
import math

import jax
import jax.numpy as jnp
from jax import lax
from jax.experimental import pallas as pl
from jax.experimental.pallas import tpu as pltpu
from jax.sharding import PartitionSpec as P


F32 = jnp.float32
BF16 = jnp.bfloat16
LANES = 128
PAD = 8
DIRECT = 8


def dot(left, right, left_dim=1, right_dim=0):
    return lax.dot_general(
        left,
        right,
        (((left_dim,), (right_dim,)), ((), ())),
        preferred_element_type=F32,
    )


def pieces(values):
    high = values.astype(BF16)
    rest = values - high.astype(F32)
    middle = rest.astype(BF16)
    low = (rest - middle.astype(F32)).astype(BF16)
    return high, middle, low


def fine(left, right, left_dim=1, right_dim=0):
    left_high = left.astype(BF16)
    left_low = (left - left_high.astype(F32)).astype(BF16)
    right_high = right.astype(BF16)
    right_low = (right - right_high.astype(F32)).astype(BF16)
    lefts = jnp.concatenate([left_high, left_low, left_high], axis=left_dim)
    rights = jnp.concatenate([right_high, right_high, right_low], axis=right_dim)
    return dot(lefts, rights, left_dim, right_dim)


def masked_sum(mask, values, values_dim=0):
    chosen = jnp.where(mask, 1.0, 0.0).astype(BF16)
    masks = jnp.concatenate([chosen] * 3, axis=1)
    return dot(masks, jnp.concatenate(pieces(values), axis=values_dim), 1, values_dim)


def head_map(width, head_dim):
    row = lax.broadcasted_iota(jnp.int32, (LANES, width), 0)
    column = lax.broadcasted_iota(jnp.int32, (LANES, width), 1)
    start = row * head_dim
    return jnp.where((column >= start) & (column < start + head_dim), 1.0, 0.0).astype(BF16)


def spread(values, heads):
    return dot(jnp.concatenate(pieces(values), axis=1), jnp.concatenate([heads] * 3, axis=0))


def collect(values, heads):
    high, middle, _ = pieces(values)
    return dot(high, heads, 1, 1) + dot(middle, heads, 1, 1)


def sigmoid(values):
    return 1.0 / (1.0 + jnp.exp(-values))


def softplus(values):
    small = jnp.exp(-jnp.abs(values))
    series = small * (1.0 - small * (0.5 - small * (1.0 / 3.0)))
    return jnp.maximum(values, 0.0) + jnp.where(small < 1e-3, series, jnp.log(1.0 + small))


def triangle(length):
    row = lax.broadcasted_iota(jnp.int32, (length, length), 0)
    column = lax.broadcasted_iota(jnp.int32, (length, length), 1)
    return row, column


def convolve(values, history, kernel, scratch):
    length = values.shape[0]
    taps = kernel.shape[0]
    scratch[:PAD] = history.astype(F32)
    scratch[PAD:] = values.astype(F32)
    total = kernel[taps - 1 : taps] * scratch[PAD : PAD + length]
    for tap in range(taps - 1):
        start = PAD - (taps - 1) + tap
        total = total + kernel[tap : tap + 1] * scratch[start : start + length]
    return total


def convolve_back(gradient, kernel, scratch):
    length = gradient.shape[0]
    taps = kernel.shape[0]
    zeros = jnp.zeros((PAD, gradient.shape[1]), F32)
    scratch[:PAD] = zeros
    scratch[PAD : PAD + length] = gradient
    scratch[PAD + length :] = zeros
    extent = length + PAD
    total = None
    for tap in range(taps):
        start = taps - 1 - tap
        term = kernel[tap : tap + 1] * scratch[start : start + extent]
        total = term if total is None else total + term
    return total


def blocks(rows, padded, dp_count, relative, place_ref, *refs):
    own_ref, step_ref, bias_ref, log_ref, skip_ref, inner_ref, mixer_ref = refs[:7]
    own_out_ref, step_out_ref, head_ref, inner_out_ref, mixer_out_ref = refs[7:12]
    out_refs, scratch, wide, sems = refs[12:-3], refs[-3], refs[-2], refs[-1]
    parts = sems.shape[1]
    depth = inner_ref.shape[0] // parts
    copies = []
    for part in range(parts):
        span = pl.ds(part * depth, depth)
        pair = ((inner_ref, inner_out_ref), (mixer_ref, mixer_out_ref))
        for number, (source, target) in enumerate(pair):
            copy = pltpu.make_async_copy(source.at[span], target.at[span], sems.at[number, part])
            copy.start()
            copies.append(copy)
    own_out_ref[...] = own_ref[...]
    head_count = bias_ref.shape[1]
    wide[...] = jnp.zeros_like(wide)
    wide[:head_count] = step_ref[...].astype(F32)
    step_out_ref[...] = wide[...].T.astype(BF16)
    head_ref[...] = jnp.zeros_like(head_ref)
    head_ref[0:1, :head_count] = bias_ref[...]
    head_ref[1:2, :head_count] = log_ref[...]
    head_ref[2:3, :head_count] = skip_ref[...]
    dp_place = place_ref[1]
    seq_count = scratch.shape[0]
    fill = jnp.zeros((own_ref.shape[0], padded - rows), F32)
    for target in range(seq_count):
        for hop in range(dp_count):
            wanted = lax.rem(dp_place + hop, dp_count)
            chosen = None
            for other in range(dp_count):
                start = (other * seq_count + target) * rows
                part = own_ref[:, start : start + rows].astype(F32)
                chosen = part if chosen is None else jnp.where(wanted == other, part, chosen)
            span = slice(hop * padded, (hop + 1) * padded)
            if padded > rows:
                chosen = jnp.concatenate([chosen, fill], axis=1)
            scratch[target, :, span] = chosen.astype(BF16)
    if relative:
        for hop, out_ref in enumerate(out_refs):
            out_ref[...] = scratch[lax.rem(place_ref[0] + hop, seq_count)]
    else:
        out_refs[0][...] = scratch[...]
    for copy in copies:
        copy.wait()


def copied(sources, targets, sems):
    copies = [
        pltpu.make_async_copy(source, target, sems.at[number])
        for number, (source, target) in enumerate(zip(sources, targets))
    ]
    for copy in copies:
        copy.start()
    return copies


def add_parts(parts_ref, out_ref):
    total = parts_ref[0].astype(F32)
    for part in range(1, parts_ref.shape[0]):
        total = total + parts_ref[part].astype(F32)
    out_ref[...] = total.astype(out_ref.dtype)


def pack(*refs):
    for number, ref in enumerate(refs[:-1]):
        refs[-1][number] = ref[...]


def add_up(*refs):
    total = refs[0][...].astype(F32)
    for part in refs[1:-1]:
        total = total + part[...].astype(F32)
    refs[-1][...] = total.astype(refs[-1].dtype)


def project(count, place_ref, *refs):
    tokens = refs[:count]
    inner_ref, mixer_ref, step_ref, inner_out, mixer_out, raw_out, tail_out, scratch = refs[count:]
    place = place_ref[2]
    rows = tokens[0].shape[0]
    for hop in range(count):
        source = lax.bitwise_xor(place, hop)
        scratch[pl.ds(pl.multiple_of(source * rows, rows), rows)] = tokens[hop][...]
    gathered = scratch[...]
    length = gathered.shape[0]
    width = inner_ref.shape[1]
    whole = width // (2 * LANES) * (2 * LANES)
    mixer = dot(gathered, mixer_ref[...]).astype(BF16)
    first = dot(gathered, inner_ref[:, :whole])
    joined = jnp.concatenate([inner_ref[:, whole:], step_ref[...]], axis=1)
    second = dot(gathered, joined)
    raw_out[...] = second[:, width - whole :]
    inner = jnp.concatenate([first, second[:, : width - whole]], axis=1).astype(BF16)
    inner_out[...] = inner
    mixer_out[...] = mixer
    tail_out[:, :width] = inner[length - 2 * PAD :]
    tail_out[:, width:] = mixer[length - 2 * PAD :]


def prepare(head_dim, relative, place_ref, *refs):
    (
        inner_ref,
        mixer_ref,
        history_ref,
        raw_ref,
        head_ref,
        upstream_ref,
        conv_inner_ref,
        conv_mixer_ref,
        inner_pre_ref,
        mixer_pre_ref,
        step_ref,
        decay_ref,
    ) = refs[:12]
    message_refs = refs[12:-2]
    inner_scratch, mixer_scratch = refs[-2:]
    length, width = inner_ref.shape
    state = mixer_ref.shape[1] // 2
    place = place_ref[0]
    history = history_ref[...].astype(F32)[PAD:]
    inner_pre = convolve(inner_ref[...], history[:, :width], conv_inner_ref[...], inner_scratch)
    mixer_pre = convolve(mixer_ref[...], history[:, width:], conv_mixer_ref[...], mixer_scratch)
    inner_pre_ref[...] = inner_pre
    mixer_pre_ref[...] = mixer_pre
    inner_act = inner_pre * sigmoid(inner_pre)
    mixer_act = mixer_pre * sigmoid(mixer_pre)
    step = softplus(raw_ref[...] + head_ref[0:1])
    log_decay = -step * jnp.exp(head_ref[1:2])
    row, column = triangle(length)
    decay = masked_sum(row >= column, log_decay)
    step_ref[...] = step
    decay_ref[...] = decay
    heads = head_map(width, head_dim)
    last = decay[length - 1 : length]
    tail = spread(jnp.exp(last - decay) * step, heads)
    lead = spread(jnp.exp(decay), heads)
    upstream = upstream_ref[...].astype(F32)
    forward = fine(mixer_act[:, :state].T, tail * inner_act).astype(BF16)
    backward = fine(mixer_act[:, state:].T, lead * upstream).astype(BF16)
    high, middle, low = pieces(last)
    kinds = (high.astype(F32), middle.astype(F32), low.astype(F32))
    index = lax.broadcasted_iota(jnp.int32, (PAD, LANES), 0)
    stacked = jnp.zeros((PAD, LANES), F32)
    for number, kind in enumerate(kinds):
        stacked = jnp.where(index == number, kind, stacked)
    extra = dot(stacked.astype(BF16), heads).astype(BF16)
    if relative:
        count = len(message_refs) + 1
        for hop, message_ref in enumerate(message_refs, 1):
            message_ref[:state] = jnp.where(place + hop < count, forward, backward)
            message_ref[state:] = extra
    else:
        message_ref = message_refs[0]
        for target in range(message_ref.shape[0]):
            message_ref[target, :state] = jnp.where(target > place, forward, backward)
            message_ref[target, state:] = extra


def within(
    head_dim,
    inner_pre_ref,
    mixer_pre_ref,
    step_ref,
    decay_ref,
    head_ref,
    upstream_ref,
    inner_weight_ref,
    mixer_weight_ref,
    inner_grad_ref,
    mixer_grad_ref,
    row_ref,
    column_ref,
    inner_near_ref,
    mixer_near_ref,
    sems,
):
    copies = copied(
        (inner_weight_ref, mixer_weight_ref), (inner_near_ref, mixer_near_ref), sems
    )
    length, width = inner_pre_ref.shape
    state = mixer_pre_ref.shape[1] // 2
    mixer_pre = mixer_pre_ref[...]
    mixer_act = mixer_pre * sigmoid(mixer_pre)
    input_mix = mixer_act[:, :state]
    output_mix = mixer_act[:, state:]
    decay = decay_ref[...]
    step = step_ref[...]
    turned = decay.T
    row, column = triangle(length)
    causal = column >= row
    scores = fine(input_mix, output_mix, 1, 1)
    heads = head_map(width, head_dim)
    skip = spread(head_ref[...], heads)[2:3]
    step_wide = spread(step, heads)
    group_heads = LANES // head_dim
    lane = lax.broadcasted_iota(jnp.int32, (length, LANES), 1)
    mixed = jnp.zeros((length, length), F32)
    rows = jnp.zeros((length, LANES), F32)
    columns = []
    for group in range(width // LANES):
        span = slice(group * LANES, (group + 1) * LANES)
        inner_pre = inner_pre_ref[:, span]
        inner_act = inner_pre * sigmoid(inner_pre)
        high = inner_act.astype(BF16)
        low = (inner_act - high.astype(F32)).astype(BF16)
        upstream = upstream_ref[:, span]
        total = None
        for member in range(group_heads):
            head = group * group_heads + member
            mine = (lane >= member * head_dim) & (lane < (member + 1) * head_dim)
            mine_upstream = jnp.where(mine, upstream.astype(F32), 0.0).astype(BF16)
            spread_of = turned[head : head + 1] - decay[:, head : head + 1]
            fall = jnp.exp(jnp.where(causal, spread_of, -1e30))
            match = dot(high, mine_upstream, 1, 1) + dot(low, mine_upstream, 1, 1)
            weight = fall * scores
            cross = weight * match
            step_column = step[:, head : head + 1]
            mixed = mixed + step_column * (fall * match)
            rows = jnp.where(lane == head, jnp.sum(cross, axis=1, keepdims=True), rows)
            columns.append(jnp.sum(step_column * cross, axis=0, keepdims=True))
            weight_high = weight.astype(BF16)
            weight_low = (weight - weight_high.astype(F32)).astype(BF16)
            term = dot(weight_high, mine_upstream) + dot(weight_low, mine_upstream)
            total = term if total is None else total + term
        inner_grad_ref[:, span] = step_wide[:, span] * total + skip[:, span] * upstream.astype(F32)
    mixer_grad_ref[:, :state] = fine(mixed, output_mix)
    mixer_grad_ref[:, state:] = fine(mixed.T, input_mix)
    row_ref[...] = rows
    index = lax.broadcasted_iota(jnp.int32, (LANES, length), 0)
    stacked = jnp.zeros((LANES, length), F32)
    for number, kind in enumerate(columns):
        stacked = jnp.where(index == number, kind, stacked)
    column_ref[...] = stacked
    for copy in copies:
        copy.wait()


def finish(
    head_dim,
    relative,
    count,
    chan_count,
    place_ref,
    *refs,
):
    messages = refs[: count - 1] if relative else refs[:1]
    inner_scratch, mixer_scratch = refs[-2:]
    mixer_sent_refs = refs[-2 - chan_count : -2]
    refs = refs[len(messages) : -2 - chan_count]
    (
        inner_pre_ref,
        mixer_pre_ref,
        step_ref,
        decay_ref,
        raw_ref,
        head_ref,
        upstream_ref,
        conv_inner_ref,
        conv_mixer_ref,
        inner_grad_ref,
        mixer_grad_ref,
        row_ref,
        column_ref,
        pair_ref,
        mixer_out_ref,
        step_out_ref,
        early_ref,
    ) = refs
    length, width = inner_pre_ref.shape
    state = mixer_pre_ref.shape[1] // 2
    place = place_ref[0]

    def message(hop):
        if relative:
            return messages[hop - 1][...].astype(F32)
        return messages[0][lax.rem(place - hop + count, count)].astype(F32)

    def shard_decay(parts):
        return parts[state : state + 1] + parts[state + 1 : state + 2] + parts[state + 2 : state + 3]

    start = jnp.zeros((state, width), F32)
    running = jnp.zeros((1, width), F32)
    end = jnp.zeros((state, width), F32)
    if relative:
        received = [None] + [message(hop) for hop in range(1, count)]
        back_running = jnp.zeros((1, width), F32)
        for hop in range(1, count):
            factor = jnp.where(hop <= place, jnp.exp(running), 0.0)
            start = start + factor * received[hop][:state]
            running = running + shard_decay(received[hop])
            other = count - hop
            factor = jnp.where(other > place, jnp.exp(back_running), 0.0)
            end = end + factor * received[other][:state]
            back_running = back_running + shard_decay(received[other])
    else:

        def before(hop, carried):
            start, running = carried
            parts = message(hop)
            return start + jnp.exp(running) * parts[:state], running + shard_decay(parts)

        def after(step, carried):
            end, running = carried
            parts = message(count - step)
            return end + jnp.exp(running) * parts[:state], running + shard_decay(parts)

        start, unused = lax.fori_loop(1, place + 1, before, (start, running))
        end, unused = lax.fori_loop(1, count - place, after, (end, running))

    inner_pre = inner_pre_ref[...]
    mixer_pre = mixer_pre_ref[...]
    inner_sig = sigmoid(inner_pre)
    mixer_sig = sigmoid(mixer_pre)
    inner_act = inner_pre * inner_sig
    mixer_act = mixer_pre * mixer_sig
    input_mix = mixer_act[:, :state]
    output_mix = mixer_act[:, state:]
    decay = decay_ref[...]
    step = step_ref[...]
    upstream = upstream_ref[...].astype(F32)
    heads = head_map(width, head_dim)
    last = decay[length - 1 : length]
    lead = jnp.exp(decay)
    rest = jnp.exp(last - decay)
    lead_wide = spread(lead, heads)
    tail_wide = spread(rest * step, heads)
    from_end = fine(input_mix, end)
    from_start = fine(output_mix, start)
    inner_grad = inner_grad_ref[...] + tail_wide * from_end
    input_grad = mixer_grad_ref[:, :state] + fine(tail_wide * inner_act, end, 1, 1)
    output_grad = mixer_grad_ref[:, state:] + fine(lead_wide * upstream, start, 1, 1)
    end_part = rest * collect(inner_act * from_end, heads)
    start_part = lead * collect(upstream * from_start, heads)
    product = jnp.sum(end * start, axis=0, keepdims=True)
    product = collect(jnp.broadcast_to(product, (PAD, width)), heads)[0:1]
    step_grad = row_ref[...] + end_part
    sums = start_part - step * step_grad
    total = jnp.sum(step * end_part, axis=0, keepdims=True) + jnp.exp(last) * product
    row, column = triangle(length)
    after_row = column >= row
    decay_grad = masked_sum(after_row, sums) + masked_sum(after_row, column_ref[...], 1) + total
    step_grad = step_grad - jnp.exp(head_ref[1:2]) * decay_grad
    raw_grad = step_grad * sigmoid(raw_ref[...] + head_ref[0:1])
    step_out_ref[...] = raw_grad.astype(BF16)
    turned = raw_grad.T
    groups = width // length
    packed = jnp.zeros((PAD, width), F32)
    index = lax.broadcasted_iota(jnp.int32, (PAD, width), 0)
    head_count = width // head_dim
    for number in range(-(-head_count // groups)):
        line = [turned[number * groups + group : number * groups + group + 1] for group in range(groups)]
        packed = jnp.where(index == number, jnp.concatenate(line, axis=1), packed)
    inner_slope = inner_sig * (1.0 + inner_pre * (1.0 - inner_sig))
    mixer_slope = mixer_sig * (1.0 + mixer_pre * (1.0 - mixer_sig))
    inner_total = convolve_back(inner_grad * inner_slope, conv_inner_ref[...], inner_scratch)
    mixer_total = jnp.concatenate([input_grad, output_grad], axis=1) * mixer_slope
    mixer_total = convolve_back(mixer_total, conv_mixer_ref[...], mixer_scratch)
    taps = conv_inner_ref.shape[0] - 1
    early = PAD - taps
    inner_scratch[:PAD] = jnp.where(index >= early, inner_total[:PAD], packed)
    early_ref[:, :width] = inner_total[:PAD]
    early_ref[:, width:] = mixer_total[:PAD]
    pair_ref[:length] = inner_total[PAD:].astype(BF16)
    pair_ref[length:] = inner_scratch[:PAD].astype(BF16)
    mixer_out_ref[...] = mixer_total[PAD:].astype(BF16)
    rows = length // chan_count
    back = mixer_total[:PAD].astype(BF16)
    mixer_scratch[:length] = mixer_total[PAD:]
    for hop, sent_ref in enumerate(mixer_sent_refs):
        target = lax.rem(place_ref[2] + hop, chan_count)
        start = pl.multiple_of(target * rows, rows)
        sent_ref[:rows] = mixer_scratch[pl.ds(start, rows)].astype(BF16)
        sent_ref[rows:] = back


def add_late(ending, extra, taps, valid):
    index = lax.broadcasted_iota(jnp.int32, ending.shape, 0)
    late = jnp.where((index >= PAD - taps) & valid, extra, 0.0)
    return ending + late


def project_back(
    pair_ref,
    late_ref,
    mixer_ref,
    step_ref,
    inner_weight_ref,
    mixer_weight_ref,
    step_weight_ref,
    out_ref,
    inner_scratch,
    mixer_scratch,
):
    count, rows, _ = out_ref.shape
    length, _ = mixer_ref.shape
    width = pair_ref.shape[1]
    head = length - PAD
    whole = width // (2 * LANES) * (2 * LANES)

    late = late_ref[...]
    inner_scratch[:head, :width] = pair_ref[:head]
    ending = pair_ref[head:length].astype(F32) + late[:, :width]
    inner_scratch[head:, :width] = ending.astype(BF16)
    inner_scratch[:, width:] = step_ref[...]
    mixer_scratch[:head] = mixer_ref[:head]
    ending = mixer_ref[head:].astype(F32) + late[:, width:]
    mixer_scratch[head:] = ending.astype(BF16)
    share = dot(inner_scratch[:, :whole], inner_weight_ref[:, :whole], 1, 1)
    right = jnp.concatenate([inner_weight_ref[:, whole:], step_weight_ref[...]], axis=1)
    share = share + dot(inner_scratch[:, whole:], right, 1, 1)
    share = share + dot(mixer_scratch[...], mixer_weight_ref[...], 1, 1)
    share = share.astype(BF16)
    for target in range(count):
        span = slice(target * rows, (target + 1) * rows)
        out_ref[target] = share[span]


def turn(place_ref, *refs):
    column_refs, out_ref, columns = refs[:-2], refs[-2], refs[-1]
    chan_place = place_ref[2]
    chan_count = len(column_refs)
    seq_count, rows, _ = column_refs[0].shape
    length = chan_count * rows
    for hop in range(seq_count):
        for chan_hop in range(chan_count):
            chan_source = lax.rem(chan_place - chan_hop + chan_count, chan_count)
            start = pl.multiple_of(hop * length + chan_source * rows, rows)
            columns[pl.ds(start, rows)] = column_refs[chan_hop][hop]
    out_ref[...] = columns[...].T


def arrange(relative, taps, used, place_ref, pair_refs, grads, steps):
    seq_place = place_ref[0]
    seq_count = len(pair_refs) if relative else pair_refs[0].shape[0]
    length = grads.shape[0] // seq_count

    def message(hop):
        return pair_refs[hop][...] if relative else pair_refs[0][hop]

    for hop in range(seq_count):
        if relative:
            shard = lax.rem(seq_place - hop + seq_count, seq_count)
            after = (hop - 1) % seq_count
        else:
            shard = hop
            after = (hop + 1) % seq_count
        pair = message(hop)
        start = hop * length
        head = length - PAD
        grads[start : start + head] = pair[:head]
        extra = message(after)[length:].astype(F32)
        ending = add_late(pair[head:length].astype(F32), extra, taps, shard < seq_count - 1)
        grads[start + head : start + length] = ending.astype(BF16)
        packed = pair[length:].astype(F32)
        groups = packed.shape[1] // length
        lines = [packed[:used, group * length : (group + 1) * length] for group in range(groups)]
        spare = steps.shape[0] - used * groups
        lines = lines + [jnp.zeros((spare, length), F32)]
        steps[:, start : start + length] = jnp.concatenate(lines, axis=0).astype(BF16)


def leave(relative, taps, used, rows, scale, place_ref, *refs):
    turned_ref = refs[0]
    out_ref, grads, steps = refs[-3:]
    arrange(relative, taps, used, place_ref, refs[1:-3], grads, steps)
    padded = turned_ref.shape[0] // 2
    chosen = turned_ref[padded : padded + rows]
    out_ref[:rows] = (dot(chosen, grads[...]) * scale).astype(BF16)
    lines = steps.shape[0]
    term = dot(steps[...], turned_ref[padded:], 1, 1) * scale
    out_ref[rows:, :padded] = term.astype(BF16)
    out_ref[rows:, padded:] = jnp.zeros((lines, out_ref.shape[1] - padded), BF16)


def keep(rows, scale, turned_ref, grads_ref, steps_ref, out_ref, step_ref):
    padded = turned_ref.shape[0] // 2
    out_ref[...] = dot(turned_ref[:rows], grads_ref[...]) * scale
    step_ref[...] = dot(steps_ref[...], turned_ref[:padded], 1, 1) * scale


def last(used, kept_ref, step_ref, arrived_ref, out_ref, step_out_ref):
    rows, _ = kept_ref.shape
    out_ref[...] = kept_ref[...] + arrived_ref[:rows].astype(F32)
    step = step_ref[:, :rows] + arrived_ref[rows:, :rows].astype(F32)
    head_count = step_out_ref.shape[0]
    groups = -(-head_count // used)
    for head in range(head_count):
        line = (head % groups) * used + head // groups
        step_out_ref[head : head + 1] = step[line : line + 1]


def mix(relative, taps, rows, scale, place_ref, *refs):
    column_ref, out_ref, columns, grads = refs[0], refs[-3], refs[-2], refs[-1]
    grad_refs = refs[1:-3]
    seq_place = place_ref[0]
    dp_place = place_ref[1]
    chan_place = place_ref[2]
    seq_count, tokens, wide = column_ref.shape
    chan_count = out_ref.shape[0] // 2

    def message(hop):
        return grad_refs[hop][...] if relative else grad_refs[0][hop]

    for hop in range(seq_count):
        if relative:
            source = lax.rem(seq_place - hop + seq_count, seq_count)
            after = (hop - 1) % seq_count
        else:
            source = hop
            after = (hop + 1) % seq_count
        start = hop * tokens
        head = tokens - PAD
        columns[start : start + tokens] = column_ref[hop]
        block = message(hop)
        grads[start : start + head] = block[:head]
        valid = (source < seq_count - 1) & (chan_place == chan_count - 1)
        extra = message(after)[tokens:].astype(F32)
        ending = add_late(block[head:tokens].astype(F32), extra, taps, valid)
        grads[start + head : start + tokens] = ending.astype(BF16)
    padded = wide // 2
    term = (dot(columns[...], grads[...], 0, 0) * scale).astype(BF16)
    for hop in range(2):
        target = lax.rem(dp_place + hop, 2)
        for chan in range(chan_count):
            start = hop * padded + chan * rows
            out_ref[target * chan_count + chan] = term[start : start + rows]


def shape(*dims, dtype=F32):
    return pltpu.VMEM(dims, dtype)


def ring(axis, hop):
    count = lax.axis_size(axis)
    return [(source, (source + hop) % count) for source in range(count)]


def call(body, place, arrays, out_shape, scratch=(), cost=3, plain=(), left=()):
    vmem = pltpu.MemorySpace.VMEM
    hbm = pltpu.MemorySpace.HBM
    arrays = [
        pltpu.with_memory_space_constraint(array, hbm if number in plain else vmem)
        for number, array in enumerate(arrays)
    ]
    in_specs = [
        pl.BlockSpec(memory_space=hbm if number in left else vmem) for number in range(len(arrays))
    ]
    out_specs = [pl.BlockSpec(memory_space=vmem)] * len(out_shape)
    if place is not None:
        in_specs = [pl.BlockSpec(memory_space=pltpu.SMEM)] + in_specs
        arrays = [place] + arrays
    return pl.pallas_call(
        body,
        out_shape=out_shape,
        in_specs=in_specs,
        out_specs=out_specs,
        scratch_shapes=list(scratch),
        cost_estimate=pl.CostEstimate(flops=cost * 10**8, bytes_accessed=0, transcendentals=0),
        compiler_params=pltpu.CompilerParams(vmem_limit_bytes=24 * 2**20),
    )(*arrays)


def around(block, axis):
    count = lax.axis_size(axis)
    return [block] + [
        lax.ppermute(block, axis, ring(axis, hop)) for hop in range(1, count)
    ]


def spread_out(block, axis):
    count = lax.axis_size(axis)
    parts = {0: block}
    bit = count // 2
    while bit:
        pairs = [(source, source ^ bit) for source in range(count)]
        for number in list(parts):
            parts[number | bit] = lax.ppermute(parts[number], axis, pairs)
        bit //= 2
    return [parts[number] for number in range(count)]


def body(
    layer_input,
    inner_weight,
    mixer_weight,
    step_weight,
    conv_inner,
    conv_mixer,
    step_bias,
    decay_log,
    skip_gain,
    output_grad,
):
    own = layer_input[0]
    dp_count = lax.axis_size("dp")
    seq_count = lax.axis_size("seq")
    chan_count = lax.axis_size("chan")
    place = lax.axis_index("seq")
    relative = seq_count <= DIRECT
    rows, model = own.shape
    length = rows * chan_count
    width = inner_weight.shape[1]
    head_count = step_bias.shape[0]
    head_dim = width // head_count
    mixed = mixer_weight.shape[1]
    state = mixed // 2
    upstream = output_grad[0]
    grad_rows = model // (dp_count * seq_count)
    padded = -(-grad_rows // LANES) * LANES
    taps = conv_inner.shape[0] - 1
    parts = next(count for count in (4, 2, 1) if model % (count * LANES) == 0)
    places = [place, lax.axis_index("dp"), lax.axis_index("chan")]
    places = jnp.stack(places).astype(jnp.int32)
    norm_factor = 1.0 / math.sqrt(length * seq_count * dp_count)

    gathered = spread_out(own, "chan")
    if relative:
        column_shapes = [shape(rows, dp_count * padded, dtype=BF16)] * seq_count
    else:
        column_shapes = [shape(seq_count, rows, dp_count * padded, dtype=BF16)]
    own_near, step_near, head_rows, inner_near, mixer_near, *sorted_columns = call(
        functools.partial(blocks, grad_rows, padded, dp_count, relative),
        places,
        [
            own,
            step_weight.T,
            step_bias[None],
            decay_log[None],
            skip_gain[None],
            inner_weight,
            mixer_weight,
        ],
        [
            shape(rows, model, dtype=BF16),
            shape(model, LANES, dtype=BF16),
            shape(PAD, LANES),
            shape(model, width, dtype=BF16),
            shape(model, mixed, dtype=BF16),
        ]
        + column_shapes,
        [
            pltpu.VMEM((seq_count, rows, dp_count * padded), BF16),
            pltpu.VMEM((LANES, model), F32),
            pltpu.SemaphoreType.DMA((2, parts)),
        ],
        cost=1,
        plain=range(7),
        left=(5, 6),
    )
    if relative:
        columns = [sorted_columns[0]]
        for hop, block in enumerate(sorted_columns[1:], 1):
            columns.append(lax.ppermute(block, "seq", ring("seq", hop)))
    else:
        columns = lax.all_to_all(sorted_columns[0], "seq", split_axis=0, concat_axis=0)
    inner_proj, mixer_proj, step_raw, tail = call(
        functools.partial(project, chan_count),
        places,
        [own_near] + gathered[1:] + [inner_near, mixer_near, step_near],
        [
            shape(length, width, dtype=BF16),
            shape(length, mixed, dtype=BF16),
            shape(length, LANES),
            shape(2 * PAD, width + mixed, dtype=BF16),
        ],
        [pltpu.VMEM((length, model), BF16)],
        cost=4,
    )
    forward_pairs = [(source, source + 1) for source in range(seq_count - 1)]
    history = lax.ppermute(tail, "seq", forward_pairs)

    if relative:
        message_shapes = [shape(state + PAD, width, dtype=BF16)] * (seq_count - 1)
    else:
        message_shapes = [shape(seq_count, state + PAD, width, dtype=BF16)]
    inner_pre, mixer_pre, step, decay, *messages = call(
        functools.partial(prepare, head_dim, relative),
        places,
        [inner_proj, mixer_proj, history, step_raw, head_rows, upstream, conv_inner, conv_mixer],
        [
            shape(length, width),
            shape(length, mixed),
            shape(length, LANES),
            shape(length, LANES),
        ]
        + message_shapes,
        [pltpu.VMEM((PAD + length, width), F32), pltpu.VMEM((PAD + length, mixed), F32)],
    )
    if relative:
        received = [
            lax.ppermute(message, "seq", ring("seq", hop))
            for hop, message in enumerate(messages, 1)
        ]
    else:
        received = [lax.all_to_all(messages[0], "seq", split_axis=0, concat_axis=0)]
    inner_part, mixer_part, row_part, column_part, inner_back, mixer_back = call(
        functools.partial(within, head_dim),
        None,
        [
            inner_pre,
            mixer_pre,
            step,
            decay,
            head_rows,
            upstream,
            inner_weight,
            mixer_weight,
        ],
        [
            shape(length, width),
            shape(length, mixed),
            shape(length, LANES),
            shape(LANES, length),
            shape(model, width, dtype=BF16),
            shape(model, mixed, dtype=BF16),
        ],
        [pltpu.SemaphoreType.DMA((2,))],
        plain=(6, 7),
        left=(6, 7),
    )
    if relative:
        (columns,) = call(
            pack, None, columns, [shape(seq_count, rows, dp_count * padded, dtype=BF16)], cost=1
        )
    all_columns = around(columns, "chan")
    (turned,) = call(
        turn,
        places,
        all_columns,
        [shape(dp_count * padded, seq_count * length, dtype=BF16)],
        [pltpu.VMEM((seq_count * length, dp_count * padded), BF16)],
    )

    pair, mixer_local, step_grad, early, *mixer_sent = call(
        functools.partial(finish, head_dim, relative, seq_count, chan_count),
        places,
        received
        + [
            inner_pre,
            mixer_pre,
            step,
            decay,
            step_raw,
            head_rows,
            upstream,
            conv_inner,
            conv_mixer,
            inner_part,
            mixer_part,
            row_part,
            column_part,
        ],
        [
            shape(length + PAD, width, dtype=BF16),
            shape(length, mixed, dtype=BF16),
            shape(length, LANES, dtype=BF16),
            shape(PAD, width + mixed),
        ]
        + [shape(rows + PAD, mixed, dtype=BF16)] * chan_count,
        [pltpu.VMEM((length + 2 * PAD, width), F32), pltpu.VMEM((length + 2 * PAD, mixed), F32)],
        cost=5,
    )

    def over_seq(block):
        if relative:
            return around(block, "seq")
        return [lax.all_gather(block, "seq")]

    backward_pairs = [(source + 1, source) for source in range(seq_count - 1)]
    late = lax.ppermute(early, "seq", backward_pairs)
    pairs = over_seq(pair)
    mixer_rows = list(mixer_sent[:1]) + [
        lax.ppermute(block, "chan", ring("chan", hop))
        for hop, block in enumerate(mixer_sent[1:], 1)
    ]
    (mixer_rows,) = call(add_up, None, mixer_rows, [shape(rows + PAD, mixed, dtype=BF16)], cost=1)
    mixers = over_seq(mixer_rows)

    (sent,) = call(
        project_back,
        None,
        [pair, late, mixer_local, step_grad, inner_back, mixer_back, step_near],
        [shape(chan_count, rows, model, dtype=BF16)],
        [pltpu.VMEM((length, width + LANES), BF16), pltpu.VMEM((length, mixed), BF16)],
        cost=4,
    )
    taken = lax.all_to_all(sent, "chan", split_axis=0, concat_axis=0)

    groups = width // length
    used = -(-head_count // groups)
    step_lines = -(-used * groups // (2 * PAD)) * (2 * PAD)
    leaving, grads, steps = call(
        functools.partial(leave, relative, taps, used, grad_rows, norm_factor),
        places,
        [turned] + pairs,
        [
            shape(grad_rows + step_lines, width, dtype=BF16),
            shape(seq_count * length, width, dtype=BF16),
            shape(step_lines, seq_count * length, dtype=BF16),
        ],
    )
    arrived = lax.ppermute(leaving, "dp", ring("dp", 1))
    kept, kept_step = call(
        functools.partial(keep, grad_rows, norm_factor),
        None,
        [turned, grads, steps],
        [shape(grad_rows, width), shape(step_lines, padded)],
    )
    (mixer_blocks,) = call(
        functools.partial(mix, relative, taps, grad_rows // chan_count, norm_factor),
        places,
        [columns] + mixers,
        [shape(dp_count * chan_count, grad_rows // chan_count, mixed, dtype=BF16)],
        [
            pltpu.VMEM((seq_count * rows, dp_count * padded), BF16),
            pltpu.VMEM((seq_count * rows, mixed), BF16),
        ],
        cost=2,
    )
    taken, mixer_blocks = lax.optimization_barrier((taken, mixer_blocks))
    mixer_blocks = lax.all_to_all(
        mixer_blocks, ("dp", "chan"), split_axis=0, concat_axis=0
    )
    (mixer_weight_grad,) = call(
        add_parts, None, [mixer_blocks], [jax.ShapeDtypeStruct(mixer_blocks.shape[1:], F32)], cost=1
    )
    (input_grad,) = call(
        add_parts, None, [taken], [jax.ShapeDtypeStruct((rows, model), BF16)], cost=1
    )
    inner_weight_grad, step_weight_grad = call(
        functools.partial(last, used),
        None,
        [kept, kept_step, arrived],
        [
            jax.ShapeDtypeStruct((grad_rows, width), F32),
            jax.ShapeDtypeStruct((head_count, grad_rows), F32),
        ],
        cost=1,
    )
    step_weight_grad = step_weight_grad.T
    return (input_grad[None], inner_weight_grad, mixer_weight_grad, step_weight_grad)


def solution(mesh):
    in_specs = (
        P("dp", ("seq", "chan"), None),
        P(None, "chan"),
        P(),
        P(None, "chan"),
        P(None, "chan"),
        P(),
        P("chan"),
        P("chan"),
        P("chan"),
        P("dp", "seq", "chan"),
    )
    out_specs = (
        P("dp", ("seq", "chan"), None),
        P(("dp", "seq"), "chan"),
        P(("dp", "seq", "chan"), None),
        P(("dp", "seq"), "chan"),
    )
    return jax.shard_map(body, mesh=mesh, in_specs=in_specs, out_specs=out_specs, check_vma=False)
```

```python
import functools
import math

import jax
import jax.numpy as jnp
from jax import lax
from jax.experimental import pallas as pl
from jax.experimental.pallas import tpu as pltpu
from jax.sharding import PartitionSpec as P


F32 = jnp.float32
BF16 = jnp.bfloat16
LANES = 128
PAD = 8
DIRECT = 8


def dot(left, right, left_dim=1, right_dim=0):
    return lax.dot_general(
        left,
        right,
        (((left_dim,), (right_dim,)), ((), ())),
        preferred_element_type=F32,
    )


def pieces(values):
    high = values.astype(BF16)
    rest = values - high.astype(F32)
    middle = rest.astype(BF16)
    low = (rest - middle.astype(F32)).astype(BF16)
    return high, middle, low


def fine(left, right, left_dim=1, right_dim=0):
    left_high = left.astype(BF16)
    left_low = (left - left_high.astype(F32)).astype(BF16)
    right_high = right.astype(BF16)
    right_low = (right - right_high.astype(F32)).astype(BF16)
    lefts = jnp.concatenate([left_high, left_low, left_high], axis=left_dim)
    rights = jnp.concatenate([right_high, right_high, right_low], axis=right_dim)
    return dot(lefts, rights, left_dim, right_dim)


def half_fine(left, right, left_dim=1, right_dim=0):
    high = left.astype(BF16)
    low = (left - high.astype(F32)).astype(BF16)
    rounded = right.astype(BF16)
    lefts = jnp.concatenate([high, low], axis=left_dim)
    return dot(lefts, jnp.concatenate([rounded, rounded], axis=right_dim), left_dim, right_dim)


def masked_sum(mask, values, values_dim=0):
    chosen = jnp.where(mask, 1.0, 0.0).astype(BF16)
    masks = jnp.concatenate([chosen] * 3, axis=1)
    return dot(masks, jnp.concatenate(pieces(values), axis=values_dim), 1, values_dim)


def head_map(width, head_dim):
    row = lax.broadcasted_iota(jnp.int32, (LANES, width), 0)
    column = lax.broadcasted_iota(jnp.int32, (LANES, width), 1)
    start = row * head_dim
    return jnp.where((column >= start) & (column < start + head_dim), 1.0, 0.0).astype(BF16)


def spread(values, heads):
    return dot(jnp.concatenate(pieces(values), axis=1), jnp.concatenate([heads] * 3, axis=0))


def collect(values, heads):
    high, middle, _ = pieces(values)
    return dot(high, heads, 1, 1) + dot(middle, heads, 1, 1)


def sigmoid(values):
    return 1.0 / (1.0 + jnp.exp(-values))


def softplus(values):
    small = jnp.exp(-jnp.abs(values))
    series = small * (1.0 - small * (0.5 - small * (1.0 / 3.0)))
    return jnp.maximum(values, 0.0) + jnp.where(small < 1e-3, series, jnp.log(1.0 + small))


def triangle(length):
    row = lax.broadcasted_iota(jnp.int32, (length, length), 0)
    column = lax.broadcasted_iota(jnp.int32, (length, length), 1)
    return row, column


def convolve(values, history, kernel, scratch):
    length = values.shape[0]
    taps = kernel.shape[0]
    scratch[:PAD] = history.astype(F32)
    scratch[PAD:] = values.astype(F32)
    total = kernel[taps - 1 : taps] * scratch[PAD : PAD + length]
    for tap in range(taps - 1):
        start = PAD - (taps - 1) + tap
        total = total + kernel[tap : tap + 1] * scratch[start : start + length]
    return total


def convolve_back(gradient, kernel, scratch):
    length = gradient.shape[0]
    taps = kernel.shape[0]
    zeros = jnp.zeros((PAD, gradient.shape[1]), F32)
    scratch[:PAD] = zeros
    scratch[PAD : PAD + length] = gradient
    scratch[PAD + length :] = zeros
    extent = length + PAD
    total = None
    for tap in range(taps):
        start = taps - 1 - tap
        term = kernel[tap : tap + 1] * scratch[start : start + extent]
        total = term if total is None else total + term
    return total


def blocks(rows, padded, dp_count, relative, place_ref, *refs):
    own_ref, step_ref, bias_ref, log_ref, skip_ref, inner_ref, mixer_ref = refs[:7]
    own_out_ref, step_out_ref, head_ref, inner_out_ref, mixer_out_ref = refs[7:12]
    out_refs, scratch, wide, sems = refs[12:-3], refs[-3], refs[-2], refs[-1]
    parts = sems.shape[1]
    depth = inner_ref.shape[0] // parts
    copies = []
    for part in range(parts):
        span = pl.ds(part * depth, depth)
        pair = ((inner_ref, inner_out_ref), (mixer_ref, mixer_out_ref))
        for number, (source, target) in enumerate(pair):
            copy = pltpu.make_async_copy(source.at[span], target.at[span], sems.at[number, part])
            copy.start()
            copies.append(copy)
    own_out_ref[...] = own_ref[...]
    head_count = bias_ref.shape[1]
    wide[...] = jnp.zeros_like(wide)
    wide[:head_count] = step_ref[...].astype(F32)
    step_out_ref[...] = wide[...].T.astype(BF16)
    head_ref[...] = jnp.zeros_like(head_ref)
    head_ref[0:1, :head_count] = bias_ref[...]
    head_ref[1:2, :head_count] = log_ref[...]
    head_ref[2:3, :head_count] = skip_ref[...]
    dp_place = place_ref[1]
    seq_count = scratch.shape[0]
    fill = jnp.zeros((own_ref.shape[0], padded - rows), F32)
    for target in range(seq_count):
        for hop in range(dp_count):
            wanted = lax.rem(dp_place + hop, dp_count)
            chosen = None
            for other in range(dp_count):
                start = (other * seq_count + target) * rows
                part = own_ref[:, start : start + rows].astype(F32)
                chosen = part if chosen is None else jnp.where(wanted == other, part, chosen)
            span = slice(hop * padded, (hop + 1) * padded)
            if padded > rows:
                chosen = jnp.concatenate([chosen, fill], axis=1)
            scratch[target, :, span] = chosen.astype(BF16)
    if relative:
        for hop, out_ref in enumerate(out_refs):
            out_ref[...] = scratch[lax.rem(place_ref[0] + hop, seq_count)]
    else:
        out_refs[0][...] = scratch[...]
    for copy in copies:
        copy.wait()


def copied(sources, targets, sems):
    copies = [
        pltpu.make_async_copy(source, target, sems.at[number])
        for number, (source, target) in enumerate(zip(sources, targets))
    ]
    for copy in copies:
        copy.start()
    return copies


def pack(*refs):
    for number, ref in enumerate(refs[:-1]):
        refs[-1][number] = ref[...]


def add_up(*refs):
    total = refs[0][...].astype(F32)
    for part in refs[1:-1]:
        total = total + part[...].astype(F32)
    refs[-1][...] = total.astype(refs[-1].dtype)


def project(count, place_ref, *refs):
    tokens = refs[:count]
    inner_ref, mixer_ref, step_ref, inner_out, mixer_out, raw_out, tail_out, scratch = refs[count:]
    place = place_ref[2]
    rows = tokens[0].shape[0]
    for hop in range(count):
        source = lax.bitwise_xor(place, hop)
        scratch[pl.ds(pl.multiple_of(source * rows, rows), rows)] = tokens[hop][...]
    gathered = scratch[...]
    length = gathered.shape[0]
    width = inner_ref.shape[1]
    whole = width // (2 * LANES) * (2 * LANES)
    mixer = dot(gathered, mixer_ref[...]).astype(BF16)
    first = dot(gathered, inner_ref[:, :whole])
    joined = jnp.concatenate([inner_ref[:, whole:], step_ref[...]], axis=1)
    second = dot(gathered, joined)
    raw_out[...] = second[:, width - whole :]
    inner = jnp.concatenate([first, second[:, : width - whole]], axis=1).astype(BF16)
    inner_out[...] = inner
    mixer_out[...] = mixer
    tail_out[:, :width] = inner[length - 2 * PAD :]
    tail_out[:, width:] = mixer[length - 2 * PAD :]


def prepare(head_dim, relative, place_ref, *refs):
    (
        inner_ref,
        mixer_ref,
        history_ref,
        raw_ref,
        head_ref,
        upstream_ref,
        conv_inner_ref,
        conv_mixer_ref,
        inner_pre_ref,
        mixer_pre_ref,
        step_ref,
        decay_ref,
    ) = refs[:12]
    message_refs = refs[12:-2]
    inner_scratch, mixer_scratch = refs[-2:]
    length, width = inner_ref.shape
    state = mixer_ref.shape[1] // 2
    place = place_ref[0]
    history = history_ref[...].astype(F32)[PAD:]
    inner_pre = convolve(inner_ref[...], history[:, :width], conv_inner_ref[...], inner_scratch)
    mixer_pre = convolve(mixer_ref[...], history[:, width:], conv_mixer_ref[...], mixer_scratch)
    inner_pre_ref[...] = inner_pre
    mixer_pre_ref[...] = mixer_pre
    inner_act = inner_pre * sigmoid(inner_pre)
    mixer_act = mixer_pre * sigmoid(mixer_pre)
    step = softplus(raw_ref[...] + head_ref[0:1])
    log_decay = -step * jnp.exp(head_ref[1:2])
    row, column = triangle(length)
    decay = masked_sum(row >= column, log_decay)
    step_ref[...] = step
    decay_ref[...] = decay
    heads = head_map(width, head_dim)
    last = decay[length - 1 : length]
    tail = spread(jnp.exp(last - decay) * step, heads)
    lead = spread(jnp.exp(decay), heads)
    upstream = upstream_ref[...].astype(F32)
    forward = half_fine(mixer_act[:, :state].T, tail * inner_act).astype(BF16)
    backward = half_fine(mixer_act[:, state:].T, lead * upstream).astype(BF16)
    high, middle, low = pieces(last)
    kinds = (high.astype(F32), middle.astype(F32), low.astype(F32))
    index = lax.broadcasted_iota(jnp.int32, (PAD, LANES), 0)
    stacked = jnp.zeros((PAD, LANES), F32)
    for number, kind in enumerate(kinds):
        stacked = jnp.where(index == number, kind, stacked)
    extra = dot(stacked.astype(BF16), heads).astype(BF16)
    if relative:
        count = len(message_refs) + 1
        for hop, message_ref in enumerate(message_refs, 1):
            message_ref[:state] = jnp.where(place + hop < count, forward, backward)
            message_ref[state:] = extra
    else:
        message_ref = message_refs[0]
        for target in range(message_ref.shape[0]):
            message_ref[target, :state] = jnp.where(target > place, forward, backward)
            message_ref[target, state:] = extra


def within(
    head_dim,
    inner_pre_ref,
    mixer_pre_ref,
    step_ref,
    decay_ref,
    head_ref,
    upstream_ref,
    inner_weight_ref,
    mixer_weight_ref,
    inner_grad_ref,
    mixer_grad_ref,
    row_ref,
    column_ref,
    lead_ref,
    tail_ref,
    inner_near_ref,
    mixer_near_ref,
    sems,
):
    copies = copied(
        (inner_weight_ref, mixer_weight_ref), (inner_near_ref, mixer_near_ref), sems
    )
    length, width = inner_pre_ref.shape
    state = mixer_pre_ref.shape[1] // 2
    mixer_pre = mixer_pre_ref[...]
    mixer_act = mixer_pre * sigmoid(mixer_pre)
    input_mix = mixer_act[:, :state]
    output_mix = mixer_act[:, state:]
    decay = decay_ref[...]
    step = step_ref[...]
    turned = decay.T
    row, column = triangle(length)
    causal = column >= row
    scores = fine(input_mix, output_mix, 1, 1)
    heads = head_map(width, head_dim)
    skip = spread(head_ref[...], heads)[2:3]
    step_wide = spread(step, heads)
    lead_ref[...] = spread(jnp.exp(decay), heads)
    tail_ref[...] = spread(jnp.exp(decay[length - 1 : length] - decay) * step, heads)
    group_heads = LANES // head_dim
    lane = lax.broadcasted_iota(jnp.int32, (length, LANES), 1)
    mixed = jnp.zeros((length, length), F32)
    rows = jnp.zeros((length, LANES), F32)
    columns = []
    for group in range(width // LANES):
        span = slice(group * LANES, (group + 1) * LANES)
        inner_pre = inner_pre_ref[:, span]
        inner_act = inner_pre * sigmoid(inner_pre)
        high = inner_act.astype(BF16)
        low = (inner_act - high.astype(F32)).astype(BF16)
        upstream = upstream_ref[:, span]
        total = None
        for member in range(group_heads):
            head = group * group_heads + member
            mine = (lane >= member * head_dim) & (lane < (member + 1) * head_dim)
            mine_upstream = jnp.where(mine, upstream.astype(F32), 0.0).astype(BF16)
            spread_of = turned[head : head + 1] - decay[:, head : head + 1]
            fall = jnp.exp(jnp.where(causal, spread_of, -1e30))
            match = dot(high, mine_upstream, 1, 1) + dot(low, mine_upstream, 1, 1)
            weight = fall * scores
            cross = weight * match
            step_column = step[:, head : head + 1]
            mixed = mixed + step_column * (fall * match)
            rows = jnp.where(lane == head, jnp.sum(cross, axis=1, keepdims=True), rows)
            columns.append(jnp.sum(step_column * cross, axis=0, keepdims=True))
            weight_high = weight.astype(BF16)
            weight_low = (weight - weight_high.astype(F32)).astype(BF16)
            term = dot(weight_high, mine_upstream) + dot(weight_low, mine_upstream)
            total = term if total is None else total + term
        inner_grad_ref[:, span] = step_wide[:, span] * total + skip[:, span] * upstream.astype(F32)
    mixer_grad_ref[:, :state] = fine(mixed, output_mix)
    mixer_grad_ref[:, state:] = fine(mixed.T, input_mix)
    row_ref[...] = rows
    index = lax.broadcasted_iota(jnp.int32, (LANES, length), 0)
    stacked = jnp.zeros((LANES, length), F32)
    for number, kind in enumerate(columns):
        stacked = jnp.where(index == number, kind, stacked)
    column_ref[...] = stacked
    for copy in copies:
        copy.wait()


def finish(
    head_dim,
    relative,
    count,
    chan_count,
    place_ref,
    *refs,
):
    messages = refs[: count - 1] if relative else refs[:1]
    inner_scratch, mixer_scratch = refs[-2:]
    mixer_sent_refs = refs[-2 - chan_count : -2]
    refs = refs[len(messages) : -2 - chan_count]
    (
        inner_pre_ref,
        mixer_pre_ref,
        step_ref,
        decay_ref,
        raw_ref,
        head_ref,
        upstream_ref,
        conv_inner_ref,
        conv_mixer_ref,
        inner_grad_ref,
        mixer_grad_ref,
        row_ref,
        column_ref,
        lead_ref,
        tail_ref,
        pair_ref,
        mixer_out_ref,
        step_out_ref,
        early_ref,
    ) = refs
    length, width = inner_pre_ref.shape
    state = mixer_pre_ref.shape[1] // 2
    place = place_ref[0]

    def message(hop):
        if relative:
            return messages[hop - 1][...].astype(F32)
        return messages[0][lax.rem(place - hop + count, count)].astype(F32)

    def shard_decay(parts):
        return parts[state : state + 1] + parts[state + 1 : state + 2] + parts[state + 2 : state + 3]

    start = jnp.zeros((state, width), F32)
    running = jnp.zeros((1, width), F32)
    end = jnp.zeros((state, width), F32)
    if relative:
        received = [None] + [message(hop) for hop in range(1, count)]
        back_running = jnp.zeros((1, width), F32)
        for hop in range(1, count):
            factor = jnp.where(hop <= place, jnp.exp(running), 0.0)
            start = start + factor * received[hop][:state]
            running = running + shard_decay(received[hop])
            other = count - hop
            factor = jnp.where(other > place, jnp.exp(back_running), 0.0)
            end = end + factor * received[other][:state]
            back_running = back_running + shard_decay(received[other])
    else:

        def before(hop, carried):
            start, running = carried
            parts = message(hop)
            return start + jnp.exp(running) * parts[:state], running + shard_decay(parts)

        def after(step, carried):
            end, running = carried
            parts = message(count - step)
            return end + jnp.exp(running) * parts[:state], running + shard_decay(parts)

        start, unused = lax.fori_loop(1, place + 1, before, (start, running))
        end, unused = lax.fori_loop(1, count - place, after, (end, running))

    inner_pre = inner_pre_ref[...]
    mixer_pre = mixer_pre_ref[...]
    inner_sig = sigmoid(inner_pre)
    mixer_sig = sigmoid(mixer_pre)
    inner_act = inner_pre * inner_sig
    mixer_act = mixer_pre * mixer_sig
    input_mix = mixer_act[:, :state]
    output_mix = mixer_act[:, state:]
    decay = decay_ref[...]
    step = step_ref[...]
    upstream = upstream_ref[...].astype(F32)
    heads = head_map(width, head_dim)
    last = decay[length - 1 : length]
    lead = jnp.exp(decay)
    rest = jnp.exp(last - decay)
    lead_wide = lead_ref[...]
    tail_wide = tail_ref[...]
    from_end = half_fine(input_mix, end)
    from_start = half_fine(output_mix, start)
    inner_grad = inner_grad_ref[...] + tail_wide * from_end
    input_grad = mixer_grad_ref[:, :state] + half_fine(tail_wide * inner_act, end, 1, 1)
    output_grad = mixer_grad_ref[:, state:] + half_fine(lead_wide * upstream, start, 1, 1)
    end_part = rest * collect(inner_act * from_end, heads)
    start_part = lead * collect(upstream * from_start, heads)
    product = jnp.sum(end * start, axis=0, keepdims=True)
    product = collect(jnp.broadcast_to(product, (PAD, width)), heads)[0:1]
    step_grad = row_ref[...] + end_part
    sums = start_part - step * step_grad
    total = jnp.sum(step * end_part, axis=0, keepdims=True) + jnp.exp(last) * product
    row, column = triangle(length)
    after_row = column >= row
    decay_grad = masked_sum(after_row, sums) + masked_sum(after_row, column_ref[...], 1) + total
    step_grad = step_grad - jnp.exp(head_ref[1:2]) * decay_grad
    raw_grad = step_grad * sigmoid(raw_ref[...] + head_ref[0:1])
    step_out_ref[...] = raw_grad.astype(BF16)
    turned = raw_grad.T
    groups = width // length
    packed = jnp.zeros((PAD, width), F32)
    index = lax.broadcasted_iota(jnp.int32, (PAD, width), 0)
    head_count = width // head_dim
    for number in range(-(-head_count // groups)):
        line = [turned[number * groups + group : number * groups + group + 1] for group in range(groups)]
        packed = jnp.where(index == number, jnp.concatenate(line, axis=1), packed)
    inner_slope = inner_sig * (1.0 + inner_pre * (1.0 - inner_sig))
    mixer_slope = mixer_sig * (1.0 + mixer_pre * (1.0 - mixer_sig))
    inner_total = convolve_back(inner_grad * inner_slope, conv_inner_ref[...], inner_scratch)
    mixer_total = jnp.concatenate([input_grad, output_grad], axis=1) * mixer_slope
    mixer_total = convolve_back(mixer_total, conv_mixer_ref[...], mixer_scratch)
    taps = conv_inner_ref.shape[0] - 1
    early = PAD - taps
    inner_scratch[:PAD] = jnp.where(index >= early, inner_total[:PAD], packed)
    early_ref[:, :width] = inner_total[:PAD]
    early_ref[:, width:] = mixer_total[:PAD]
    pair_ref[:length] = inner_total[PAD:].astype(BF16)
    pair_ref[length:] = inner_scratch[:PAD].astype(BF16)
    mixer_out_ref[...] = mixer_total[PAD:].astype(BF16)
    rows = length // chan_count
    back = mixer_total[:PAD].astype(BF16)
    mixer_scratch[:length] = mixer_total[PAD:]
    for hop, sent_ref in enumerate(mixer_sent_refs):
        target = lax.rem(place_ref[2] + hop, chan_count)
        start = pl.multiple_of(target * rows, rows)
        sent_ref[:rows] = mixer_scratch[pl.ds(start, rows)].astype(BF16)
        sent_ref[rows:] = back


def add_late(ending, extra, taps, valid):
    index = lax.broadcasted_iota(jnp.int32, ending.shape, 0)
    late = jnp.where((index >= PAD - taps) & valid, extra, 0.0)
    return ending + late


def project_back(
    chan_count,
    place_ref,
    pair_ref,
    early_ref,
    mixer_ref,
    step_ref,
    inner_weight_ref,
    mixer_weight_ref,
    step_weight_ref,
    *refs,
):
    out_refs = refs[:chan_count]
    inner_scratch, mixer_scratch, share_scratch = refs[chan_count:]
    length, mixed = mixer_ref.shape
    width = pair_ref.shape[1]
    rows = length // chan_count
    whole = width // (2 * LANES) * (2 * LANES)
    fill = jnp.zeros((PAD, width + mixed), F32)
    early = jnp.concatenate([early_ref[...], fill], axis=0).astype(BF16)
    inner_scratch[:length, :width] = pair_ref[:length]
    inner_scratch[:length, width:] = step_ref[...]
    inner_scratch[length:, :width] = early[:, :width]
    inner_scratch[length:, width:] = jnp.zeros((2 * PAD, LANES), BF16)
    mixer_scratch[:length] = mixer_ref[...]
    mixer_scratch[length:] = early[:, width:]
    share = dot(inner_scratch[:, :whole], inner_weight_ref[:, :whole], 1, 1)
    right = jnp.concatenate([inner_weight_ref[:, whole:], step_weight_ref[...]], axis=1)
    share = share + dot(inner_scratch[:, whole:], right, 1, 1)
    share = share + dot(mixer_scratch[...], mixer_weight_ref[...], 1, 1)
    share_scratch[...] = share.astype(BF16)
    for hop, out_ref in enumerate(out_refs):
        target = lax.rem(place_ref[2] + hop, chan_count)
        start = pl.multiple_of(target * rows, rows)
        out_ref[:rows] = share_scratch[pl.ds(start, rows)]
        out_ref[rows:] = share_scratch[length : length + PAD]


def gather_share(*refs):
    total_ref, ending_ref, back_ref = refs[-3:]
    total = refs[0][...].astype(F32)
    for part in refs[1:-3]:
        total = total + part[...].astype(F32)
    rows = total_ref.shape[0]
    total_ref[...] = total[:rows].astype(BF16)
    ending_ref[...] = total[rows - PAD : rows]
    back_ref[...] = total[rows:].astype(BF16)


def close_share(
    taps, chan_count, place_ref, total_ref, ending_ref, late_ref, out_ref, scratch, done
):
    del total_ref
    valid = place_ref[2] == chan_count - 1
    ending = add_late(ending_ref[...], late_ref[...].astype(F32), taps, valid)
    scratch[...] = ending.astype(BF16)
    head = out_ref.shape[0] - PAD
    copy = pltpu.make_async_copy(scratch, out_ref.at[pl.ds(head, PAD)], done)
    copy.start()
    copy.wait()


def turn(place_ref, *refs):
    column_refs, out_ref, own_ref, columns = refs[:-3], refs[-3], refs[-2], refs[-1]
    chan_place = place_ref[2]
    chan_count = len(column_refs)
    seq_count, rows, _ = column_refs[0].shape
    length = chan_count * rows
    for hop in range(seq_count):
        for chan_hop in range(chan_count):
            chan_source = lax.rem(chan_place - chan_hop + chan_count, chan_count)
            start = pl.multiple_of(hop * length + chan_source * rows, rows)
            columns[pl.ds(start, rows)] = column_refs[chan_hop][hop]
    out_ref[...] = columns[...].T
    own = [column_refs[0][hop] for hop in range(seq_count)]
    own_ref[...] = jnp.concatenate(own, axis=0).T


def arrange(relative, taps, used, place_ref, pair_refs, grads, steps):
    seq_place = place_ref[0]
    seq_count = len(pair_refs) if relative else pair_refs[0].shape[0]
    length = grads.shape[0] // seq_count

    def message(hop):
        return pair_refs[hop][...] if relative else pair_refs[0][hop]

    for hop in range(seq_count):
        if relative:
            shard = lax.rem(seq_place - hop + seq_count, seq_count)
            after = (hop - 1) % seq_count
        else:
            shard = hop
            after = (hop + 1) % seq_count
        pair = message(hop)
        start = hop * length
        head = length - PAD
        grads[start : start + head] = pair[:head]
        extra = message(after)[length:].astype(F32)
        ending = add_late(pair[head:length].astype(F32), extra, taps, shard < seq_count - 1)
        grads[start + head : start + length] = ending.astype(BF16)
        packed = pair[length:].astype(F32)
        groups = packed.shape[1] // length
        lines = [packed[:used, group * length : (group + 1) * length] for group in range(groups)]
        spare = steps.shape[0] - used * groups
        lines = lines + [jnp.zeros((spare, length), F32)]
        steps[:, start : start + length] = jnp.concatenate(lines, axis=0).astype(BF16)


def leave(relative, taps, used, rows, scale, place_ref, *refs):
    turned_ref = refs[0]
    out_ref, grads, steps = refs[-3:]
    arrange(relative, taps, used, place_ref, refs[1:-3], grads, steps)
    padded = turned_ref.shape[0] // 2
    chosen = turned_ref[padded : padded + rows]
    out_ref[:rows] = (dot(chosen, grads[...]) * scale).astype(BF16)
    lines = steps.shape[0]
    term = dot(steps[...], turned_ref[padded:], 1, 1) * scale
    out_ref[rows:, :padded] = term.astype(BF16)
    out_ref[rows:, padded:] = jnp.zeros((lines, out_ref.shape[1] - padded), BF16)


def keep(rows, scale, turned_ref, grads_ref, steps_ref, out_ref, step_ref):
    padded = turned_ref.shape[0] // 2
    out_ref[...] = dot(turned_ref[:rows], grads_ref[...]) * scale
    step_ref[...] = dot(steps_ref[...], turned_ref[:padded], 1, 1) * scale


def last(used, kept_ref, step_ref, arrived_ref, out_ref, step_out_ref):
    rows, _ = kept_ref.shape
    out_ref[...] = kept_ref[...] + arrived_ref[:rows].astype(F32)
    step = step_ref[:, :rows] + arrived_ref[rows:, :rows].astype(F32)
    head_count = step_out_ref.shape[0]
    groups = -(-head_count // used)
    for head in range(head_count):
        line = (head % groups) * used + head // groups
        step_out_ref[head : head + 1] = step[line : line + 1]


def mix(relative, taps, rows, scale, chan_count, place_ref, *refs):
    column_ref, scratch, grads = refs[0], refs[-2], refs[-1]
    grad_refs = refs[1 : -2 - chan_count]
    out_refs = refs[-2 - chan_count : -2]
    seq_place = place_ref[0]
    chan_place = place_ref[2]
    wide = column_ref.shape[0]
    seq_count = len(grad_refs) if relative else grad_refs[0].shape[0]
    tokens = grads.shape[0] // seq_count

    def message(hop):
        return grad_refs[hop][...] if relative else grad_refs[0][hop]

    for hop in range(seq_count):
        if relative:
            source = lax.rem(seq_place - hop + seq_count, seq_count)
            after = (hop - 1) % seq_count
        else:
            source = hop
            after = (hop + 1) % seq_count
        start = hop * tokens
        head = tokens - PAD
        block = message(hop)
        grads[start : start + head] = block[:head]
        valid = (source < seq_count - 1) & (chan_place == chan_count - 1)
        extra = message(after)[tokens:].astype(F32)
        ending = add_late(block[head:tokens].astype(F32), extra, taps, valid)
        grads[start + head : start + tokens] = ending.astype(BF16)
    padded = wide // 2
    scratch[...] = dot(column_ref[...], grads[...]) * scale
    for hop, out_ref in enumerate(out_refs):
        target = lax.rem(chan_place + hop, chan_count)
        for dp_hop in range(2):
            start = pl.multiple_of(dp_hop * padded + target * rows, PAD)
            part = scratch[pl.ds(start, rows)]
            out_ref[dp_hop * rows : (dp_hop + 1) * rows] = part.astype(BF16)


def add_chan(*refs):
    kept_ref, leaving_ref = refs[-2:]
    total = refs[0][...].astype(F32)
    for part in refs[1:-2]:
        total = total + part[...].astype(F32)
    rows = kept_ref.shape[0]
    kept_ref[...] = total[:rows]
    leaving_ref[...] = total[rows:].astype(BF16)


def add_pair(kept_ref, arrived_ref, out_ref):
    out_ref[...] = kept_ref[...] + arrived_ref[...].astype(F32)


def shape(*dims, dtype=F32):
    return pltpu.VMEM(dims, dtype)


def ring(axis, hop):
    count = lax.axis_size(axis)
    return [(source, (source + hop) % count) for source in range(count)]


def call(body, place, arrays, out_shape, scratch=(), cost=3, plain=(), left=(), in_place=False):
    vmem = pltpu.MemorySpace.VMEM
    hbm = pltpu.MemorySpace.HBM
    arrays = [
        pltpu.with_memory_space_constraint(array, hbm if number in plain else vmem)
        for number, array in enumerate(arrays)
    ]
    in_specs = [
        pl.BlockSpec(memory_space=hbm if number in left else vmem) for number in range(len(arrays))
    ]
    out_specs = [pl.BlockSpec(memory_space=hbm if in_place else vmem)] * len(out_shape)
    if place is not None:
        in_specs = [pl.BlockSpec(memory_space=pltpu.SMEM)] + in_specs
        arrays = [place] + arrays
    return pl.pallas_call(
        body,
        out_shape=out_shape,
        in_specs=in_specs,
        out_specs=out_specs,
        scratch_shapes=list(scratch),
        input_output_aliases={1: 0} if in_place else {},
        cost_estimate=pl.CostEstimate(flops=cost * 10**8, bytes_accessed=0, transcendentals=0),
        compiler_params=pltpu.CompilerParams(vmem_limit_bytes=24 * 2**20),
    )(*arrays)


def around(block, axis):
    count = lax.axis_size(axis)
    return [block] + [
        lax.ppermute(block, axis, ring(axis, hop)) for hop in range(1, count)
    ]


def spread_out(block, axis):
    count = lax.axis_size(axis)
    parts = {0: block}
    bit = count // 2
    while bit:
        pairs = [(source, source ^ bit) for source in range(count)]
        for number in list(parts):
            parts[number | bit] = lax.ppermute(parts[number], axis, pairs)
        bit //= 2
    return [parts[number] for number in range(count)]


def body(
    layer_input,
    inner_weight,
    mixer_weight,
    step_weight,
    conv_inner,
    conv_mixer,
    step_bias,
    decay_log,
    skip_gain,
    output_grad,
):
    own = layer_input[0]
    dp_count = lax.axis_size("dp")
    seq_count = lax.axis_size("seq")
    chan_count = lax.axis_size("chan")
    place = lax.axis_index("seq")
    relative = seq_count <= DIRECT
    rows, model = own.shape
    length = rows * chan_count
    width = inner_weight.shape[1]
    head_count = step_bias.shape[0]
    head_dim = width // head_count
    mixed = mixer_weight.shape[1]
    state = mixed // 2
    upstream = output_grad[0]
    grad_rows = model // (dp_count * seq_count)
    padded = -(-grad_rows // (2 * PAD)) * (2 * PAD)
    taps = conv_inner.shape[0] - 1
    parts = next(count for count in (4, 2, 1) if model % (count * LANES) == 0)
    places = [place, lax.axis_index("dp"), lax.axis_index("chan")]
    places = jnp.stack(places).astype(jnp.int32)
    norm_factor = 1.0 / math.sqrt(length * seq_count * dp_count)

    gathered = spread_out(own, "chan")
    if relative:
        column_shapes = [shape(rows, dp_count * padded, dtype=BF16)] * seq_count
    else:
        column_shapes = [shape(seq_count, rows, dp_count * padded, dtype=BF16)]
    own_near, step_near, head_rows, inner_near, mixer_near, *sorted_columns = call(
        functools.partial(blocks, grad_rows, padded, dp_count, relative),
        places,
        [
            own,
            step_weight.T,
            step_bias[None],
            decay_log[None],
            skip_gain[None],
            inner_weight,
            mixer_weight,
        ],
        [
            shape(rows, model, dtype=BF16),
            shape(model, LANES, dtype=BF16),
            shape(PAD, LANES),
            shape(model, width, dtype=BF16),
            shape(model, mixed, dtype=BF16),
        ]
        + column_shapes,
        [
            pltpu.VMEM((seq_count, rows, dp_count * padded), BF16),
            pltpu.VMEM((LANES, model), F32),
            pltpu.SemaphoreType.DMA((2, parts)),
        ],
        cost=1,
        plain=range(7),
        left=(5, 6),
    )
    if relative:
        columns = [sorted_columns[0]]
        for hop, block in enumerate(sorted_columns[1:], 1):
            columns.append(lax.ppermute(block, "seq", ring("seq", hop)))
    else:
        columns = lax.all_to_all(sorted_columns[0], "seq", split_axis=0, concat_axis=0)
    inner_proj, mixer_proj, step_raw, tail = call(
        functools.partial(project, chan_count),
        places,
        [own_near] + gathered[1:] + [inner_near, mixer_near, step_near],
        [
            shape(length, width, dtype=BF16),
            shape(length, mixed, dtype=BF16),
            shape(length, LANES),
            shape(2 * PAD, width + mixed, dtype=BF16),
        ],
        [pltpu.VMEM((length, model), BF16)],
        cost=4,
    )
    forward_pairs = [(source, source + 1) for source in range(seq_count - 1)]
    history = lax.ppermute(tail, "seq", forward_pairs)

    if relative:
        message_shapes = [shape(state + PAD, width, dtype=BF16)] * (seq_count - 1)
    else:
        message_shapes = [shape(seq_count, state + PAD, width, dtype=BF16)]
    inner_pre, mixer_pre, step, decay, *messages = call(
        functools.partial(prepare, head_dim, relative),
        places,
        [inner_proj, mixer_proj, history, step_raw, head_rows, upstream, conv_inner, conv_mixer],
        [
            shape(length, width),
            shape(length, mixed),
            shape(length, LANES),
            shape(length, LANES),
        ]
        + message_shapes,
        [pltpu.VMEM((PAD + length, width), F32), pltpu.VMEM((PAD + length, mixed), F32)],
    )
    if relative:
        received = [
            lax.ppermute(message, "seq", ring("seq", hop))
            for hop, message in enumerate(messages, 1)
        ]
    else:
        received = [lax.all_to_all(messages[0], "seq", split_axis=0, concat_axis=0)]
    *inside, inner_back, mixer_back = call(
        functools.partial(within, head_dim),
        None,
        [
            inner_pre,
            mixer_pre,
            step,
            decay,
            head_rows,
            upstream,
            inner_weight,
            mixer_weight,
        ],
        [
            shape(length, width),
            shape(length, mixed),
            shape(length, LANES),
            shape(LANES, length),
            shape(length, width),
            shape(length, width),
            shape(model, width, dtype=BF16),
            shape(model, mixed, dtype=BF16),
        ],
        [pltpu.SemaphoreType.DMA((2,))],
        plain=(6, 7),
        left=(6, 7),
    )
    if relative:
        (columns,) = call(
            pack, None, columns, [shape(seq_count, rows, dp_count * padded, dtype=BF16)], cost=1
        )
    all_columns = around(columns, "chan")
    turned, own_turned = call(
        turn,
        places,
        all_columns,
        [
            shape(dp_count * padded, seq_count * length, dtype=BF16),
            shape(dp_count * padded, seq_count * rows, dtype=BF16),
        ],
        [pltpu.VMEM((seq_count * length, dp_count * padded), BF16)],
    )

    pair, mixer_local, step_grad, early, *mixer_sent = call(
        functools.partial(finish, head_dim, relative, seq_count, chan_count),
        places,
        received
        + [inner_pre, mixer_pre, step, decay, step_raw, head_rows, upstream, conv_inner, conv_mixer]
        + list(inside),
        [
            shape(length + PAD, width, dtype=BF16),
            shape(length, mixed, dtype=BF16),
            shape(length, LANES, dtype=BF16),
            shape(PAD, width + mixed),
        ]
        + [shape(rows + PAD, mixed, dtype=BF16)] * chan_count,
        [pltpu.VMEM((length + 2 * PAD, width), F32), pltpu.VMEM((length + 2 * PAD, mixed), F32)],
        cost=5,
    )

    def over_seq(block):
        if relative:
            return around(block, "seq")
        return [lax.all_gather(block, "seq")]

    pairs = over_seq(pair)
    mixer_rows = list(mixer_sent[:1]) + [
        lax.ppermute(block, "chan", ring("chan", hop))
        for hop, block in enumerate(mixer_sent[1:], 1)
    ]
    (mixer_rows,) = call(add_up, None, mixer_rows, [shape(rows + PAD, mixed, dtype=BF16)], cost=1)
    mixers = over_seq(mixer_rows)

    sent = call(
        functools.partial(project_back, chan_count),
        places,
        [pair, early, mixer_local, step_grad, inner_back, mixer_back, step_near],
        [shape(rows + PAD, model, dtype=BF16)] * chan_count,
        [
            pltpu.VMEM((length + 2 * PAD, width + LANES), BF16),
            pltpu.VMEM((length + 2 * PAD, mixed), BF16),
            pltpu.VMEM((length + 2 * PAD, model), BF16),
        ],
        cost=4,
    )
    taken = list(sent[:1]) + [
        lax.ppermute(block, "chan", ring("chan", hop))
        for hop, block in enumerate(sent[1:], 1)
    ]

    groups = width // length
    used = -(-head_count // groups)
    step_lines = -(-used * groups // (2 * PAD)) * (2 * PAD)
    leaving, grads, steps = call(
        functools.partial(leave, relative, taps, used, grad_rows, norm_factor),
        places,
        [turned] + pairs,
        [
            shape(grad_rows + step_lines, width, dtype=BF16),
            shape(seq_count * length, width, dtype=BF16),
            shape(step_lines, seq_count * length, dtype=BF16),
        ],
    )
    arrived = lax.ppermute(leaving, "dp", ring("dp", 1))
    kept, kept_step = call(
        functools.partial(keep, grad_rows, norm_factor),
        None,
        [turned, grads, steps],
        [shape(grad_rows, width), shape(step_lines, padded)],
    )
    mixer_blocks = call(
        functools.partial(mix, relative, taps, grad_rows // chan_count, norm_factor, chan_count),
        places,
        [own_turned] + mixers,
        [shape(grad_rows // chan_count * dp_count, mixed, dtype=BF16)] * chan_count,
        [pltpu.VMEM((dp_count * padded, mixed), F32), pltpu.VMEM((seq_count * rows, mixed), BF16)],
        cost=2,
    )
    mixer_blocks = list(mixer_blocks[:1]) + [
        lax.ppermute(block, "chan", ring("chan", hop))
        for hop, block in enumerate(mixer_blocks[1:], 1)
    ]
    mixer_kept, mixer_leaving = call(
        add_chan,
        None,
        mixer_blocks,
        [shape(grad_rows // chan_count, mixed), shape(grad_rows // chan_count, mixed, dtype=BF16)],
        cost=1,
    )
    mixer_arrived = lax.ppermute(mixer_leaving, "dp", ring("dp", 1))
    (mixer_weight_grad,) = call(
        add_pair,
        None,
        [mixer_kept, mixer_arrived],
        [jax.ShapeDtypeStruct((grad_rows // chan_count, mixed), F32)],
        cost=1,
    )
    total, ending, back = call(
        gather_share,
        None,
        taken,
        [
            jax.ShapeDtypeStruct((rows, model), BF16),
            shape(PAD, model),
            shape(PAD, model, dtype=BF16),
        ],
        cost=1,
    )
    backward_pairs = [(source + 1, source) for source in range(seq_count - 1)]
    late = lax.ppermute(back, "seq", backward_pairs)
    (input_grad,) = call(
        functools.partial(close_share, taps, chan_count),
        places,
        [total, ending, late],
        [jax.ShapeDtypeStruct((rows, model), BF16)],
        [pltpu.VMEM((PAD, model), BF16), pltpu.SemaphoreType.DMA],
        cost=1,
        plain=(0,),
        left=(0,),
        in_place=True,
    )
    inner_weight_grad, step_weight_grad = call(
        functools.partial(last, used),
        None,
        [kept, kept_step, arrived],
        [
            jax.ShapeDtypeStruct((grad_rows, width), F32),
            jax.ShapeDtypeStruct((head_count, grad_rows), F32),
        ],
        cost=1,
    )
    step_weight_grad = step_weight_grad.T
    return (input_grad[None], inner_weight_grad, mixer_weight_grad, step_weight_grad)


def solution(mesh):
    in_specs = (
        P("dp", ("seq", "chan"), None),
        P(None, "chan"),
        P(),
        P(None, "chan"),
        P(None, "chan"),
        P(),
        P("chan"),
        P("chan"),
        P("chan"),
        P("dp", "seq", "chan"),
    )
    out_specs = (
        P("dp", ("seq", "chan"), None),
        P(("dp", "seq"), "chan"),
        P(("dp", "seq", "chan"), None),
        P(("dp", "seq"), "chan"),
    )
    return jax.shard_map(body, mesh=mesh, in_specs=in_specs, out_specs=out_specs, check_vma=False)
```

```python
import functools
import math

import jax
import jax.numpy as jnp
from jax import lax
from jax.experimental import pallas as pl
from jax.experimental.pallas import tpu as pltpu
from jax.sharding import PartitionSpec as P


F32 = jnp.float32
BF16 = jnp.bfloat16
LANES = 128
PAD = 8
DIRECT = 8


def dot(left, right, left_dim=1, right_dim=0):
    return lax.dot_general(
        left,
        right,
        (((left_dim,), (right_dim,)), ((), ())),
        preferred_element_type=F32,
    )


def pieces(values):
    high = values.astype(BF16)
    rest = values - high.astype(F32)
    middle = rest.astype(BF16)
    low = (rest - middle.astype(F32)).astype(BF16)
    return high, middle, low


def fine(left, right, left_dim=1, right_dim=0):
    left_high = left.astype(BF16)
    left_low = (left - left_high.astype(F32)).astype(BF16)
    right_high = right.astype(BF16)
    right_low = (right - right_high.astype(F32)).astype(BF16)
    lefts = jnp.concatenate([left_high, left_low, left_high], axis=left_dim)
    rights = jnp.concatenate([right_high, right_high, right_low], axis=right_dim)
    return dot(lefts, rights, left_dim, right_dim)


def half_fine(left, right, left_dim=1, right_dim=0):
    high = left.astype(BF16)
    low = (left - high.astype(F32)).astype(BF16)
    rounded = right.astype(BF16)
    lefts = jnp.concatenate([high, low], axis=left_dim)
    return dot(lefts, jnp.concatenate([rounded, rounded], axis=right_dim), left_dim, right_dim)


def masked_sum(mask, values, values_dim=0):
    chosen = jnp.where(mask, 1.0, 0.0).astype(BF16)
    masks = jnp.concatenate([chosen] * 3, axis=1)
    return dot(masks, jnp.concatenate(pieces(values), axis=values_dim), 1, values_dim)


def head_map(width, head_dim):
    row = lax.broadcasted_iota(jnp.int32, (LANES, width), 0)
    column = lax.broadcasted_iota(jnp.int32, (LANES, width), 1)
    start = row * head_dim
    return jnp.where((column >= start) & (column < start + head_dim), 1.0, 0.0).astype(BF16)


def spread(values, heads):
    return dot(jnp.concatenate(pieces(values), axis=1), jnp.concatenate([heads] * 3, axis=0))


def collect(values, heads):
    high, middle, _ = pieces(values)
    return dot(high, heads, 1, 1) + dot(middle, heads, 1, 1)


def sigmoid(values):
    return 1.0 / (1.0 + jnp.exp(-values))


def softplus(values):
    small = jnp.exp(-jnp.abs(values))
    series = small * (1.0 - small * (0.5 - small * (1.0 / 3.0)))
    return jnp.maximum(values, 0.0) + jnp.where(small < 1e-3, series, jnp.log(1.0 + small))


def triangle(length):
    row = lax.broadcasted_iota(jnp.int32, (length, length), 0)
    column = lax.broadcasted_iota(jnp.int32, (length, length), 1)
    return row, column


def convolve(values, history, kernel, scratch):
    length = values.shape[0]
    taps = kernel.shape[0]
    scratch[:PAD] = history.astype(F32)
    scratch[PAD:] = values.astype(F32)
    total = kernel[taps - 1 : taps] * scratch[PAD : PAD + length]
    for tap in range(taps - 1):
        start = PAD - (taps - 1) + tap
        total = total + kernel[tap : tap + 1] * scratch[start : start + length]
    return total


def convolve_back(gradient, kernel, scratch):
    length = gradient.shape[0]
    taps = kernel.shape[0]
    zeros = jnp.zeros((PAD, gradient.shape[1]), F32)
    scratch[:PAD] = zeros
    scratch[PAD : PAD + length] = gradient
    scratch[PAD + length :] = zeros
    extent = length + PAD
    total = None
    for tap in range(taps):
        start = taps - 1 - tap
        term = kernel[tap : tap + 1] * scratch[start : start + extent]
        total = term if total is None else total + term
    return total


def blocks(rows, padded, dp_count, relative, place_ref, *refs):
    own_ref, step_ref, bias_ref, log_ref, skip_ref, inner_ref, mixer_ref = refs[:7]
    own_out_ref, step_out_ref, head_ref, inner_out_ref, mixer_out_ref = refs[7:12]
    out_refs, scratch, wide, sems = refs[12:-3], refs[-3], refs[-2], refs[-1]
    parts = sems.shape[1]
    depth = inner_ref.shape[0] // parts
    copies = []
    for part in range(parts):
        span = pl.ds(part * depth, depth)
        pair = ((inner_ref, inner_out_ref), (mixer_ref, mixer_out_ref))
        for number, (source, target) in enumerate(pair):
            copy = pltpu.make_async_copy(source.at[span], target.at[span], sems.at[number, part])
            copy.start()
            copies.append(copy)
    own_out_ref[...] = own_ref[...]
    head_count = bias_ref.shape[1]
    wide[...] = jnp.zeros_like(wide)
    wide[:head_count] = step_ref[...].astype(F32)
    step_out_ref[...] = wide[...].T.astype(BF16)
    head_ref[...] = jnp.zeros_like(head_ref)
    head_ref[0:1, :head_count] = bias_ref[...]
    head_ref[1:2, :head_count] = log_ref[...]
    head_ref[2:3, :head_count] = skip_ref[...]
    dp_place = place_ref[1]
    seq_count = scratch.shape[0]
    fill = jnp.zeros((own_ref.shape[0], padded - rows), F32)
    for target in range(seq_count):
        for hop in range(dp_count):
            wanted = lax.rem(dp_place + hop, dp_count)
            chosen = None
            for other in range(dp_count):
                start = (other * seq_count + target) * rows
                part = own_ref[:, start : start + rows].astype(F32)
                chosen = part if chosen is None else jnp.where(wanted == other, part, chosen)
            span = slice(hop * padded, (hop + 1) * padded)
            if padded > rows:
                chosen = jnp.concatenate([chosen, fill], axis=1)
            scratch[target, :, span] = chosen.astype(BF16)
    if relative:
        for hop, out_ref in enumerate(out_refs):
            out_ref[...] = scratch[lax.rem(place_ref[0] + hop, seq_count)]
    else:
        out_refs[0][...] = scratch[...]
    for copy in copies:
        copy.wait()


def copied(sources, targets, sems):
    copies = [
        pltpu.make_async_copy(source, target, sems.at[number])
        for number, (source, target) in enumerate(zip(sources, targets))
    ]
    for copy in copies:
        copy.start()
    return copies


def pack(*refs):
    for number, ref in enumerate(refs[:-1]):
        refs[-1][number] = ref[...]


def add_up(*refs):
    total = refs[0][...].astype(F32)
    for part in refs[1:-1]:
        total = total + part[...].astype(F32)
    refs[-1][...] = total.astype(refs[-1].dtype)


def project(count, place_ref, *refs):
    tokens = refs[:count]
    inner_ref, mixer_ref, step_ref, inner_out, mixer_out, raw_out, tail_out, scratch = refs[count:]
    place = place_ref[2]
    rows = tokens[0].shape[0]
    for hop in range(count):
        source = lax.bitwise_xor(place, hop)
        scratch[pl.ds(pl.multiple_of(source * rows, rows), rows)] = tokens[hop][...]
    gathered = scratch[...]
    length = gathered.shape[0]
    width = inner_ref.shape[1]
    whole = width // (2 * LANES) * (2 * LANES)
    mixer = dot(gathered, mixer_ref[...]).astype(BF16)
    first = dot(gathered, inner_ref[:, :whole])
    joined = jnp.concatenate([inner_ref[:, whole:], step_ref[...]], axis=1)
    second = dot(gathered, joined)
    raw_out[...] = second[:, width - whole :]
    inner = jnp.concatenate([first, second[:, : width - whole]], axis=1).astype(BF16)
    inner_out[...] = inner
    mixer_out[...] = mixer
    tail_out[:, :width] = inner[length - 2 * PAD :]
    tail_out[:, width:] = mixer[length - 2 * PAD :]


def prepare(head_dim, relative, place_ref, *refs):
    (
        inner_ref,
        mixer_ref,
        history_ref,
        raw_ref,
        head_ref,
        upstream_ref,
        conv_inner_ref,
        conv_mixer_ref,
        inner_pre_ref,
        mixer_pre_ref,
        step_ref,
        decay_ref,
    ) = refs[:12]
    message_refs = refs[12:-2]
    inner_scratch, mixer_scratch = refs[-2:]
    length, width = inner_ref.shape
    state = mixer_ref.shape[1] // 2
    place = place_ref[0]
    history = history_ref[...].astype(F32)[PAD:]
    inner_pre = convolve(inner_ref[...], history[:, :width], conv_inner_ref[...], inner_scratch)
    mixer_pre = convolve(mixer_ref[...], history[:, width:], conv_mixer_ref[...], mixer_scratch)
    inner_pre_ref[...] = inner_pre
    mixer_pre_ref[...] = mixer_pre
    inner_act = inner_pre * sigmoid(inner_pre)
    mixer_act = mixer_pre * sigmoid(mixer_pre)
    step = softplus(raw_ref[...] + head_ref[0:1])
    log_decay = -step * jnp.exp(head_ref[1:2])
    row, column = triangle(length)
    decay = masked_sum(row >= column, log_decay)
    step_ref[...] = step
    decay_ref[...] = decay
    heads = head_map(width, head_dim)
    last = decay[length - 1 : length]
    tail = spread(jnp.exp(last - decay) * step, heads)
    lead = spread(jnp.exp(decay), heads)
    upstream = upstream_ref[...].astype(F32)
    forward = half_fine(mixer_act[:, :state].T, tail * inner_act).astype(BF16)
    backward = half_fine(mixer_act[:, state:].T, lead * upstream).astype(BF16)
    high, middle, low = pieces(last)
    kinds = (high.astype(F32), middle.astype(F32), low.astype(F32))
    index = lax.broadcasted_iota(jnp.int32, (PAD, LANES), 0)
    stacked = jnp.zeros((PAD, LANES), F32)
    for number, kind in enumerate(kinds):
        stacked = jnp.where(index == number, kind, stacked)
    extra = dot(stacked.astype(BF16), heads).astype(BF16)
    if relative:
        count = len(message_refs) + 1
        for hop, message_ref in enumerate(message_refs, 1):
            message_ref[:state] = jnp.where(place + hop < count, forward, backward)
            message_ref[state:] = extra
    else:
        message_ref = message_refs[0]
        for target in range(message_ref.shape[0]):
            message_ref[target, :state] = jnp.where(target > place, forward, backward)
            message_ref[target, state:] = extra


def within(
    head_dim,
    inner_pre_ref,
    mixer_pre_ref,
    step_ref,
    decay_ref,
    head_ref,
    upstream_ref,
    inner_weight_ref,
    mixer_weight_ref,
    inner_grad_ref,
    mixer_grad_ref,
    row_ref,
    column_ref,
    lead_ref,
    tail_ref,
    inner_near_ref,
    mixer_near_ref,
    sems,
):
    copies = copied(
        (inner_weight_ref, mixer_weight_ref), (inner_near_ref, mixer_near_ref), sems
    )
    length, width = inner_pre_ref.shape
    state = mixer_pre_ref.shape[1] // 2
    mixer_pre = mixer_pre_ref[...]
    mixer_act = mixer_pre * sigmoid(mixer_pre)
    input_mix = mixer_act[:, :state]
    output_mix = mixer_act[:, state:]
    decay = decay_ref[...]
    step = step_ref[...]
    turned = decay.T
    row, column = triangle(length)
    causal = column >= row
    scores = fine(input_mix, output_mix, 1, 1)
    heads = head_map(width, head_dim)
    skip = spread(head_ref[...], heads)[2:3]
    step_wide = spread(step, heads)
    lead_ref[...] = spread(jnp.exp(decay), heads)
    tail_ref[...] = spread(jnp.exp(decay[length - 1 : length] - decay) * step, heads)
    group_heads = LANES // head_dim
    lane = lax.broadcasted_iota(jnp.int32, (length, LANES), 1)
    mixed = jnp.zeros((length, length), F32)
    rows = jnp.zeros((length, LANES), F32)
    columns = []
    for group in range(width // LANES):
        span = slice(group * LANES, (group + 1) * LANES)
        inner_pre = inner_pre_ref[:, span]
        inner_act = inner_pre * sigmoid(inner_pre)
        high = inner_act.astype(BF16)
        low = (inner_act - high.astype(F32)).astype(BF16)
        upstream = upstream_ref[:, span]
        total = None
        for member in range(group_heads):
            head = group * group_heads + member
            mine = (lane >= member * head_dim) & (lane < (member + 1) * head_dim)
            mine_upstream = jnp.where(mine, upstream.astype(F32), 0.0).astype(BF16)
            spread_of = turned[head : head + 1] - decay[:, head : head + 1]
            fall = jnp.exp(jnp.where(causal, spread_of, -1e30))
            match = dot(high, mine_upstream, 1, 1) + dot(low, mine_upstream, 1, 1)
            weight = fall * scores
            cross = weight * match
            step_column = step[:, head : head + 1]
            mixed = mixed + step_column * (fall * match)
            rows = jnp.where(lane == head, jnp.sum(cross, axis=1, keepdims=True), rows)
            columns.append(jnp.sum(step_column * cross, axis=0, keepdims=True))
            weight_high = weight.astype(BF16)
            weight_low = (weight - weight_high.astype(F32)).astype(BF16)
            term = dot(weight_high, mine_upstream) + dot(weight_low, mine_upstream)
            total = term if total is None else total + term
        inner_grad_ref[:, span] = step_wide[:, span] * total + skip[:, span] * upstream.astype(F32)
    mixer_grad_ref[:, :state] = fine(mixed, output_mix)
    mixer_grad_ref[:, state:] = fine(mixed.T, input_mix)
    row_ref[...] = rows
    index = lax.broadcasted_iota(jnp.int32, (LANES, length), 0)
    stacked = jnp.zeros((LANES, length), F32)
    for number, kind in enumerate(columns):
        stacked = jnp.where(index == number, kind, stacked)
    column_ref[...] = stacked
    for copy in copies:
        copy.wait()


def finish(
    head_dim,
    relative,
    count,
    chan_count,
    place_ref,
    *refs,
):
    messages = refs[: count - 1] if relative else refs[:1]
    inner_scratch, mixer_scratch = refs[-2:]
    mixer_sent_refs = refs[-2 - chan_count : -2]
    refs = refs[len(messages) : -2 - chan_count]
    (
        inner_pre_ref,
        mixer_pre_ref,
        step_ref,
        decay_ref,
        raw_ref,
        head_ref,
        upstream_ref,
        conv_inner_ref,
        conv_mixer_ref,
        inner_grad_ref,
        mixer_grad_ref,
        row_ref,
        column_ref,
        lead_ref,
        tail_ref,
        pair_ref,
        mixer_out_ref,
        step_out_ref,
        early_ref,
    ) = refs
    length, width = inner_pre_ref.shape
    state = mixer_pre_ref.shape[1] // 2
    place = place_ref[0]

    def message(hop):
        if relative:
            return messages[hop - 1][...].astype(F32)
        return messages[0][lax.rem(place - hop + count, count)].astype(F32)

    def shard_decay(parts):
        return parts[state : state + 1] + parts[state + 1 : state + 2] + parts[state + 2 : state + 3]

    start = jnp.zeros((state, width), F32)
    running = jnp.zeros((1, width), F32)
    end = jnp.zeros((state, width), F32)
    if relative:
        received = [None] + [message(hop) for hop in range(1, count)]
        back_running = jnp.zeros((1, width), F32)
        for hop in range(1, count):
            factor = jnp.where(hop <= place, jnp.exp(running), 0.0)
            start = start + factor * received[hop][:state]
            running = running + shard_decay(received[hop])
            other = count - hop
            factor = jnp.where(other > place, jnp.exp(back_running), 0.0)
            end = end + factor * received[other][:state]
            back_running = back_running + shard_decay(received[other])
    else:

        def before(hop, carried):
            start, running = carried
            parts = message(hop)
            return start + jnp.exp(running) * parts[:state], running + shard_decay(parts)

        def after(step, carried):
            end, running = carried
            parts = message(count - step)
            return end + jnp.exp(running) * parts[:state], running + shard_decay(parts)

        start, unused = lax.fori_loop(1, place + 1, before, (start, running))
        end, unused = lax.fori_loop(1, count - place, after, (end, running))

    inner_pre = inner_pre_ref[...]
    mixer_pre = mixer_pre_ref[...]
    inner_sig = sigmoid(inner_pre)
    mixer_sig = sigmoid(mixer_pre)
    inner_act = inner_pre * inner_sig
    mixer_act = mixer_pre * mixer_sig
    input_mix = mixer_act[:, :state]
    output_mix = mixer_act[:, state:]
    decay = decay_ref[...]
    step = step_ref[...]
    upstream = upstream_ref[...].astype(F32)
    heads = head_map(width, head_dim)
    last = decay[length - 1 : length]
    lead = jnp.exp(decay)
    rest = jnp.exp(last - decay)
    lead_wide = lead_ref[...]
    tail_wide = tail_ref[...]
    from_end = half_fine(input_mix, end)
    from_start = half_fine(output_mix, start)
    inner_grad = inner_grad_ref[...] + tail_wide * from_end
    input_grad = mixer_grad_ref[:, :state] + half_fine(tail_wide * inner_act, end, 1, 1)
    output_grad = mixer_grad_ref[:, state:] + half_fine(lead_wide * upstream, start, 1, 1)
    end_part = rest * collect(inner_act * from_end, heads)
    start_part = lead * collect(upstream * from_start, heads)
    product = jnp.sum(end * start, axis=0, keepdims=True)
    product = collect(jnp.broadcast_to(product, (PAD, width)), heads)[0:1]
    step_grad = row_ref[...] + end_part
    sums = start_part - step * step_grad
    total = jnp.sum(step * end_part, axis=0, keepdims=True) + jnp.exp(last) * product
    row, column = triangle(length)
    after_row = column >= row
    decay_grad = masked_sum(after_row, sums) + masked_sum(after_row, column_ref[...], 1) + total
    step_grad = step_grad - jnp.exp(head_ref[1:2]) * decay_grad
    raw_grad = step_grad * sigmoid(raw_ref[...] + head_ref[0:1])
    step_out_ref[...] = raw_grad.astype(BF16)
    turned = raw_grad.T
    groups = width // length
    packed = jnp.zeros((PAD, width), F32)
    index = lax.broadcasted_iota(jnp.int32, (PAD, width), 0)
    head_count = width // head_dim
    for number in range(-(-head_count // groups)):
        line = [turned[number * groups + group : number * groups + group + 1] for group in range(groups)]
        packed = jnp.where(index == number, jnp.concatenate(line, axis=1), packed)
    inner_slope = inner_sig * (1.0 + inner_pre * (1.0 - inner_sig))
    mixer_slope = mixer_sig * (1.0 + mixer_pre * (1.0 - mixer_sig))
    inner_total = convolve_back(inner_grad * inner_slope, conv_inner_ref[...], inner_scratch)
    mixer_total = jnp.concatenate([input_grad, output_grad], axis=1) * mixer_slope
    mixer_total = convolve_back(mixer_total, conv_mixer_ref[...], mixer_scratch)
    taps = conv_inner_ref.shape[0] - 1
    early = PAD - taps
    inner_scratch[:PAD] = jnp.where(index >= early, inner_total[:PAD], packed)
    early_ref[:, :width] = inner_total[:PAD]
    early_ref[:, width:] = mixer_total[:PAD]
    pair_ref[:length] = inner_total[PAD:].astype(BF16)
    pair_ref[length:] = inner_scratch[:PAD].astype(BF16)
    mixer_out_ref[...] = mixer_total[PAD:].astype(BF16)
    rows = length // chan_count
    back = mixer_total[:PAD].astype(BF16)
    mixer_scratch[:length] = mixer_total[PAD:]
    for hop, sent_ref in enumerate(mixer_sent_refs):
        target = lax.rem(place_ref[2] + hop, chan_count)
        start = pl.multiple_of(target * rows, rows)
        sent_ref[:rows] = mixer_scratch[pl.ds(start, rows)].astype(BF16)
        sent_ref[rows:] = back


def add_late(ending, extra, taps, valid):
    index = lax.broadcasted_iota(jnp.int32, ending.shape, 0)
    late = jnp.where((index >= PAD - taps) & valid, extra, 0.0)
    return ending + late


def project_back(
    chan_count,
    place_ref,
    pair_ref,
    early_ref,
    mixer_ref,
    step_ref,
    inner_weight_ref,
    mixer_weight_ref,
    step_weight_ref,
    *refs,
):
    out_refs = refs[:chan_count]
    inner_scratch, mixer_scratch, share_scratch = refs[chan_count:]
    length, mixed = mixer_ref.shape
    width = pair_ref.shape[1]
    rows = length // chan_count
    whole = width // (2 * LANES) * (2 * LANES)
    fill = jnp.zeros((PAD, width + mixed), F32)
    early = jnp.concatenate([early_ref[...], fill], axis=0).astype(BF16)
    inner_scratch[:length, :width] = pair_ref[:length]
    inner_scratch[:length, width:] = step_ref[...]
    inner_scratch[length:, :width] = early[:, :width]
    inner_scratch[length:, width:] = jnp.zeros((2 * PAD, LANES), BF16)
    mixer_scratch[:length] = mixer_ref[...]
    mixer_scratch[length:] = early[:, width:]
    share = dot(inner_scratch[:, :whole], inner_weight_ref[:, :whole], 1, 1)
    right = jnp.concatenate([inner_weight_ref[:, whole:], step_weight_ref[...]], axis=1)
    share = share + dot(inner_scratch[:, whole:], right, 1, 1)
    share = share + dot(mixer_scratch[...], mixer_weight_ref[...], 1, 1)
    share_scratch[...] = share.astype(BF16)
    for hop, out_ref in enumerate(out_refs):
        target = lax.rem(place_ref[2] + hop, chan_count)
        start = pl.multiple_of(target * rows, rows)
        out_ref[:rows] = share_scratch[pl.ds(start, rows)]
        out_ref[rows:] = share_scratch[length : length + PAD]


def gather_share(*refs):
    total_ref, ending_ref, back_ref = refs[-3:]
    total = refs[0][...].astype(F32)
    for part in refs[1:-3]:
        total = total + part[...].astype(F32)
    rows = total_ref.shape[0]
    total_ref[...] = total[:rows].astype(BF16)
    ending_ref[...] = total[rows - PAD : rows]
    back_ref[...] = total[rows:].astype(BF16)


def close(
    taps,
    chan_count,
    used,
    place_ref,
    kept_ref,
    step_ref,
    arrived_ref,
    total_ref,
    ending_ref,
    late_ref,
    mixer_kept_ref,
    mixer_arrived_ref,
    inner_out_ref,
    step_out_ref,
    input_out_ref,
    mixer_out_ref,
    scratch,
    done,
):
    del total_ref
    valid = place_ref[2] == chan_count - 1
    ending = add_late(ending_ref[...], late_ref[...].astype(F32), taps, valid)
    scratch[...] = ending.astype(BF16)
    head = input_out_ref.shape[0] - PAD
    copy = pltpu.make_async_copy(scratch, input_out_ref.at[pl.ds(head, PAD)], done)
    copy.start()
    rows = kept_ref.shape[0]
    inner_out_ref[...] = kept_ref[...] + arrived_ref[:rows].astype(F32)
    mixer_out_ref[...] = mixer_kept_ref[...] + mixer_arrived_ref[...].astype(F32)
    step = step_ref[:, :rows] + arrived_ref[rows:, :rows].astype(F32)
    head_count = step_out_ref.shape[0]
    groups = -(-head_count // used)
    for head in range(head_count):
        line = (head % groups) * used + head // groups
        step_out_ref[head : head + 1] = step[line : line + 1]
    copy.wait()


def turn(place_ref, *refs):
    column_refs, out_ref, own_ref, columns = refs[:-3], refs[-3], refs[-2], refs[-1]
    chan_place = place_ref[2]
    chan_count = len(column_refs)
    seq_count, rows, _ = column_refs[0].shape
    length = chan_count * rows
    for hop in range(seq_count):
        for chan_hop in range(chan_count):
            chan_source = lax.rem(chan_place - chan_hop + chan_count, chan_count)
            start = pl.multiple_of(hop * length + chan_source * rows, rows)
            columns[pl.ds(start, rows)] = column_refs[chan_hop][hop]
    out_ref[...] = columns[...].T
    own = [column_refs[0][hop] for hop in range(seq_count)]
    own_ref[...] = jnp.concatenate(own, axis=0).T


def arrange(relative, taps, used, place_ref, pair_refs, grads, steps):
    seq_place = place_ref[0]
    seq_count = len(pair_refs) if relative else pair_refs[0].shape[0]
    length = grads.shape[0] // seq_count

    def message(hop):
        return pair_refs[hop][...] if relative else pair_refs[0][hop]

    for hop in range(seq_count):
        if relative:
            shard = lax.rem(seq_place - hop + seq_count, seq_count)
            after = (hop - 1) % seq_count
        else:
            shard = hop
            after = (hop + 1) % seq_count
        pair = message(hop)
        start = hop * length
        head = length - PAD
        grads[start : start + head] = pair[:head]
        extra = message(after)[length:].astype(F32)
        ending = add_late(pair[head:length].astype(F32), extra, taps, shard < seq_count - 1)
        grads[start + head : start + length] = ending.astype(BF16)
        packed = pair[length:].astype(F32)
        groups = packed.shape[1] // length
        lines = [packed[:used, group * length : (group + 1) * length] for group in range(groups)]
        spare = steps.shape[0] - used * groups
        lines = lines + [jnp.zeros((spare, length), F32)]
        steps[:, start : start + length] = jnp.concatenate(lines, axis=0).astype(BF16)


def leave(relative, taps, used, rows, scale, place_ref, *refs):
    turned_ref = refs[0]
    out_ref, grads, steps = refs[-3:]
    arrange(relative, taps, used, place_ref, refs[1:-3], grads, steps)
    padded = turned_ref.shape[0] // 2
    chosen = turned_ref[padded : padded + rows]
    out_ref[:rows] = (dot(chosen, grads[...]) * scale).astype(BF16)
    lines = steps.shape[0]
    term = dot(steps[...], turned_ref[padded:], 1, 1) * scale
    out_ref[rows:, :padded] = term.astype(BF16)
    out_ref[rows:, padded:] = jnp.zeros((lines, out_ref.shape[1] - padded), BF16)


def keep(rows, scale, turned_ref, grads_ref, steps_ref, out_ref, step_ref):
    padded = turned_ref.shape[0] // 2
    out_ref[...] = dot(turned_ref[:rows], grads_ref[...]) * scale
    step_ref[...] = dot(steps_ref[...], turned_ref[:padded], 1, 1) * scale


def mix(relative, taps, rows, scale, chan_count, place_ref, *refs):
    column_ref, scratch, grads = refs[0], refs[-2], refs[-1]
    grad_refs = refs[1 : -2 - chan_count]
    out_refs = refs[-2 - chan_count : -2]
    seq_place = place_ref[0]
    chan_place = place_ref[2]
    wide = column_ref.shape[0]
    seq_count = len(grad_refs) if relative else grad_refs[0].shape[0]
    tokens = grads.shape[0] // seq_count

    def message(hop):
        return grad_refs[hop][...] if relative else grad_refs[0][hop]

    for hop in range(seq_count):
        if relative:
            source = lax.rem(seq_place - hop + seq_count, seq_count)
            after = (hop - 1) % seq_count
        else:
            source = hop
            after = (hop + 1) % seq_count
        start = hop * tokens
        head = tokens - PAD
        block = message(hop)
        grads[start : start + head] = block[:head]
        valid = (source < seq_count - 1) & (chan_place == chan_count - 1)
        extra = message(after)[tokens:].astype(F32)
        ending = add_late(block[head:tokens].astype(F32), extra, taps, valid)
        grads[start + head : start + tokens] = ending.astype(BF16)
    padded = wide // 2
    scratch[...] = dot(column_ref[...], grads[...]) * scale
    for hop, out_ref in enumerate(out_refs):
        target = lax.rem(chan_place + hop, chan_count)
        for dp_hop in range(2):
            start = pl.multiple_of(dp_hop * padded + target * rows, PAD)
            part = scratch[pl.ds(start, rows)]
            out_ref[dp_hop * rows : (dp_hop + 1) * rows] = part.astype(BF16)


def add_chan(*refs):
    kept_ref, leaving_ref = refs[-2:]
    total = refs[0][...].astype(F32)
    for part in refs[1:-2]:
        total = total + part[...].astype(F32)
    rows = kept_ref.shape[0]
    kept_ref[...] = total[:rows]
    leaving_ref[...] = total[rows:].astype(BF16)


def shape(*dims, dtype=F32):
    return pltpu.VMEM(dims, dtype)


def ring(axis, hop):
    count = lax.axis_size(axis)
    return [(source, (source + hop) % count) for source in range(count)]


def call(body, place, arrays, out_shape, scratch=(), cost=3, plain=(), left=(), in_place=None):
    vmem = pltpu.MemorySpace.VMEM
    hbm = pltpu.MemorySpace.HBM
    arrays = [
        pltpu.with_memory_space_constraint(array, hbm if number in plain else vmem)
        for number, array in enumerate(arrays)
    ]
    in_specs = [
        pl.BlockSpec(memory_space=hbm if number in left else vmem) for number in range(len(arrays))
    ]
    out_specs = [
        pl.BlockSpec(memory_space=hbm if in_place and in_place[1] == number else vmem)
        for number in range(len(out_shape))
    ]
    if place is not None:
        in_specs = [pl.BlockSpec(memory_space=pltpu.SMEM)] + in_specs
        arrays = [place] + arrays
    return pl.pallas_call(
        body,
        out_shape=out_shape,
        in_specs=in_specs,
        out_specs=out_specs,
        scratch_shapes=list(scratch),
        input_output_aliases={in_place[0] + 1: in_place[1]} if in_place else {},
        cost_estimate=pl.CostEstimate(flops=cost * 10**8, bytes_accessed=0, transcendentals=0),
        compiler_params=pltpu.CompilerParams(vmem_limit_bytes=24 * 2**20),
    )(*arrays)


def around(block, axis):
    count = lax.axis_size(axis)
    return [block] + [
        lax.ppermute(block, axis, ring(axis, hop)) for hop in range(1, count)
    ]


def spread_out(block, axis):
    count = lax.axis_size(axis)
    parts = {0: block}
    bit = count // 2
    while bit:
        pairs = [(source, source ^ bit) for source in range(count)]
        for number in list(parts):
            parts[number | bit] = lax.ppermute(parts[number], axis, pairs)
        bit //= 2
    return [parts[number] for number in range(count)]


def body(
    layer_input,
    inner_weight,
    mixer_weight,
    step_weight,
    conv_inner,
    conv_mixer,
    step_bias,
    decay_log,
    skip_gain,
    output_grad,
):
    own = layer_input[0]
    dp_count = lax.axis_size("dp")
    seq_count = lax.axis_size("seq")
    chan_count = lax.axis_size("chan")
    place = lax.axis_index("seq")
    relative = seq_count <= DIRECT
    rows, model = own.shape
    length = rows * chan_count
    width = inner_weight.shape[1]
    head_count = step_bias.shape[0]
    head_dim = width // head_count
    mixed = mixer_weight.shape[1]
    state = mixed // 2
    upstream = output_grad[0]
    grad_rows = model // (dp_count * seq_count)
    padded = -(-grad_rows // (2 * PAD)) * (2 * PAD)
    taps = conv_inner.shape[0] - 1
    parts = next(count for count in (4, 2, 1) if model % (count * LANES) == 0)
    places = [place, lax.axis_index("dp"), lax.axis_index("chan")]
    places = jnp.stack(places).astype(jnp.int32)
    norm_factor = 1.0 / math.sqrt(length * seq_count * dp_count)

    gathered = spread_out(own, "chan")
    if relative:
        column_shapes = [shape(rows, dp_count * padded, dtype=BF16)] * seq_count
    else:
        column_shapes = [shape(seq_count, rows, dp_count * padded, dtype=BF16)]
    own_near, step_near, head_rows, inner_near, mixer_near, *sorted_columns = call(
        functools.partial(blocks, grad_rows, padded, dp_count, relative),
        places,
        [
            own,
            step_weight.T,
            step_bias[None],
            decay_log[None],
            skip_gain[None],
            inner_weight,
            mixer_weight,
        ],
        [
            shape(rows, model, dtype=BF16),
            shape(model, LANES, dtype=BF16),
            shape(PAD, LANES),
            shape(model, width, dtype=BF16),
            shape(model, mixed, dtype=BF16),
        ]
        + column_shapes,
        [
            pltpu.VMEM((seq_count, rows, dp_count * padded), BF16),
            pltpu.VMEM((LANES, model), F32),
            pltpu.SemaphoreType.DMA((2, parts)),
        ],
        cost=1,
        plain=range(7),
        left=(5, 6),
    )
    if relative:
        columns = [sorted_columns[0]]
        for hop, block in enumerate(sorted_columns[1:], 1):
            columns.append(lax.ppermute(block, "seq", ring("seq", hop)))
    else:
        columns = lax.all_to_all(sorted_columns[0], "seq", split_axis=0, concat_axis=0)
    inner_proj, mixer_proj, step_raw, tail = call(
        functools.partial(project, chan_count),
        places,
        [own_near] + gathered[1:] + [inner_near, mixer_near, step_near],
        [
            shape(length, width, dtype=BF16),
            shape(length, mixed, dtype=BF16),
            shape(length, LANES),
            shape(2 * PAD, width + mixed, dtype=BF16),
        ],
        [pltpu.VMEM((length, model), BF16)],
        cost=4,
    )
    forward_pairs = [(source, source + 1) for source in range(seq_count - 1)]
    history = lax.ppermute(tail, "seq", forward_pairs)

    if relative:
        message_shapes = [shape(state + PAD, width, dtype=BF16)] * (seq_count - 1)
    else:
        message_shapes = [shape(seq_count, state + PAD, width, dtype=BF16)]
    inner_pre, mixer_pre, step, decay, *messages = call(
        functools.partial(prepare, head_dim, relative),
        places,
        [inner_proj, mixer_proj, history, step_raw, head_rows, upstream, conv_inner, conv_mixer],
        [
            shape(length, width),
            shape(length, mixed),
            shape(length, LANES),
            shape(length, LANES),
        ]
        + message_shapes,
        [pltpu.VMEM((PAD + length, width), F32), pltpu.VMEM((PAD + length, mixed), F32)],
    )
    if relative:
        received = [
            lax.ppermute(message, "seq", ring("seq", hop))
            for hop, message in enumerate(messages, 1)
        ]
    else:
        received = [lax.all_to_all(messages[0], "seq", split_axis=0, concat_axis=0)]
    *inside, inner_back, mixer_back = call(
        functools.partial(within, head_dim),
        None,
        [
            inner_pre,
            mixer_pre,
            step,
            decay,
            head_rows,
            upstream,
            inner_weight,
            mixer_weight,
        ],
        [
            shape(length, width),
            shape(length, mixed),
            shape(length, LANES),
            shape(LANES, length),
            shape(length, width),
            shape(length, width),
            shape(model, width, dtype=BF16),
            shape(model, mixed, dtype=BF16),
        ],
        [pltpu.SemaphoreType.DMA((2,))],
        plain=(6, 7),
        left=(6, 7),
    )
    if relative:
        (columns,) = call(
            pack, None, columns, [shape(seq_count, rows, dp_count * padded, dtype=BF16)], cost=1
        )
    all_columns = around(columns, "chan")
    turned, own_turned = call(
        turn,
        places,
        all_columns,
        [
            shape(dp_count * padded, seq_count * length, dtype=BF16),
            shape(dp_count * padded, seq_count * rows, dtype=BF16),
        ],
        [pltpu.VMEM((seq_count * length, dp_count * padded), BF16)],
    )

    pair, mixer_local, step_grad, early, *mixer_sent = call(
        functools.partial(finish, head_dim, relative, seq_count, chan_count),
        places,
        received
        + [inner_pre, mixer_pre, step, decay, step_raw, head_rows, upstream, conv_inner, conv_mixer]
        + list(inside),
        [
            shape(length + PAD, width, dtype=BF16),
            shape(length, mixed, dtype=BF16),
            shape(length, LANES, dtype=BF16),
            shape(PAD, width + mixed),
        ]
        + [shape(rows + PAD, mixed, dtype=BF16)] * chan_count,
        [pltpu.VMEM((length + 2 * PAD, width), F32), pltpu.VMEM((length + 2 * PAD, mixed), F32)],
        cost=5,
    )

    def over_seq(block):
        if relative:
            return around(block, "seq")
        return [lax.all_gather(block, "seq")]

    pairs = over_seq(pair)
    mixer_rows = list(mixer_sent[:1]) + [
        lax.ppermute(block, "chan", ring("chan", hop))
        for hop, block in enumerate(mixer_sent[1:], 1)
    ]
    (mixer_rows,) = call(add_up, None, mixer_rows, [shape(rows + PAD, mixed, dtype=BF16)], cost=1)
    mixers = over_seq(mixer_rows)

    sent = call(
        functools.partial(project_back, chan_count),
        places,
        [pair, early, mixer_local, step_grad, inner_back, mixer_back, step_near],
        [shape(rows + PAD, model, dtype=BF16)] * chan_count,
        [
            pltpu.VMEM((length + 2 * PAD, width + LANES), BF16),
            pltpu.VMEM((length + 2 * PAD, mixed), BF16),
            pltpu.VMEM((length + 2 * PAD, model), BF16),
        ],
        cost=4,
    )
    taken = list(sent[:1]) + [
        lax.ppermute(block, "chan", ring("chan", hop))
        for hop, block in enumerate(sent[1:], 1)
    ]

    groups = width // length
    used = -(-head_count // groups)
    step_lines = -(-used * groups // (2 * PAD)) * (2 * PAD)
    leaving, grads, steps = call(
        functools.partial(leave, relative, taps, used, grad_rows, norm_factor),
        places,
        [turned] + pairs,
        [
            shape(grad_rows + step_lines, width, dtype=BF16),
            shape(seq_count * length, width, dtype=BF16),
            shape(step_lines, seq_count * length, dtype=BF16),
        ],
    )
    arrived = lax.ppermute(leaving, "dp", ring("dp", 1))
    kept, kept_step = call(
        functools.partial(keep, grad_rows, norm_factor),
        None,
        [turned, grads, steps],
        [shape(grad_rows, width), shape(step_lines, padded)],
    )
    mixer_blocks = call(
        functools.partial(mix, relative, taps, grad_rows // chan_count, norm_factor, chan_count),
        places,
        [own_turned] + mixers,
        [shape(grad_rows // chan_count * dp_count, mixed, dtype=BF16)] * chan_count,
        [pltpu.VMEM((dp_count * padded, mixed), F32), pltpu.VMEM((seq_count * rows, mixed), BF16)],
        cost=2,
    )
    mixer_blocks = list(mixer_blocks[:1]) + [
        lax.ppermute(block, "chan", ring("chan", hop))
        for hop, block in enumerate(mixer_blocks[1:], 1)
    ]
    mixer_kept, mixer_leaving = call(
        add_chan,
        None,
        mixer_blocks,
        [shape(grad_rows // chan_count, mixed), shape(grad_rows // chan_count, mixed, dtype=BF16)],
        cost=1,
    )
    mixer_arrived = lax.ppermute(mixer_leaving, "dp", ring("dp", 1))
    total, ending, back = call(
        gather_share,
        None,
        taken,
        [
            jax.ShapeDtypeStruct((rows, model), BF16),
            shape(PAD, model),
            shape(PAD, model, dtype=BF16),
        ],
        cost=1,
    )
    backward_pairs = [(source + 1, source) for source in range(seq_count - 1)]
    late = lax.ppermute(back, "seq", backward_pairs)
    inner_weight_grad, step_weight_grad, input_grad, mixer_weight_grad = call(
        functools.partial(close, taps, chan_count, used),
        places,
        [kept, kept_step, arrived, total, ending, late, mixer_kept, mixer_arrived],
        [
            jax.ShapeDtypeStruct((grad_rows, width), F32),
            jax.ShapeDtypeStruct((head_count, grad_rows), F32),
            jax.ShapeDtypeStruct((rows, model), BF16),
            jax.ShapeDtypeStruct((grad_rows // chan_count, mixed), F32),
        ],
        [pltpu.VMEM((PAD, model), BF16), pltpu.SemaphoreType.DMA],
        cost=1,
        plain=(3,),
        left=(3,),
        in_place=(3, 2),
    )
    step_weight_grad = step_weight_grad.T
    return (input_grad[None], inner_weight_grad, mixer_weight_grad, step_weight_grad)


def solution(mesh):
    in_specs = (
        P("dp", ("seq", "chan"), None),
        P(None, "chan"),
        P(),
        P(None, "chan"),
        P(None, "chan"),
        P(),
        P("chan"),
        P("chan"),
        P("chan"),
        P("dp", "seq", "chan"),
    )
    out_specs = (
        P("dp", ("seq", "chan"), None),
        P(("dp", "seq"), "chan"),
        P(("dp", "seq", "chan"), None),
        P(("dp", "seq"), "chan"),
    )
    return jax.shard_map(body, mesh=mesh, in_specs=in_specs, out_specs=out_specs, check_vma=False)
```

```python
import functools
import math

import jax
import jax.numpy as jnp
from jax import lax
from jax.experimental import pallas as pl
from jax.experimental.pallas import tpu as pltpu
from jax.sharding import PartitionSpec as P


F32 = jnp.float32
BF16 = jnp.bfloat16
LANES = 128
PAD = 8
DIRECT = 8


def dot(left, right, left_dim=1, right_dim=0):
    return lax.dot_general(
        left,
        right,
        (((left_dim,), (right_dim,)), ((), ())),
        preferred_element_type=F32,
    )


def pieces(values):
    high = values.astype(BF16)
    rest = values - high.astype(F32)
    middle = rest.astype(BF16)
    low = (rest - middle.astype(F32)).astype(BF16)
    return high, middle, low


def fine(left, right, left_dim=1, right_dim=0):
    left_high = left.astype(BF16)
    left_low = (left - left_high.astype(F32)).astype(BF16)
    right_high = right.astype(BF16)
    right_low = (right - right_high.astype(F32)).astype(BF16)
    lefts = jnp.concatenate([left_high, left_low, left_high], axis=left_dim)
    rights = jnp.concatenate([right_high, right_high, right_low], axis=right_dim)
    return dot(lefts, rights, left_dim, right_dim)


def half_fine(left, right, left_dim=1, right_dim=0):
    high = left.astype(BF16)
    low = (left - high.astype(F32)).astype(BF16)
    rounded = right.astype(BF16)
    lefts = jnp.concatenate([high, low], axis=left_dim)
    return dot(lefts, jnp.concatenate([rounded, rounded], axis=right_dim), left_dim, right_dim)


def masked_sum(mask, values, values_dim=0):
    chosen = jnp.where(mask, 1.0, 0.0).astype(BF16)
    masks = jnp.concatenate([chosen] * 3, axis=1)
    return dot(masks, jnp.concatenate(pieces(values), axis=values_dim), 1, values_dim)


def head_map(width, head_dim):
    row = lax.broadcasted_iota(jnp.int32, (LANES, width), 0)
    column = lax.broadcasted_iota(jnp.int32, (LANES, width), 1)
    start = row * head_dim
    return jnp.where((column >= start) & (column < start + head_dim), 1.0, 0.0).astype(BF16)


def spread(values, heads):
    return dot(jnp.concatenate(pieces(values), axis=1), jnp.concatenate([heads] * 3, axis=0))


def collect(values, heads):
    high, middle, _ = pieces(values)
    return dot(high, heads, 1, 1) + dot(middle, heads, 1, 1)


def sigmoid(values):
    return 1.0 / (1.0 + jnp.exp(-values))


def softplus(values):
    small = jnp.exp(-jnp.abs(values))
    series = small * (1.0 - small * (0.5 - small * (1.0 / 3.0)))
    return jnp.maximum(values, 0.0) + jnp.where(small < 1e-3, series, jnp.log(1.0 + small))


def triangle(length):
    row = lax.broadcasted_iota(jnp.int32, (length, length), 0)
    column = lax.broadcasted_iota(jnp.int32, (length, length), 1)
    return row, column


def convolve(values, history, kernel, scratch):
    length = values.shape[0]
    taps = kernel.shape[0]
    scratch[:PAD] = history.astype(F32)
    scratch[PAD:] = values.astype(F32)
    total = kernel[taps - 1 : taps] * scratch[PAD : PAD + length]
    for tap in range(taps - 1):
        start = PAD - (taps - 1) + tap
        total = total + kernel[tap : tap + 1] * scratch[start : start + length]
    return total


def convolve_back(gradient, kernel, scratch):
    length = gradient.shape[0]
    taps = kernel.shape[0]
    zeros = jnp.zeros((PAD, gradient.shape[1]), F32)
    scratch[:PAD] = zeros
    scratch[PAD : PAD + length] = gradient
    scratch[PAD + length :] = zeros
    extent = length + PAD
    total = None
    for tap in range(taps):
        start = taps - 1 - tap
        term = kernel[tap : tap + 1] * scratch[start : start + extent]
        total = term if total is None else total + term
    return total


def blocks(rows, padded, dp_count, relative, place_ref, *refs):
    own_ref, step_ref, bias_ref, log_ref, skip_ref, inner_ref, mixer_ref = refs[:7]
    own_out_ref, step_out_ref, head_ref, inner_out_ref, mixer_out_ref = refs[7:12]
    out_refs, scratch, wide, sems = refs[12:-3], refs[-3], refs[-2], refs[-1]
    parts = sems.shape[1]
    depth = inner_ref.shape[0] // parts
    copies = []
    for part in range(parts):
        span = pl.ds(part * depth, depth)
        pair = ((inner_ref, inner_out_ref), (mixer_ref, mixer_out_ref))
        for number, (source, target) in enumerate(pair):
            copy = pltpu.make_async_copy(source.at[span], target.at[span], sems.at[number, part])
            copy.start()
            copies.append(copy)
    own_out_ref[...] = own_ref[...]
    head_count = bias_ref.shape[1]
    wide[...] = jnp.zeros_like(wide)
    wide[:head_count] = step_ref[...].astype(F32)
    step_out_ref[...] = wide[...].T.astype(BF16)
    head_ref[...] = jnp.zeros_like(head_ref)
    head_ref[0:1, :head_count] = bias_ref[...]
    head_ref[1:2, :head_count] = log_ref[...]
    head_ref[2:3, :head_count] = skip_ref[...]
    dp_place = place_ref[1]
    seq_count = scratch.shape[0]
    fill = jnp.zeros((own_ref.shape[0], padded - rows), F32)
    for target in range(seq_count):
        for hop in range(dp_count):
            wanted = lax.rem(dp_place + hop, dp_count)
            chosen = None
            for other in range(dp_count):
                start = (other * seq_count + target) * rows
                part = own_ref[:, start : start + rows].astype(F32)
                chosen = part if chosen is None else jnp.where(wanted == other, part, chosen)
            span = slice(hop * padded, (hop + 1) * padded)
            if padded > rows:
                chosen = jnp.concatenate([chosen, fill], axis=1)
            scratch[target, :, span] = chosen.astype(BF16)
    if relative:
        for hop, out_ref in enumerate(out_refs):
            out_ref[...] = scratch[lax.rem(place_ref[0] + hop, seq_count)]
    else:
        out_refs[0][...] = scratch[...]
    for copy in copies:
        copy.wait()


def copied(sources, targets, sems):
    copies = [
        pltpu.make_async_copy(source, target, sems.at[number])
        for number, (source, target) in enumerate(zip(sources, targets))
    ]
    for copy in copies:
        copy.start()
    return copies


def pack(*refs):
    for number, ref in enumerate(refs[:-1]):
        refs[-1][number] = ref[...]


def add_up(*refs):
    total = refs[0][...].astype(F32)
    for part in refs[1:-1]:
        total = total + part[...].astype(F32)
    refs[-1][...] = total.astype(refs[-1].dtype)


def project(count, place_ref, *refs):
    tokens = refs[:count]
    inner_ref, mixer_ref, step_ref, inner_out, mixer_out, raw_out, tail_out, scratch = refs[count:]
    place = place_ref[2]
    rows = tokens[0].shape[0]
    for hop in range(count):
        source = lax.bitwise_xor(place, hop)
        scratch[pl.ds(pl.multiple_of(source * rows, rows), rows)] = tokens[hop][...]
    gathered = scratch[...]
    length = gathered.shape[0]
    width = inner_ref.shape[1]
    whole = width // (2 * LANES) * (2 * LANES)
    mixer = dot(gathered, mixer_ref[...]).astype(BF16)
    first = dot(gathered, inner_ref[:, :whole])
    joined = jnp.concatenate([inner_ref[:, whole:], step_ref[...]], axis=1)
    second = dot(gathered, joined)
    raw_out[...] = second[:, width - whole :]
    inner = jnp.concatenate([first, second[:, : width - whole]], axis=1).astype(BF16)
    inner_out[...] = inner
    mixer_out[...] = mixer
    tail_out[:, :width] = inner[length - 2 * PAD :]
    tail_out[:, width:] = mixer[length - 2 * PAD :]


def prepare(head_dim, relative, place_ref, *refs):
    (
        inner_ref,
        mixer_ref,
        history_ref,
        raw_ref,
        head_ref,
        upstream_ref,
        conv_inner_ref,
        conv_mixer_ref,
        inner_pre_ref,
        mixer_pre_ref,
        step_ref,
        decay_ref,
    ) = refs[:12]
    message_refs = refs[12:-2]
    inner_scratch, mixer_scratch = refs[-2:]
    length, width = inner_ref.shape
    state = mixer_ref.shape[1] // 2
    place = place_ref[0]
    history = history_ref[...].astype(F32)[PAD:]
    inner_pre = convolve(inner_ref[...], history[:, :width], conv_inner_ref[...], inner_scratch)
    mixer_pre = convolve(mixer_ref[...], history[:, width:], conv_mixer_ref[...], mixer_scratch)
    inner_pre_ref[...] = inner_pre
    mixer_pre_ref[...] = mixer_pre
    inner_act = inner_pre * sigmoid(inner_pre)
    mixer_act = mixer_pre * sigmoid(mixer_pre)
    step = softplus(raw_ref[...] + head_ref[0:1])
    log_decay = -step * jnp.exp(head_ref[1:2])
    row, column = triangle(length)
    decay = masked_sum(row >= column, log_decay)
    step_ref[...] = step
    decay_ref[...] = decay
    heads = head_map(width, head_dim)
    last = decay[length - 1 : length]
    tail = spread(jnp.exp(last - decay) * step, heads)
    lead = spread(jnp.exp(decay), heads)
    upstream = upstream_ref[...].astype(F32)
    forward = half_fine(mixer_act[:, :state].T, tail * inner_act).astype(BF16)
    backward = half_fine(mixer_act[:, state:].T, lead * upstream).astype(BF16)
    high, middle, low = pieces(last)
    kinds = (high.astype(F32), middle.astype(F32), low.astype(F32))
    index = lax.broadcasted_iota(jnp.int32, (PAD, LANES), 0)
    stacked = jnp.zeros((PAD, LANES), F32)
    for number, kind in enumerate(kinds):
        stacked = jnp.where(index == number, kind, stacked)
    extra = dot(stacked.astype(BF16), heads).astype(BF16)
    if relative:
        count = len(message_refs) + 1
        for hop, message_ref in enumerate(message_refs, 1):
            message_ref[:state] = jnp.where(place + hop < count, forward, backward)
            message_ref[state:] = extra
    else:
        message_ref = message_refs[0]
        for target in range(message_ref.shape[0]):
            message_ref[target, :state] = jnp.where(target > place, forward, backward)
            message_ref[target, state:] = extra


def within(
    head_dim,
    inner_pre_ref,
    mixer_pre_ref,
    step_ref,
    decay_ref,
    head_ref,
    upstream_ref,
    inner_weight_ref,
    mixer_weight_ref,
    inner_grad_ref,
    mixer_grad_ref,
    row_ref,
    column_ref,
    lead_ref,
    tail_ref,
    inner_near_ref,
    mixer_near_ref,
    sems,
):
    copies = copied(
        (inner_weight_ref, mixer_weight_ref), (inner_near_ref, mixer_near_ref), sems
    )
    length, width = inner_pre_ref.shape
    state = mixer_pre_ref.shape[1] // 2
    mixer_pre = mixer_pre_ref[...]
    mixer_act = mixer_pre * sigmoid(mixer_pre)
    input_mix = mixer_act[:, :state]
    output_mix = mixer_act[:, state:]
    decay = decay_ref[...]
    step = step_ref[...]
    turned = decay.T
    row, column = triangle(length)
    causal = column >= row
    scores = fine(input_mix, output_mix, 1, 1)
    heads = head_map(width, head_dim)
    skip = spread(head_ref[...], heads)[2:3]
    step_wide = spread(step, heads)
    lead_ref[...] = spread(jnp.exp(decay), heads)
    tail_ref[...] = spread(jnp.exp(decay[length - 1 : length] - decay) * step, heads)
    group_heads = LANES // head_dim
    lane = lax.broadcasted_iota(jnp.int32, (length, LANES), 1)
    mixed = jnp.zeros((length, length), F32)
    rows = jnp.zeros((length, LANES), F32)
    columns = []
    for group in range(width // LANES):
        span = slice(group * LANES, (group + 1) * LANES)
        inner_pre = inner_pre_ref[:, span]
        inner_act = inner_pre * sigmoid(inner_pre)
        high = inner_act.astype(BF16)
        low = (inner_act - high.astype(F32)).astype(BF16)
        upstream = upstream_ref[:, span]
        total = None
        for member in range(group_heads):
            head = group * group_heads + member
            mine = (lane >= member * head_dim) & (lane < (member + 1) * head_dim)
            mine_upstream = jnp.where(mine, upstream.astype(F32), 0.0).astype(BF16)
            spread_of = turned[head : head + 1] - decay[:, head : head + 1]
            fall = jnp.exp(jnp.where(causal, spread_of, -1e30))
            match = dot(high, mine_upstream, 1, 1) + dot(low, mine_upstream, 1, 1)
            weight = fall * scores
            cross = weight * match
            step_column = step[:, head : head + 1]
            mixed = mixed + step_column * (fall * match)
            rows = jnp.where(lane == head, jnp.sum(cross, axis=1, keepdims=True), rows)
            columns.append(jnp.sum(step_column * cross, axis=0, keepdims=True))
            weight_high = weight.astype(BF16)
            weight_low = (weight - weight_high.astype(F32)).astype(BF16)
            term = dot(weight_high, mine_upstream) + dot(weight_low, mine_upstream)
            total = term if total is None else total + term
        inner_grad_ref[:, span] = step_wide[:, span] * total + skip[:, span] * upstream.astype(F32)
    mixer_grad_ref[:, :state] = fine(mixed, output_mix)
    mixer_grad_ref[:, state:] = fine(mixed.T, input_mix)
    row_ref[...] = rows
    index = lax.broadcasted_iota(jnp.int32, (LANES, length), 0)
    stacked = jnp.zeros((LANES, length), F32)
    for number, kind in enumerate(columns):
        stacked = jnp.where(index == number, kind, stacked)
    column_ref[...] = stacked
    for copy in copies:
        copy.wait()


def finish(
    head_dim,
    relative,
    count,
    chan_count,
    place_ref,
    *refs,
):
    messages = refs[: count - 1] if relative else refs[:1]
    inner_scratch, mixer_scratch = refs[-2:]
    mixer_sent_refs = refs[-2 - chan_count : -2]
    refs = refs[len(messages) : -2 - chan_count]
    (
        inner_pre_ref,
        mixer_pre_ref,
        step_ref,
        decay_ref,
        raw_ref,
        head_ref,
        upstream_ref,
        conv_inner_ref,
        conv_mixer_ref,
        inner_grad_ref,
        mixer_grad_ref,
        row_ref,
        column_ref,
        lead_ref,
        tail_ref,
        pair_ref,
        mixer_out_ref,
        step_out_ref,
        early_ref,
    ) = refs
    length, width = inner_pre_ref.shape
    state = mixer_pre_ref.shape[1] // 2
    place = place_ref[0]

    def message(hop):
        if relative:
            return messages[hop - 1][...].astype(F32)
        return messages[0][lax.rem(place - hop + count, count)].astype(F32)

    def shard_decay(parts):
        return parts[state : state + 1] + parts[state + 1 : state + 2] + parts[state + 2 : state + 3]

    start = jnp.zeros((state, width), F32)
    running = jnp.zeros((1, width), F32)
    end = jnp.zeros((state, width), F32)
    if relative:
        received = [None] + [message(hop) for hop in range(1, count)]
        back_running = jnp.zeros((1, width), F32)
        for hop in range(1, count):
            factor = jnp.where(hop <= place, jnp.exp(running), 0.0)
            start = start + factor * received[hop][:state]
            running = running + shard_decay(received[hop])
            other = count - hop
            factor = jnp.where(other > place, jnp.exp(back_running), 0.0)
            end = end + factor * received[other][:state]
            back_running = back_running + shard_decay(received[other])
    else:

        def before(hop, carried):
            start, running = carried
            parts = message(hop)
            return start + jnp.exp(running) * parts[:state], running + shard_decay(parts)

        def after(step, carried):
            end, running = carried
            parts = message(count - step)
            return end + jnp.exp(running) * parts[:state], running + shard_decay(parts)

        start, unused = lax.fori_loop(1, place + 1, before, (start, running))
        end, unused = lax.fori_loop(1, count - place, after, (end, running))

    inner_pre = inner_pre_ref[...]
    mixer_pre = mixer_pre_ref[...]
    inner_sig = sigmoid(inner_pre)
    mixer_sig = sigmoid(mixer_pre)
    inner_act = inner_pre * inner_sig
    mixer_act = mixer_pre * mixer_sig
    input_mix = mixer_act[:, :state]
    output_mix = mixer_act[:, state:]
    decay = decay_ref[...]
    step = step_ref[...]
    upstream = upstream_ref[...].astype(F32)
    heads = head_map(width, head_dim)
    last = decay[length - 1 : length]
    lead = jnp.exp(decay)
    rest = jnp.exp(last - decay)
    lead_wide = lead_ref[...]
    tail_wide = tail_ref[...]
    from_end = half_fine(input_mix, end)
    from_start = half_fine(output_mix, start)
    inner_grad = inner_grad_ref[...] + tail_wide * from_end
    input_grad = mixer_grad_ref[:, :state] + half_fine(tail_wide * inner_act, end, 1, 1)
    output_grad = mixer_grad_ref[:, state:] + half_fine(lead_wide * upstream, start, 1, 1)
    product = jnp.sum(end * start, axis=0, keepdims=True)
    product = jnp.broadcast_to(product, (2 * PAD, width))
    gathered = jnp.concatenate([inner_act * from_end, upstream * from_start, product], axis=0)
    gathered = collect(gathered, heads)
    end_part = rest * gathered[:length]
    start_part = lead * gathered[length : 2 * length]
    product = gathered[2 * length : 2 * length + 1]
    step_grad = row_ref[...] + end_part
    sums = start_part - step * step_grad
    total = jnp.sum(step * end_part, axis=0, keepdims=True) + jnp.exp(last) * product
    row, column = triangle(length)
    after_row = column >= row
    decay_grad = masked_sum(after_row, sums) + masked_sum(after_row, column_ref[...], 1) + total
    step_grad = step_grad - jnp.exp(head_ref[1:2]) * decay_grad
    raw_grad = step_grad * sigmoid(raw_ref[...] + head_ref[0:1])
    step_out_ref[...] = raw_grad.astype(BF16)
    turned = raw_grad.T
    groups = width // length
    packed = jnp.zeros((PAD, width), F32)
    index = lax.broadcasted_iota(jnp.int32, (PAD, width), 0)
    head_count = width // head_dim
    for number in range(-(-head_count // groups)):
        line = [turned[number * groups + group : number * groups + group + 1] for group in range(groups)]
        packed = jnp.where(index == number, jnp.concatenate(line, axis=1), packed)
    inner_slope = inner_sig * (1.0 + inner_pre * (1.0 - inner_sig))
    mixer_slope = mixer_sig * (1.0 + mixer_pre * (1.0 - mixer_sig))
    inner_total = convolve_back(inner_grad * inner_slope, conv_inner_ref[...], inner_scratch)
    mixer_total = jnp.concatenate([input_grad, output_grad], axis=1) * mixer_slope
    mixer_total = convolve_back(mixer_total, conv_mixer_ref[...], mixer_scratch)
    taps = conv_inner_ref.shape[0] - 1
    early = PAD - taps
    inner_scratch[:PAD] = jnp.where(index >= early, inner_total[:PAD], packed)
    early_ref[:, :width] = inner_total[:PAD]
    early_ref[:, width:] = mixer_total[:PAD]
    pair_ref[:length] = inner_total[PAD:].astype(BF16)
    pair_ref[length:] = inner_scratch[:PAD].astype(BF16)
    mixer_out_ref[...] = mixer_total[PAD:].astype(BF16)
    rows = length // chan_count
    back = mixer_total[:PAD].astype(BF16)
    mixer_scratch[:length] = mixer_total[PAD:]
    for hop, sent_ref in enumerate(mixer_sent_refs):
        target = lax.rem(place_ref[2] + hop, chan_count)
        start = pl.multiple_of(target * rows, rows)
        sent_ref[:rows] = mixer_scratch[pl.ds(start, rows)].astype(BF16)
        sent_ref[rows:] = back


def add_late(ending, extra, taps, valid):
    index = lax.broadcasted_iota(jnp.int32, ending.shape, 0)
    late = jnp.where((index >= PAD - taps) & valid, extra, 0.0)
    return ending + late


def project_back(
    chan_count,
    place_ref,
    pair_ref,
    early_ref,
    mixer_ref,
    step_ref,
    inner_weight_ref,
    mixer_weight_ref,
    step_weight_ref,
    *refs,
):
    out_refs = refs[:chan_count]
    inner_scratch, mixer_scratch, share_scratch = refs[chan_count:]
    length, mixed = mixer_ref.shape
    width = pair_ref.shape[1]
    rows = length // chan_count
    whole = width // (2 * LANES) * (2 * LANES)
    fill = jnp.zeros((PAD, width + mixed), F32)
    early = jnp.concatenate([early_ref[...], fill], axis=0).astype(BF16)
    inner_scratch[:length, :width] = pair_ref[:length]
    inner_scratch[:length, width:] = step_ref[...]
    inner_scratch[length:, :width] = early[:, :width]
    inner_scratch[length:, width:] = jnp.zeros((2 * PAD, LANES), BF16)
    mixer_scratch[:length] = mixer_ref[...]
    mixer_scratch[length:] = early[:, width:]
    share = dot(inner_scratch[:, :whole], inner_weight_ref[:, :whole], 1, 1)
    right = jnp.concatenate([inner_weight_ref[:, whole:], step_weight_ref[...]], axis=1)
    share = share + dot(inner_scratch[:, whole:], right, 1, 1)
    share = share + dot(mixer_scratch[...], mixer_weight_ref[...], 1, 1)
    share_scratch[...] = share.astype(BF16)
    for hop, out_ref in enumerate(out_refs):
        target = lax.rem(place_ref[2] + hop, chan_count)
        start = pl.multiple_of(target * rows, rows)
        out_ref[:rows] = share_scratch[pl.ds(start, rows)]
        out_ref[rows:] = share_scratch[length : length + PAD]


def gather_share(*refs):
    total_ref, ending_ref, back_ref = refs[-3:]
    total = refs[0][...].astype(F32)
    for part in refs[1:-3]:
        total = total + part[...].astype(F32)
    rows = total_ref.shape[0]
    total_ref[...] = total[:rows].astype(BF16)
    ending_ref[...] = total[rows - PAD : rows]
    back_ref[...] = total[rows:].astype(BF16)


def close(
    taps,
    chan_count,
    used,
    place_ref,
    kept_ref,
    step_ref,
    arrived_ref,
    total_ref,
    ending_ref,
    late_ref,
    mixer_kept_ref,
    mixer_arrived_ref,
    inner_out_ref,
    step_out_ref,
    input_out_ref,
    mixer_out_ref,
    scratch,
    done,
):
    del total_ref
    valid = place_ref[2] == chan_count - 1
    ending = add_late(ending_ref[...], late_ref[...].astype(F32), taps, valid)
    scratch[...] = ending.astype(BF16)
    head = input_out_ref.shape[0] - PAD
    copy = pltpu.make_async_copy(scratch, input_out_ref.at[pl.ds(head, PAD)], done)
    copy.start()
    rows = kept_ref.shape[0]
    inner_out_ref[...] = kept_ref[...] + arrived_ref[:rows].astype(F32)
    mixer_out_ref[...] = mixer_kept_ref[...] + mixer_arrived_ref[...].astype(F32)
    step = step_ref[:, :rows] + arrived_ref[rows:, :rows].astype(F32)
    head_count = step_out_ref.shape[0]
    groups = -(-head_count // used)
    for head in range(head_count):
        line = (head % groups) * used + head // groups
        step_out_ref[head : head + 1] = step[line : line + 1]
    copy.wait()


def turn(place_ref, *refs):
    column_refs, out_ref, own_ref, columns = refs[:-3], refs[-3], refs[-2], refs[-1]
    chan_place = place_ref[2]
    chan_count = len(column_refs)
    seq_count, rows, _ = column_refs[0].shape
    length = chan_count * rows
    for hop in range(seq_count):
        for chan_hop in range(chan_count):
            chan_source = lax.rem(chan_place - chan_hop + chan_count, chan_count)
            start = pl.multiple_of(hop * length + chan_source * rows, rows)
            columns[pl.ds(start, rows)] = column_refs[chan_hop][hop]
    out_ref[...] = columns[...].T
    own = [column_refs[0][hop] for hop in range(seq_count)]
    own_ref[...] = jnp.concatenate(own, axis=0).T


def arrange(relative, taps, used, place_ref, pair_refs, grads, steps):
    seq_place = place_ref[0]
    seq_count = len(pair_refs) if relative else pair_refs[0].shape[0]
    length = grads.shape[0] // seq_count

    def message(hop):
        return pair_refs[hop][...] if relative else pair_refs[0][hop]

    for hop in range(seq_count):
        if relative:
            shard = lax.rem(seq_place - hop + seq_count, seq_count)
            after = (hop - 1) % seq_count
        else:
            shard = hop
            after = (hop + 1) % seq_count
        pair = message(hop)
        start = hop * length
        head = length - PAD
        grads[start : start + head] = pair[:head]
        extra = message(after)[length:].astype(F32)
        ending = add_late(pair[head:length].astype(F32), extra, taps, shard < seq_count - 1)
        grads[start + head : start + length] = ending.astype(BF16)
        packed = pair[length:].astype(F32)
        groups = packed.shape[1] // length
        lines = [packed[:used, group * length : (group + 1) * length] for group in range(groups)]
        spare = steps.shape[0] - used * groups
        lines = lines + [jnp.zeros((spare, length), F32)]
        steps[:, start : start + length] = jnp.concatenate(lines, axis=0).astype(BF16)


def leave(relative, taps, used, rows, scale, place_ref, *refs):
    turned_ref = refs[0]
    out_ref, grads, steps = refs[-3:]
    arrange(relative, taps, used, place_ref, refs[1:-3], grads, steps)
    padded = turned_ref.shape[0] // 2
    chosen = turned_ref[padded : padded + rows]
    out_ref[:rows] = (dot(chosen, grads[...]) * scale).astype(BF16)
    lines = steps.shape[0]
    term = dot(steps[...], turned_ref[padded:], 1, 1) * scale
    out_ref[rows:, :padded] = term.astype(BF16)
    out_ref[rows:, padded:] = jnp.zeros((lines, out_ref.shape[1] - padded), BF16)


def keep(rows, scale, turned_ref, grads_ref, steps_ref, out_ref, step_ref):
    padded = turned_ref.shape[0] // 2
    out_ref[...] = dot(turned_ref[:rows], grads_ref[...]) * scale
    step_ref[...] = dot(steps_ref[...], turned_ref[:padded], 1, 1) * scale


def mix(relative, taps, rows, scale, chan_count, place_ref, *refs):
    column_ref, scratch, grads = refs[0], refs[-2], refs[-1]
    grad_refs = refs[1 : -2 - chan_count]
    out_refs = refs[-2 - chan_count : -2]
    seq_place = place_ref[0]
    chan_place = place_ref[2]
    wide = column_ref.shape[0]
    seq_count = len(grad_refs) if relative else grad_refs[0].shape[0]
    tokens = grads.shape[0] // seq_count

    def message(hop):
        return grad_refs[hop][...] if relative else grad_refs[0][hop]

    for hop in range(seq_count):
        if relative:
            source = lax.rem(seq_place - hop + seq_count, seq_count)
            after = (hop - 1) % seq_count
        else:
            source = hop
            after = (hop + 1) % seq_count
        start = hop * tokens
        head = tokens - PAD
        block = message(hop)
        grads[start : start + head] = block[:head]
        valid = (source < seq_count - 1) & (chan_place == chan_count - 1)
        extra = message(after)[tokens:].astype(F32)
        ending = add_late(block[head:tokens].astype(F32), extra, taps, valid)
        grads[start + head : start + tokens] = ending.astype(BF16)
    padded = wide // 2
    scratch[...] = dot(column_ref[...], grads[...]) * scale
    for hop, out_ref in enumerate(out_refs):
        target = lax.rem(chan_place + hop, chan_count)
        for dp_hop in range(2):
            start = pl.multiple_of(dp_hop * padded + target * rows, PAD)
            part = scratch[pl.ds(start, rows)]
            out_ref[dp_hop * rows : (dp_hop + 1) * rows] = part.astype(BF16)


def add_chan(*refs):
    kept_ref, leaving_ref = refs[-2:]
    total = refs[0][...].astype(F32)
    for part in refs[1:-2]:
        total = total + part[...].astype(F32)
    rows = kept_ref.shape[0]
    kept_ref[...] = total[:rows]
    leaving_ref[...] = total[rows:].astype(BF16)


def shape(*dims, dtype=F32):
    return pltpu.VMEM(dims, dtype)


def ring(axis, hop):
    count = lax.axis_size(axis)
    return [(source, (source + hop) % count) for source in range(count)]


def call(body, place, arrays, out_shape, scratch=(), cost=3, plain=(), left=(), in_place=None):
    vmem = pltpu.MemorySpace.VMEM
    hbm = pltpu.MemorySpace.HBM
    arrays = [
        pltpu.with_memory_space_constraint(array, hbm if number in plain else vmem)
        for number, array in enumerate(arrays)
    ]
    in_specs = [
        pl.BlockSpec(memory_space=hbm if number in left else vmem) for number in range(len(arrays))
    ]
    out_specs = [
        pl.BlockSpec(memory_space=hbm if in_place and in_place[1] == number else vmem)
        for number in range(len(out_shape))
    ]
    if place is not None:
        in_specs = [pl.BlockSpec(memory_space=pltpu.SMEM)] + in_specs
        arrays = [place] + arrays
    return pl.pallas_call(
        body,
        out_shape=out_shape,
        in_specs=in_specs,
        out_specs=out_specs,
        scratch_shapes=list(scratch),
        input_output_aliases={in_place[0] + 1: in_place[1]} if in_place else {},
        cost_estimate=pl.CostEstimate(flops=cost * 10**8, bytes_accessed=0, transcendentals=0),
        compiler_params=pltpu.CompilerParams(vmem_limit_bytes=24 * 2**20),
    )(*arrays)


def around(block, axis):
    count = lax.axis_size(axis)
    return [block] + [
        lax.ppermute(block, axis, ring(axis, hop)) for hop in range(1, count)
    ]


def spread_out(block, axis):
    count = lax.axis_size(axis)
    parts = {0: block}
    bit = count // 2
    while bit:
        pairs = [(source, source ^ bit) for source in range(count)]
        for number in list(parts):
            parts[number | bit] = lax.ppermute(parts[number], axis, pairs)
        bit //= 2
    return [parts[number] for number in range(count)]


def body(
    layer_input,
    inner_weight,
    mixer_weight,
    step_weight,
    conv_inner,
    conv_mixer,
    step_bias,
    decay_log,
    skip_gain,
    output_grad,
):
    own = layer_input[0]
    dp_count = lax.axis_size("dp")
    seq_count = lax.axis_size("seq")
    chan_count = lax.axis_size("chan")
    place = lax.axis_index("seq")
    relative = seq_count <= DIRECT
    rows, model = own.shape
    length = rows * chan_count
    width = inner_weight.shape[1]
    head_count = step_bias.shape[0]
    head_dim = width // head_count
    mixed = mixer_weight.shape[1]
    state = mixed // 2
    upstream = output_grad[0]
    grad_rows = model // (dp_count * seq_count)
    padded = -(-grad_rows // (2 * PAD)) * (2 * PAD)
    taps = conv_inner.shape[0] - 1
    parts = next(count for count in (4, 2, 1) if model % (count * LANES) == 0)
    places = [place, lax.axis_index("dp"), lax.axis_index("chan")]
    places = jnp.stack(places).astype(jnp.int32)
    norm_factor = 1.0 / math.sqrt(length * seq_count * dp_count)

    gathered = spread_out(own, "chan")
    if relative:
        column_shapes = [shape(rows, dp_count * padded, dtype=BF16)] * seq_count
    else:
        column_shapes = [shape(seq_count, rows, dp_count * padded, dtype=BF16)]
    own_near, step_near, head_rows, inner_near, mixer_near, *sorted_columns = call(
        functools.partial(blocks, grad_rows, padded, dp_count, relative),
        places,
        [
            own,
            step_weight.T,
            step_bias[None],
            decay_log[None],
            skip_gain[None],
            inner_weight,
            mixer_weight,
        ],
        [
            shape(rows, model, dtype=BF16),
            shape(model, LANES, dtype=BF16),
            shape(PAD, LANES),
            shape(model, width, dtype=BF16),
            shape(model, mixed, dtype=BF16),
        ]
        + column_shapes,
        [
            pltpu.VMEM((seq_count, rows, dp_count * padded), BF16),
            pltpu.VMEM((LANES, model), F32),
            pltpu.SemaphoreType.DMA((2, parts)),
        ],
        cost=1,
        plain=range(7),
        left=(5, 6),
    )
    if relative:
        columns = [sorted_columns[0]]
        for hop, block in enumerate(sorted_columns[1:], 1):
            columns.append(lax.ppermute(block, "seq", ring("seq", hop)))
    else:
        columns = lax.all_to_all(sorted_columns[0], "seq", split_axis=0, concat_axis=0)
    inner_proj, mixer_proj, step_raw, tail = call(
        functools.partial(project, chan_count),
        places,
        [own_near] + gathered[1:] + [inner_near, mixer_near, step_near],
        [
            shape(length, width, dtype=BF16),
            shape(length, mixed, dtype=BF16),
            shape(length, LANES),
            shape(2 * PAD, width + mixed, dtype=BF16),
        ],
        [pltpu.VMEM((length, model), BF16)],
        cost=4,
    )
    forward_pairs = [(source, source + 1) for source in range(seq_count - 1)]
    history = lax.ppermute(tail, "seq", forward_pairs)

    if relative:
        message_shapes = [shape(state + PAD, width, dtype=BF16)] * (seq_count - 1)
    else:
        message_shapes = [shape(seq_count, state + PAD, width, dtype=BF16)]
    inner_pre, mixer_pre, step, decay, *messages = call(
        functools.partial(prepare, head_dim, relative),
        places,
        [inner_proj, mixer_proj, history, step_raw, head_rows, upstream, conv_inner, conv_mixer],
        [
            shape(length, width),
            shape(length, mixed),
            shape(length, LANES),
            shape(length, LANES),
        ]
        + message_shapes,
        [pltpu.VMEM((PAD + length, width), F32), pltpu.VMEM((PAD + length, mixed), F32)],
    )
    if relative:
        received = [
            lax.ppermute(message, "seq", ring("seq", hop))
            for hop, message in enumerate(messages, 1)
        ]
    else:
        received = [lax.all_to_all(messages[0], "seq", split_axis=0, concat_axis=0)]
    *inside, inner_back, mixer_back = call(
        functools.partial(within, head_dim),
        None,
        [
            inner_pre,
            mixer_pre,
            step,
            decay,
            head_rows,
            upstream,
            inner_weight,
            mixer_weight,
        ],
        [
            shape(length, width),
            shape(length, mixed),
            shape(length, LANES),
            shape(LANES, length),
            shape(length, width),
            shape(length, width),
            shape(model, width, dtype=BF16),
            shape(model, mixed, dtype=BF16),
        ],
        [pltpu.SemaphoreType.DMA((2,))],
        plain=(6, 7),
        left=(6, 7),
    )
    if relative:
        (columns,) = call(
            pack, None, columns, [shape(seq_count, rows, dp_count * padded, dtype=BF16)], cost=1
        )
    all_columns = around(columns, "chan")
    turned, own_turned = call(
        turn,
        places,
        all_columns,
        [
            shape(dp_count * padded, seq_count * length, dtype=BF16),
            shape(dp_count * padded, seq_count * rows, dtype=BF16),
        ],
        [pltpu.VMEM((seq_count * length, dp_count * padded), BF16)],
    )

    pair, mixer_local, step_grad, early, *mixer_sent = call(
        functools.partial(finish, head_dim, relative, seq_count, chan_count),
        places,
        received
        + [inner_pre, mixer_pre, step, decay, step_raw, head_rows, upstream, conv_inner, conv_mixer]
        + list(inside),
        [
            shape(length + PAD, width, dtype=BF16),
            shape(length, mixed, dtype=BF16),
            shape(length, LANES, dtype=BF16),
            shape(PAD, width + mixed),
        ]
        + [shape(rows + PAD, mixed, dtype=BF16)] * chan_count,
        [pltpu.VMEM((length + 2 * PAD, width), F32), pltpu.VMEM((length + 2 * PAD, mixed), F32)],
        cost=5,
    )

    def over_seq(block):
        if relative:
            return around(block, "seq")
        return [lax.all_gather(block, "seq")]

    pairs = over_seq(pair)
    mixer_rows = list(mixer_sent[:1]) + [
        lax.ppermute(block, "chan", ring("chan", hop))
        for hop, block in enumerate(mixer_sent[1:], 1)
    ]
    (mixer_rows,) = call(add_up, None, mixer_rows, [shape(rows + PAD, mixed, dtype=BF16)], cost=1)
    mixers = over_seq(mixer_rows)

    sent = call(
        functools.partial(project_back, chan_count),
        places,
        [pair, early, mixer_local, step_grad, inner_back, mixer_back, step_near],
        [shape(rows + PAD, model, dtype=BF16)] * chan_count,
        [
            pltpu.VMEM((length + 2 * PAD, width + LANES), BF16),
            pltpu.VMEM((length + 2 * PAD, mixed), BF16),
            pltpu.VMEM((length + 2 * PAD, model), BF16),
        ],
        cost=4,
    )
    taken = list(sent[:1]) + [
        lax.ppermute(block, "chan", ring("chan", hop))
        for hop, block in enumerate(sent[1:], 1)
    ]

    groups = width // length
    used = -(-head_count // groups)
    step_lines = -(-used * groups // (2 * PAD)) * (2 * PAD)
    leaving, grads, steps = call(
        functools.partial(leave, relative, taps, used, grad_rows, norm_factor),
        places,
        [turned] + pairs,
        [
            shape(grad_rows + step_lines, width, dtype=BF16),
            shape(seq_count * length, width, dtype=BF16),
            shape(step_lines, seq_count * length, dtype=BF16),
        ],
    )
    arrived = lax.ppermute(leaving, "dp", ring("dp", 1))
    kept, kept_step = call(
        functools.partial(keep, grad_rows, norm_factor),
        None,
        [turned, grads, steps],
        [shape(grad_rows, width), shape(step_lines, padded)],
    )
    mixer_blocks = call(
        functools.partial(mix, relative, taps, grad_rows // chan_count, norm_factor, chan_count),
        places,
        [own_turned] + mixers,
        [shape(grad_rows // chan_count * dp_count, mixed, dtype=BF16)] * chan_count,
        [pltpu.VMEM((dp_count * padded, mixed), F32), pltpu.VMEM((seq_count * rows, mixed), BF16)],
        cost=2,
    )
    mixer_blocks = list(mixer_blocks[:1]) + [
        lax.ppermute(block, "chan", ring("chan", hop))
        for hop, block in enumerate(mixer_blocks[1:], 1)
    ]
    mixer_kept, mixer_leaving = call(
        add_chan,
        None,
        mixer_blocks,
        [shape(grad_rows // chan_count, mixed), shape(grad_rows // chan_count, mixed, dtype=BF16)],
        cost=1,
    )
    mixer_arrived = lax.ppermute(mixer_leaving, "dp", ring("dp", 1))
    total, ending, back = call(
        gather_share,
        None,
        taken,
        [
            jax.ShapeDtypeStruct((rows, model), BF16),
            shape(PAD, model),
            shape(PAD, model, dtype=BF16),
        ],
        cost=1,
    )
    backward_pairs = [(source + 1, source) for source in range(seq_count - 1)]
    late = lax.ppermute(back, "seq", backward_pairs)
    inner_weight_grad, step_weight_grad, input_grad, mixer_weight_grad = call(
        functools.partial(close, taps, chan_count, used),
        places,
        [kept, kept_step, arrived, total, ending, late, mixer_kept, mixer_arrived],
        [
            jax.ShapeDtypeStruct((grad_rows, width), F32),
            jax.ShapeDtypeStruct((head_count, grad_rows), F32),
            jax.ShapeDtypeStruct((rows, model), BF16),
            jax.ShapeDtypeStruct((grad_rows // chan_count, mixed), F32),
        ],
        [pltpu.VMEM((PAD, model), BF16), pltpu.SemaphoreType.DMA],
        cost=1,
        plain=(3,),
        left=(3,),
        in_place=(3, 2),
    )
    step_weight_grad = step_weight_grad.T
    return (input_grad[None], inner_weight_grad, mixer_weight_grad, step_weight_grad)


def solution(mesh):
    in_specs = (
        P("dp", ("seq", "chan"), None),
        P(None, "chan"),
        P(),
        P(None, "chan"),
        P(None, "chan"),
        P(),
        P("chan"),
        P("chan"),
        P("chan"),
        P("dp", "seq", "chan"),
    )
    out_specs = (
        P("dp", ("seq", "chan"), None),
        P(("dp", "seq"), "chan"),
        P(("dp", "seq", "chan"), None),
        P(("dp", "seq"), "chan"),
    )
    return jax.shard_map(body, mesh=mesh, in_specs=in_specs, out_specs=out_specs, check_vma=False)
```
